128 devices in a mesh: seq: 32 (over z, y_hi, x), head: 4 (over y_lo, core).
Axes of the slice: x: 4, y: 4 (y_hi: 2, y_lo: 2; y = y_hi * 2 + y_lo), z: 4, core: 2. Of those that a mesh axis runs over, the one named last changes fastest.
Arguments:
- queries: bfloat16 [8192, 3584], P('seq', 'head'), may hold values from -5 to 5
- keys: bfloat16 [8192, 3584], P('seq', 'head'), may hold values from -5 to 5
- values: bfloat16 [8192, 3584], P('seq', 'head'), may hold values from -6 to 6
- attn_grad: bfloat16 [8192, 3584], P('seq', 'head'), may hold values from -6 to 6
- doc_ids: int32 [8192], replicated, may hold values from 0 to 7, never falling along the last dimension, each value on 1 to 4096 neighbouring positions
- conv_input: bfloat16 [8192, 7168], P('seq', 'head'), may hold values from -6 to 6
- conv_weight: float32 [4, 7168], P(None, 'head'), may hold values from -3 to 3
- step_raw: float32 [8192, 112], P('seq', 'head'), may hold values from -4 to 4
- step_bias: float32 [112], P('head'), may hold values from -1.5 to 0
- rate_log: float32 [112], P('head'), may hold values from -13 to -1
- skip_gain: float32 [112], P('head'), may hold values from 0.5 to 1.5
- input_coeff: bfloat16 [8192, 128], P('seq'), may hold values from -0.625 to 0.625
- output_coeff: bfloat16 [8192, 128], P('seq'), may hold values from -0.625 to 0.625
- gate_input: bfloat16 [8192, 7168], P('seq', 'head'), may hold values from -6 to 6
- mix_grad: bfloat16 [8192, 7168], P('seq', 'head'), may hold values from -1.5 to 1.5
Outputs:
- grad_queries: bfloat16 [8192, 3584], P('seq', 'head')
- grad_keys: bfloat16 [8192, 3584], P('seq', 'head')
- grad_values: bfloat16 [8192, 3584], P('seq', 'head')
- grad_conv_input: bfloat16 [8192, 7168], P('seq', 'head')
- grad_gate: bfloat16 [8192, 7168], P('seq', 'head')
- grad_step: float32 [8192, 112], P('seq', 'head')
- grad_input_coeff: float32 [8192, 128], P('seq')
- grad_output_coeff: float32 [8192, 128], P('seq')
- grad_conv_weight: float32 [4, 7168], P(None, 'head')
- grad_step_bias: float32 [112], P('head')
- grad_rate_log: float32 [112], P('head')
- grad_skip: float32 [112], P('head')
The draws below stay inside these ranges and needn't reach their ends.
Inputs may be any that keep to these rules, and one draw needn't show every extreme that they name: doc_ids never fall along the sequence.
All inputs are finite; a program needn't handle non-finite values.
Results may differ from the reference program's by a relative error of at most 0.012.
Values may be sent and summed in bfloat16 or wider, within the bound.
No kernel may reach another device: no remote copies, remote signals or barrier semaphores. Data moves between devices by JAX's collectives and lax.ppermute only.
A program may use at most 128 MiB of HBM per device.

```python
import math
import jax
import jax.numpy as jnp
import numpy as np
from jax import lax

T_DEV = 256
HEADS = 16
HEAD_DIM = 224
WINDOW = 1024
SSM_HEADS = 112
SSM_DIM = 64
STATE = 64
GROUPS = 2
KERNEL = 4
STRETCH = 128
SEQLEN = 8192
INNER = 7168
DOCS = 8


def aligned_pair(key):
    shape = (SEQLEN, HEADS * HEAD_DIM)
    normal_query = jax.random.truncated_normal(jax.random.fold_in(key, 11), -4.5, 4.5, shape, jnp.float32)
    normal_key = jax.random.truncated_normal(jax.random.fold_in(key, 12), -4.5, 4.5, shape, jnp.float32)
    return (normal_query, normal_key)


def draw_queries(key, part):
    return aligned_pair(key)[0].astype(jnp.bfloat16)


def draw_keys(key, part):
    return aligned_pair(key)[1].astype(jnp.bfloat16)


def draw_step_raw(key, part):
    blocks = SEQLEN // STRETCH
    offsets = jax.random.uniform(jax.random.fold_in(key, 21), (blocks, 1, SSM_HEADS), jnp.float32, -1.0, 1.0)
    noise = 0.5 * jax.random.truncated_normal(jax.random.fold_in(key, 23), -5.0, 5.0, (blocks, STRETCH, SSM_HEADS), jnp.float32)
    return (noise + offsets).reshape(SEQLEN, SSM_HEADS)


def draw_rate_log(key, part):
    chance = 0.5
    picked = jax.random.uniform(jax.random.fold_in(key, 31), (SSM_HEADS,), jnp.float32) < chance
    quick = jnp.log(jax.random.uniform(jax.random.fold_in(key, 32), (SSM_HEADS,), jnp.float32, 0.05, 0.3))
    slowly = jnp.log(jax.random.uniform(jax.random.fold_in(key, 33), (SSM_HEADS,), jnp.float32, 0.3, 2.0) / SEQLEN)
    return jnp.where(picked, quick, slowly)


def level_of(rng, shape, cuts, least, top_value):
    factor_of = 1.0
    for dim, shards_of in cuts:
        steps = jax.random.uniform(jax.random.fold_in(jax.random.fold_in(rng, 6), dim), (shards_of,), jnp.float32, least / len(cuts), top_value / len(cuts))
        factor_of = factor_of * jnp.repeat(jnp.exp(steps), shape[dim] // shards_of).reshape((-1,) + (1,) * (len(shape) - 1 - dim))
    return factor_of


def length_profile(count, total, bound, skew):
    loads = [(1 << 20) // math.isqrt(standing ** skew) + 1 for standing in range(2, count + 1)]
    rest, holding = total - bound - (count - 1), [1] * (count - 1)
    while rest > 0:
        free = [i for i in range(count - 1) if holding[i] < bound]
        whole, left = sum([loads[i] for i in free]), rest
        for i in free:
            addition = min(bound - holding[i], max(1, left * loads[i] // whole), rest)
            holding[i] = holding[i] + addition
            rest = rest - addition
    return np.array([bound] + holding)


def ragged_sizes(rng, number_of, total, reach, slope):
    if number_of == 2:
        one = jax.random.randint(rng, (), max(1, total - reach), min(reach, total - 1) + 1)
        return jnp.stack([one, total - one])
    sizes = jnp.asarray(length_profile(number_of, total, reach, slope), jnp.int32)
    twos = (number_of - 1) // 2
    giver, sink = sizes[1:1 + 2 * twos:2], sizes[2:2 + 2 * twos:2]
    margin = jnp.minimum(giver - 1, reach - sink)
    moved = jax.random.randint(jax.random.fold_in(rng, 1), (twos,), 0, 1 << 20) % (margin + 1)
    sizes = sizes.at[1:1 + 2 * twos:2].set(giver - moved).at[2:2 + 2 * twos:2].set(sink + moved)
    return sizes[jax.random.permutation(jax.random.fold_in(rng, 2), number_of)]


def bell_draw(key, shape, scale, most, split=(), kind=jnp.bfloat16):
    entries = jax.random.normal(key, shape, jnp.float32) * scale
    if len(split) > 0:
        entries = level_of(key, shape, split, -0.22, 0.18) * entries
    return jnp.clip(entries, min=-most, max=most).astype(kind)


def setup_inputs(seed: int = 0) -> dict:
    arg_keys = jax.random.split(jax.random.key(seed), 16)
    queries = draw_queries(jax.random.fold_in(arg_keys[15], 71), 0)
    keys = draw_keys(jax.random.fold_in(arg_keys[15], 71), 0)
    values = bell_draw(arg_keys[2], (SEQLEN, HEADS * HEAD_DIM), 1.0, 6.0, ((0, 32), (1, 4)))
    attn_grad = bell_draw(arg_keys[3], (SEQLEN, HEADS * HEAD_DIM), 1.0, 6.0, ((0, 32), (1, 4)))
    doc_ids = jnp.searchsorted(jnp.cumsum(ragged_sizes(arg_keys[4], DOCS, SEQLEN, SEQLEN // 2, 2)), jnp.arange(SEQLEN), side="right").astype(jnp.int32)
    conv_input = bell_draw(arg_keys[5], (SEQLEN, INNER), 1.0, 6.0, ((0, 32), (1, 4)))
    conv_weight = bell_draw(arg_keys[6], (KERNEL, INNER), KERNEL ** -0.5, 3.0, ((1, 4),), jnp.float32)
    step_raw = draw_step_raw(jax.random.fold_in(arg_keys[15], 71), 0)
    step_bias = jnp.clip(-1.5 + 1.5 * jax.random.uniform(arg_keys[8], (SSM_HEADS,), jnp.float32) ** level_of(arg_keys[8], (SSM_HEADS,), ((0, 4),), -0.2, 0.2), -1.5, 0.0)
    rate_log = draw_rate_log(jax.random.fold_in(arg_keys[15], 71), 0)
    skip_gain = jnp.clip(0.5 + 1.0 * jax.random.uniform(arg_keys[10], (SSM_HEADS,), jnp.float32) ** level_of(arg_keys[10], (SSM_HEADS,), ((0, 4),), -0.2, 0.2), 0.5, 1.5)
    input_coeff = bell_draw(arg_keys[11], (SEQLEN, GROUPS * STATE), 0.1, 0.625, ((0, 32),))
    output_coeff = bell_draw(arg_keys[12], (SEQLEN, GROUPS * STATE), 0.1, 0.625, ((0, 32),))
    gate_input = bell_draw(arg_keys[13], (SEQLEN, INNER), 1.0, 6.0, ((0, 32), (1, 4)))
    mix_grad = bell_draw(arg_keys[14], (SEQLEN, INNER), 0.25, 1.5, ((0, 32), (1, 4)))
    return dict(queries=queries, keys=keys, values=values, attn_grad=attn_grad, doc_ids=doc_ids, conv_input=conv_input, conv_weight=conv_weight, step_raw=step_raw, step_bias=step_bias, rate_log=rate_log, skip_gain=skip_gain, input_coeff=input_coeff, output_coeff=output_coeff, gate_input=gate_input, mix_grad=mix_grad)


NEG_FILL = -1e+30
EXACT = lax.Precision.HIGHEST

def conv_act(padded, doc_ext, weight):
    kernel_taps = weight.shape[0]
    length = padded.shape[0] - kernel_taps + 1
    doc_now = doc_ext[kernel_taps - 1:]
    summed = jnp.zeros((length, padded.shape[1]), jnp.float32)
    for lagged in range(kernel_taps):
        first_row = kernel_taps - 1 - lagged
        shifted = padded[first_row:first_row + length]
        same_doc = doc_ext[first_row:first_row + length] == doc_now
        summed = summed + weight[lagged] * jnp.where(same_doc[:, None], shifted, 0.0)
    return jax.nn.silu(summed)

def stretch_layout(log_decay, doc_row, doc_before):
    blocks = doc_row.shape[0] // STRETCH
    cumulative = jnp.cumsum(log_decay.reshape(blocks, STRETCH), axis=1)
    doc_grid = doc_row.reshape(blocks, STRETCH)
    previous = jnp.concatenate([jnp.reshape(doc_before, (1,)), doc_grid[:-1, -1]])
    return (cumulative, doc_grid, previous)

def head_final(head_act, step_size, log_decay, in_grid, start_state, doc_row, doc_before):
    cumulative, doc_grid, previous = stretch_layout(log_decay, doc_row, doc_before)
    blocks = cumulative.shape[0]
    scaled = (head_act * step_size[:, None]).reshape(blocks, STRETCH, head_act.shape[1])
    same_end = doc_grid == doc_grid[:, -1:]
    to_end = jnp.where(same_end, jnp.exp(jnp.where(same_end, cumulative[:, -1:] - cumulative, 0.0)), 0.0)
    local_state = jnp.einsum('cjp,cjn->cpn', scaled * to_end[:, :, None], in_grid, precision=EXACT)
    through = jnp.where(doc_grid[:, -1] == previous, jnp.exp(cumulative[:, -1]), 0.0)

    def advance(carry_state, pair_item):
        return (pair_item[0] * carry_state + pair_item[1], carry_state)
    final_state, starts = lax.scan(advance, start_state, (through, local_state))
    return (final_state, starts, cumulative, doc_grid, previous, scaled)

def head_output(head_act, step_size, log_decay, pair_grid, in_grid, out_grid, gate_part, skip_gain, start_state, doc_row, doc_before):
    final_state, starts, cumulative, doc_grid, previous, scaled = head_final(head_act, step_size, log_decay, in_grid, start_state, doc_row, doc_before)
    causal = jnp.arange(STRETCH)[:, None] >= jnp.arange(STRETCH)[None, :]
    same_doc = (doc_grid[:, :, None] == doc_grid[:, None, :]) & causal[None]
    weights = jnp.where(same_doc, jnp.exp(jnp.where(same_doc, cumulative[:, :, None] - cumulative[:, None, :], 0.0)), 0.0)
    inner_part = jnp.einsum('cij,cjp->cip', pair_grid * weights, scaled, precision=EXACT)
    enter_gain = jnp.where(doc_grid == previous[:, None], jnp.exp(cumulative), 0.0)
    carried = jnp.einsum('cin,cpn->cip', out_grid, starts, precision=EXACT) * enter_gain[:, :, None]
    mixed_out = (inner_part + carried).reshape(head_act.shape) + skip_gain * head_act
    return (mixed_out * jax.nn.silu(gate_part), final_state)

def round_edge(term):
    edge = lax.optimization_barrier(term[:WINDOW].astype(jnp.bfloat16)).astype(jnp.float32)
    return jnp.concatenate([edge, term[WINDOW:]], axis=0)

def attention_grads(queries, keys, values, attn_grad, doc_ids):
    width = HEADS * HEAD_DIM
    span = WINDOW + T_DEV
    scale = HEAD_DIM ** (-0.5)
    key_pad = jnp.concatenate([jnp.zeros((WINDOW, width), keys.dtype), keys])
    value_pad = jnp.concatenate([jnp.zeros((WINDOW, width), values.dtype), values])
    doc_pad = jnp.concatenate([jnp.full((WINDOW,), -1, jnp.int32), doc_ids])
    distance = jnp.arange(T_DEV)[:, None] + WINDOW - jnp.arange(span)[None, :]
    in_window = (distance >= 0) & (distance < WINDOW)

    def one_block(carry, index):
        key_acc, value_acc = carry
        first_row = index * T_DEV
        query_part = lax.dynamic_slice_in_dim(queries, first_row, T_DEV).astype(jnp.float32).reshape(T_DEV, HEADS, HEAD_DIM)
        grad_part = lax.dynamic_slice_in_dim(attn_grad, first_row, T_DEV).astype(jnp.float32).reshape(T_DEV, HEADS, HEAD_DIM)
        key_part = lax.dynamic_slice_in_dim(key_pad, first_row, span).astype(jnp.float32).reshape(span, HEADS, HEAD_DIM)
        value_part = lax.dynamic_slice_in_dim(value_pad, first_row, span).astype(jnp.float32).reshape(span, HEADS, HEAD_DIM)
        doc_query = lax.dynamic_slice_in_dim(doc_ids, first_row, T_DEV)
        doc_key = lax.dynamic_slice_in_dim(doc_pad, first_row, span)
        allowed = in_window & (doc_query[:, None] == doc_key[None, :])
        scores = jnp.where(allowed[None], jnp.einsum('ihd,jhd->hij', query_part, key_part) * scale, NEG_FILL)
        row_max = lax.optimization_barrier(jnp.max(scores, axis=-1))
        expo = jnp.where(allowed[None], jnp.exp(scores - row_max[:, :, None]), 0.0)
        row_sum = lax.optimization_barrier(jnp.sum(expo, axis=-1))
        probs = expo / jnp.maximum(row_sum, 1.0)[:, :, None]
        probs_half = lax.optimization_barrier(probs.astype(jnp.bfloat16)).astype(jnp.float32)
        attn_out = jnp.einsum('hij,jhd->ihd', probs_half, value_part)
        delta = lax.optimization_barrier(jnp.sum(grad_part * attn_out, axis=-1)).T
        dprob = jnp.einsum('ihd,jhd->hij', grad_part, value_part)
        dscore = lax.optimization_barrier((probs * (dprob - delta[:, :, None])).astype(jnp.bfloat16)).astype(jnp.float32)
        grad_query = (jnp.einsum('hij,jhd->ihd', dscore, key_part) * scale).reshape(T_DEV, width).astype(jnp.bfloat16)
        key_term = round_edge(jnp.einsum('hij,ihd->jhd', dscore, query_part).reshape(span, width))
        value_term = round_edge(jnp.einsum('hij,ihd->jhd', probs_half, grad_part).reshape(span, width))
        key_acc = lax.dynamic_update_slice_in_dim(key_acc, lax.dynamic_slice_in_dim(key_acc, first_row, span) + key_term, first_row, 0)
        value_acc = lax.dynamic_update_slice_in_dim(value_acc, lax.dynamic_slice_in_dim(value_acc, first_row, span) + value_term, first_row, 0)
        return ((key_acc, value_acc), grad_query)
    zero_acc = jnp.zeros((WINDOW + SEQLEN, width), jnp.float32)
    (key_acc, value_acc), grad_blocks = lax.scan(one_block, (zero_acc, zero_acc), jnp.arange(SEQLEN // T_DEV, dtype=jnp.int32))
    grad_queries = grad_blocks.reshape(SEQLEN, width)
    grad_keys = (key_acc[WINDOW:] * scale).astype(jnp.bfloat16)
    grad_values = value_acc[WINDOW:].astype(jnp.bfloat16)
    return (grad_queries, grad_keys, grad_values)

def mixer_grads(doc_ids, conv_input, conv_weight, step_raw, step_bias, rate_log, skip_gain, input_coeff, output_coeff, gate_input, mix_grad):
    doc_ext = jnp.concatenate([jnp.full((KERNEL - 1,), -1, jnp.int32), doc_ids])
    padded_all = jnp.concatenate([jnp.zeros((KERNEL - 1, INNER), jnp.float32), conv_input.astype(jnp.float32)])
    group_heads = SSM_HEADS // GROUPS
    blocks = SEQLEN // STRETCH
    zero_state = jnp.zeros((SSM_DIM, STATE), jnp.float32)
    start_doc = jnp.int32(-1)

    def forward(padded, weight, raw_step, bias_one, rate_one, skip_one, group_in, group_out, gate_part):
        head_act = conv_act(padded, doc_ext, weight)
        step_size = jax.nn.softplus(raw_step + bias_one)
        log_decay = -step_size * jnp.exp(rate_one)
        in_grid = group_in.reshape(blocks, STRETCH, STATE)
        out_grid = group_out.reshape(blocks, STRETCH, STATE)
        pair_grid = jnp.einsum('cin,cjn->cij', out_grid, in_grid, precision=EXACT)
        return head_output(head_act, step_size, log_decay, pair_grid, in_grid, out_grid, gate_part, skip_one, zero_state, doc_ids, start_doc)[0]

    def one_head(carry, head_index):
        sum_in, sum_out = carry
        column = head_index * SSM_DIM
        group_col = head_index // group_heads * STATE
        primals = (lax.dynamic_slice_in_dim(padded_all, column, SSM_DIM, 1), lax.dynamic_slice_in_dim(conv_weight, column, SSM_DIM, 1), lax.dynamic_index_in_dim(step_raw, head_index, 1, keepdims=False), step_bias[head_index], rate_log[head_index], skip_gain[head_index], lax.dynamic_slice_in_dim(input_coeff, group_col, STATE, 1).astype(jnp.float32), lax.dynamic_slice_in_dim(output_coeff, group_col, STATE, 1).astype(jnp.float32), lax.dynamic_slice_in_dim(gate_input, column, SSM_DIM, 1).astype(jnp.float32))
        cotangent = lax.dynamic_slice_in_dim(mix_grad, column, SSM_DIM, 1).astype(jnp.float32)
        gradients = jax.vjp(forward, *primals)[1](cotangent)
        sum_in = lax.dynamic_update_slice_in_dim(sum_in, lax.dynamic_slice_in_dim(sum_in, group_col, STATE, 1) + gradients[6], group_col, 1)
        sum_out = lax.dynamic_update_slice_in_dim(sum_out, lax.dynamic_slice_in_dim(sum_out, group_col, STATE, 1) + gradients[7], group_col, 1)
        return ((sum_in, sum_out), (gradients[0][KERNEL - 1:].astype(jnp.bfloat16), gradients[8].astype(jnp.bfloat16), gradients[2], gradients[1], gradients[3], gradients[4], gradients[5]))
    zero_cols = jnp.zeros((SEQLEN, GROUPS * STATE), jnp.float32)
    (sum_in, sum_out), stacked = lax.scan(one_head, (zero_cols, zero_cols), jnp.arange(SSM_HEADS, dtype=jnp.int32))
    conv_grad, gate_grad, step_grad, weight_grad, bias_grad, rate_grad, skip_grad = stacked
    grad_conv_input = jnp.transpose(conv_grad, (1, 0, 2)).reshape(SEQLEN, INNER)
    grad_gate = jnp.transpose(gate_grad, (1, 0, 2)).reshape(SEQLEN, INNER)
    grad_conv_weight = jnp.transpose(weight_grad, (1, 0, 2)).reshape(KERNEL, INNER)
    return (grad_conv_input, grad_gate, step_grad.T, sum_in, sum_out, grad_conv_weight, bias_grad, rate_grad, skip_grad)

def reference(queries, keys, values, attn_grad, doc_ids, conv_input, conv_weight, step_raw, step_bias, rate_log, skip_gain, input_coeff, output_coeff, gate_input, mix_grad):
    grad_queries, grad_keys, grad_values = attention_grads(queries, keys, values, attn_grad, doc_ids)
    grad_conv_input, grad_gate, grad_step, grad_input_coeff, grad_output_coeff, grad_conv_weight, grad_step_bias, grad_rate_log, grad_skip = mixer_grads(doc_ids, conv_input, conv_weight, step_raw, step_bias, rate_log, skip_gain, input_coeff, output_coeff, gate_input, mix_grad)
    return (grad_queries, grad_keys, grad_values, grad_conv_input, grad_gate, grad_step, grad_input_coeff, grad_output_coeff, grad_conv_weight, grad_step_bias, grad_rate_log, grad_skip)
```

```python
import jax
import jax.numpy as jnp
from jax import lax
from jax.experimental import pallas as pl
from jax.experimental.pallas import tpu as pltpu
from jax.sharding import Mesh
from jax.sharding import PartitionSpec as P

HEAD_DIM = 224
WINDOW = 1024
SSM_HEADS = 112
STATE = 64
GROUPS = 2
KERNEL = 4
SEQ = ("seq_0", "seq_1", "seq_2")
SHARDS = 32
T = 256
LOCAL_HEADS = 4
REACH = WINDOW // T
BLK = 256
HEADS_BLK = BLK // 64
COLS = 1792
STEPS = COLS // BLK
NEG = -1e30
F32 = jnp.float32
BF16 = jnp.bfloat16

NN = (((1,), (0,)), ((), ()))
NT = (((1,), (1,)), ((), ()))
TN = (((0,), (0,)), ((), ()))


def dot(a, b, dims=NN):
    return lax.dot_general(a, b, dims, preferred_element_type=F32)


def exact(a, b, dims=NN):
    return lax.dot_general(
        a, b, dims, preferred_element_type=F32, precision=lax.Precision.HIGHEST
    )


def split(a, pieces):
    parts = []
    for _ in range(pieces):
        part = a.astype(BF16)
        parts.append(part)
        a = a - part.astype(F32)
    return parts


def sigmoid(v):
    return 1.0 / (1.0 + jnp.exp(-v))


def iota(shape, dim):
    return lax.broadcasted_iota(jnp.int32, shape, dim)


def columns_of(row):
    return jnp.transpose(jnp.broadcast_to(row, (T, T)))


def token_setup(docs, step_pad, params, cum_s, step_s, mask_s, prev_s, end_s):
    own = columns_of(docs[0:1].astype(F32))
    for lag in range(1, KERNEL):
        lagged = columns_of(docs[4 + lag : 5 + lag].astype(F32))
        mask_s[lag - 1] = jnp.where(own == lagged, 1.0, 0.0)
    before = docs[5:6, 0:1].astype(F32)
    last = docs[0:1, T - 1 : T].astype(F32)
    prev_s[...] = jnp.where(own == before, 0.0, NEG)
    end_s[...] = jnp.where(own == last, 0.0, NEG)
    raw = step_pad + params[0:1]
    step = jnp.maximum(raw, 0.0) + jnp.log1p(jnp.exp(-jnp.abs(raw)))
    decay = -step * jnp.exp(params[1:2])
    lower = jnp.where(iota((T, T), 0) >= iota((T, T), 1), 1.0, 0.0)
    cum = exact(lower, decay)
    for n, part in enumerate(split(cum, 3)):
        cum_s[n] = part
    for n, part in enumerate(split(step, 2)):
        step_s[n] = part
    return raw, step, decay, cum


def spread_of(step_id):
    head = iota((128, BLK), 0)
    owner = step_id * HEADS_BLK + iota((128, BLK), 1) // 64
    return jnp.where(head == owner, 1.0, 0.0).astype(BF16)


def block_gains(step_id, cum_s, step_s, prev_s, end_s):
    spread = spread_of(step_id)
    cum = dot(cum_s[0], spread) + dot(cum_s[1], spread) + dot(cum_s[2], spread)
    step = dot(step_s[0], spread) + dot(step_s[1], spread)
    enter = jnp.exp(cum + prev_s[...])
    to_end = jnp.exp(cum[T - 1 : T] - cum + end_s[...])
    return spread, cum, step, enter, to_end


def conv_pre(x, halo, weight, mask_s):
    extended = jnp.concatenate([halo.astype(F32), x.astype(F32)], axis=0)
    shifted = [extended[8:]]
    summed = weight[0:1] * shifted[0]
    for lag in range(1, KERNEL):
        moved = pltpu.roll(extended, lag, 0)[8:] * mask_s[lag - 1]
        shifted.append(moved)
        summed = summed + weight[lag : lag + 1] * moved
    return summed, shifted


def mixer_first_kernel(
    x_ref, halo_ref, weight_ref, gate_ref, grad_ref, step_ref, par_ref, docs_ref, bc_ref,
    state_ref, through_ref,
    cum_s, step_s, mask_s, prev_s, end_s,
):
    step_id = pl.program_id(0)

    @pl.when(step_id == 0)
    def _():
        cum = token_setup(
            docs_ref[...], step_ref[...], par_ref[...], cum_s, step_s, mask_s, prev_s, end_s
        )[3]
        through = jnp.exp(cum[T - 1 : T] + prev_s[T - 1 : T, 0:1])
        high, low = split(through, 2)
        row = iota((8, 128), 0)
        both = jnp.where(row == 0, high.astype(F32), jnp.where(row == 1, low.astype(F32), 0.0))
        through_ref[...] = both.astype(BF16)

    _, _, step, enter, to_end = block_gains(step_id, cum_s, step_s, prev_s, end_s)
    pre, _ = conv_pre(x_ref[...], halo_ref[...], weight_ref[...], mask_s)
    act = pre * sigmoid(pre)
    gate = gate_ref[...].astype(F32)
    out_grad = grad_ref[...].astype(F32) * gate * sigmoid(gate)
    lane = iota((T, 128), 1)
    bc = bc_ref[...].astype(F32)
    in_half = jnp.where(lane < STATE, bc, 0.0).astype(BF16)
    out_half = jnp.where(lane < STATE, 0.0, bc).astype(BF16)
    ended = (act * step * to_end).astype(BF16)
    entered = (out_grad * enter).astype(BF16)
    state_ref[...] = (dot(ended, in_half, TN) + dot(entered, out_half, TN)).astype(BF16)


def whole(shape):
    return pl.BlockSpec(shape, lambda c: (0,) * len(shape))


def column_block(rows):
    return pl.BlockSpec((rows, BLK), lambda c: (0, c))


TOKEN_SCRATCH = [
    pltpu.VMEM((3, T, 128), BF16),
    pltpu.VMEM((2, T, 128), BF16),
    pltpu.VMEM((KERNEL - 1, T, BLK), F32),
    pltpu.VMEM((T, BLK), F32),
    pltpu.VMEM((T, BLK), F32),
]


def mixer_first(x, halo, weight, gate, grad, step_pad, params, docs, in_out):
    return pl.pallas_call(
        mixer_first_kernel,
        grid=(STEPS,),
        in_specs=[
            column_block(T), column_block(8), column_block(KERNEL), column_block(T),
            column_block(T), whole((T, 128)), whole((8, 128)), whole((8, T)), whole((T, 128)),
        ],
        out_specs=[pl.BlockSpec((BLK, 128), lambda c: (c, 0)), whole((8, 128))],
        out_shape=[
            jax.ShapeDtypeStruct((COLS, 128), BF16),
            jax.ShapeDtypeStruct((8, 128), BF16),
        ],
        scratch_shapes=TOKEN_SCRATCH,
        name="mixer_first",
    )(x, halo, weight, gate, grad, step_pad, params, docs, in_out)


ROWS = COLS // SHARDS


def chain_kernel(slot_ref, parts_ref, out_ref, forward_s):
    slot = slot_ref[0]
    owner = (slot * ROWS + iota((ROWS, 128), 0)) // 64
    choose = jnp.where(owner == iota((ROWS, 128), 1), 1.0, 0.0)
    lane = iota((ROWS, 128), 1)
    through = []
    carry = jnp.zeros((ROWS, 128), F32)
    for shard in range(SHARDS):
        row = parts_ref[shard, ROWS : ROWS + 1].astype(F32)
        row = row + parts_ref[shard, ROWS + 1 : ROWS + 2].astype(F32)
        gain = jnp.sum(choose * row, axis=1, keepdims=True)
        through.append(gain)
        forward_s[shard] = carry
        carry = gain * carry + parts_ref[shard, 0:ROWS].astype(F32)
    carry = jnp.zeros((ROWS, 128), F32)
    for shard in reversed(range(SHARDS)):
        out_ref[shard] = jnp.where(lane < STATE, forward_s[shard], carry).astype(BF16)
        carry = through[shard] * carry + parts_ref[shard, 0:ROWS].astype(F32)


def chain(slot, parts):
    return pl.pallas_call(
        chain_kernel,
        in_specs=[
            pl.BlockSpec(memory_space=pltpu.SMEM),
            pl.BlockSpec(memory_space=pltpu.VMEM),
        ],
        out_specs=pl.BlockSpec(memory_space=pltpu.VMEM),
        out_shape=jax.ShapeDtypeStruct((SHARDS, ROWS, 128), BF16),
        scratch_shapes=[pltpu.VMEM((SHARDS, ROWS, 128), F32)],
        name="chain",
    )(slot, parts)


def mixer_second_kernel(
    x_ref, halo_ref, weight_ref, gate_ref, grad_ref, step_ref, par_ref, docs_ref, cb_ref,
    state_ref,
    dx_ref, tail_ref, spill_ref, dgate_ref, dstep_ref, coeff_ref, dweight_ref, small_ref,
    cum_s, step_s, mask_s, prev_s, end_s,
    cumt_s, pair_s, causal_s, dpair_s, coeff_s, row_s, dt_s, ends_s,
):
    step_id = pl.program_id(0)
    lane = iota((T, 128), 1)
    cb = cb_ref[...].astype(F32)
    out_low = jnp.where(lane < STATE, cb, 0.0).astype(BF16)
    in_high = jnp.where(lane < STATE, 0.0, cb).astype(BF16)

    @pl.when(step_id == 0)
    def _():
        docs = docs_ref[...]
        cum = token_setup(docs, step_ref[...], par_ref[...], cum_s, step_s, mask_s, prev_s, end_s)[3]
        cumt_s[...] = jnp.transpose(cum)
        doc_row = docs[0:1].astype(F32)
        same = columns_of(doc_row) == doc_row
        same = same & (iota((T, T), 0) >= iota((T, T), 1))
        causal_s[...] = jnp.where(same, 0.0, NEG)
        swapped = pltpu.roll(cb, 64, 1)
        in_low = jnp.where(lane < STATE, swapped, 0.0).astype(BF16)
        pair_s[...] = dot(out_low, in_low, NT)
        dpair_s[...] = jnp.zeros((T, T), F32)
        coeff_s[...] = jnp.zeros((T, 128), F32)
        row_s[...] = jnp.zeros((T, 128), F32)
        dt_s[...] = jnp.zeros((T, 128), F32)
        ends_s[...] = jnp.zeros((8, 128), F32)

    spread, cum, step, enter, to_end = block_gains(step_id, cum_s, step_s, prev_s, end_s)
    skip = sum(dot(part, spread) for part in split(par_ref[...], 3))[2:3]
    weight = weight_ref[...]
    pre, shifted = conv_pre(x_ref[...], halo_ref[...], weight, mask_s)
    sig = sigmoid(pre)
    act = pre * sig
    gate = gate_ref[...].astype(F32)
    gate_sig = sigmoid(gate)
    mix_grad = grad_ref[...].astype(F32)
    out_grad = mix_grad * gate * gate_sig
    scaled = act * step
    scaled_half = scaled.astype(BF16)
    grad_half = out_grad.astype(BF16)

    block_head = iota((T, BLK), 1) // 64
    inner = jnp.zeros((T, BLK), F32)
    dscaled = jnp.zeros((T, BLK), F32)
    dpair = dpair_s[...]
    for k in range(HEADS_BLK):
        mine = block_head == k
        cum_col = jnp.broadcast_to(cum[:, 64 * k : 64 * k + 1], (T, T))
        cum_row = cumt_s[pl.ds(step_id * HEADS_BLK + k, 1), :]
        weights = jnp.exp(cum_col - cum_row + causal_s[...])
        mixing = (pair_s[...] * weights).astype(BF16)
        scaled_k = jnp.where(mine, scaled_half, jnp.zeros_like(scaled_half))
        grad_k = jnp.where(mine, grad_half, jnp.zeros_like(grad_half))
        inner = inner + dot(mixing, scaled_k)
        dscaled = dscaled + dot(mixing, grad_k, TN)
        dpair = dpair + dot(grad_k, scaled_half, NT) * weights
    dpair_s[...] = dpair

    state = state_ref[...]
    carried = dot(out_low, state, NT) * enter
    from_end = dot(in_high, state, NT) * to_end
    ssm_out = inner + carried
    dscaled = dscaled + from_end
    mixed_out = ssm_out + skip * act
    dgate_ref[...] = (
        mix_grad * mixed_out * gate_sig * (1.0 + gate * (1.0 - gate_sig))
    ).astype(BF16)

    gave_out = dot((out_grad * enter).astype(BF16), state)
    gave_in = dot((scaled * to_end).astype(BF16), state)
    coeff_s[...] += jnp.where(lane < STATE, gave_out, gave_in)

    grad_round = grad_half.astype(F32)
    scaled_round = scaled_half.astype(F32)
    balance = grad_round * ssm_out - scaled_round * dscaled
    row_s[...] += sum(dot(part, spread, NT) for part in split(balance, 3))
    dt_s[...] += sum(dot(part, spread, NT) for part in split(dscaled * act, 2))

    state_wide = state.astype(F32)
    product = state_wide * pltpu.roll(state_wide, 64, 1)
    through = jnp.sum(jnp.where(iota((BLK, 128), 1) < STATE, product, 0.0), axis=1, keepdims=True)
    through_row = jnp.transpose(jnp.broadcast_to(through, (BLK, BLK)))[0:1]
    end_row = jnp.sum(scaled_round * from_end, axis=0, keepdims=True)
    end_row = end_row + through_row * enter[T - 1 : T]
    skip_row = jnp.sum(out_grad * act, axis=0, keepdims=True)
    row8 = iota((8, BLK), 0)
    both = jnp.where(row8 == 0, end_row, jnp.where(row8 == 1, skip_row, 0.0))
    ends_s[...] += sum(dot(part, spread, NT) for part in split(both, 3))

    dact = step * dscaled + skip * out_grad
    dpre = dact * sig * (1.0 + pre * (1.0 - sig))
    zeros = jnp.zeros((8, BLK), F32)
    dx = weight[0:1] * dpre
    spill = zeros
    dweight_ref[0:1] = jnp.sum(dpre * shifted[0], axis=0, keepdims=True)
    for lag in range(1, KERNEL):
        masked = dpre * mask_s[lag - 1]
        dweight_ref[lag : lag + 1] = jnp.sum(dpre * shifted[lag], axis=0, keepdims=True)
        later = pltpu.roll(jnp.concatenate([masked, zeros], axis=0), T + 8 - lag, 0)[:T]
        dx = dx + weight[lag : lag + 1] * later
        edge = pltpu.roll(jnp.concatenate([zeros, masked[:8]], axis=0), 16 - lag, 0)[:8]
        spill = spill + weight[lag : lag + 1] * edge
    dx_ref[...] = dx.astype(BF16)
    tail_ref[...] = dx[T - 8 :]
    spill_ref[...] = spill

    @pl.when(step_id == STEPS - 1)
    def _():
        params = par_ref[...]
        raw = step_ref[...] + params[0:1]
        step_all = jnp.maximum(raw, 0.0) + jnp.log1p(jnp.exp(-jnp.abs(raw)))
        rate = jnp.exp(params[1:2])
        decay = -step_all * rate
        upper = jnp.where(iota((T, T), 1) >= iota((T, T), 0), 1.0, 0.0)
        ends = ends_s[...]
        ddecay = exact(upper, row_s[...]) + ends[0:1]
        dstep = (dt_s[...] - ddecay * rate) * sigmoid(raw)
        dstep_ref[...] = dstep
        dbias = jnp.sum(dstep, axis=0, keepdims=True)
        drate = jnp.sum(ddecay * decay, axis=0, keepdims=True)
        row = iota((8, 128), 0)
        small = jnp.zeros((8, 128), F32)
        for n, vector in enumerate((dbias, drate, ends[1:2])):
            for m, part in enumerate(split(vector, 2)):
                small = jnp.where(row == 2 * n + m, part.astype(F32), small)
        small_ref[...] = small
        dpair_half = dpair_s[...].astype(BF16)
        swapped = pltpu.roll(cb, 64, 1)
        in_low = jnp.where(lane < STATE, swapped, 0.0).astype(BF16)
        out_high = jnp.where(lane < STATE, 0.0, swapped).astype(BF16)
        total = coeff_s[...] + dot(dpair_half, in_low) + dot(dpair_half, out_high, TN)
        coeff_ref[...] = total.astype(BF16)


def mixer_second(x, halo, weight, gate, grad, step_pad, params, docs, out_in, state):
    return pl.pallas_call(
        mixer_second_kernel,
        grid=(STEPS,),
        in_specs=[
            column_block(T), column_block(8), column_block(KERNEL), column_block(T),
            column_block(T), whole((T, 128)), whole((8, 128)), whole((8, T)), whole((T, 128)),
            pl.BlockSpec((BLK, 128), lambda c: (c, 0)),
        ],
        out_specs=[
            column_block(T), column_block(8), column_block(8), column_block(T),
            whole((T, 128)), whole((T, 128)), column_block(KERNEL), whole((8, 128)),
        ],
        out_shape=[
            jax.ShapeDtypeStruct((T, COLS), BF16),
            jax.ShapeDtypeStruct((8, COLS), F32),
            jax.ShapeDtypeStruct((8, COLS), F32),
            jax.ShapeDtypeStruct((T, COLS), BF16),
            jax.ShapeDtypeStruct((T, 128), F32),
            jax.ShapeDtypeStruct((T, 128), BF16),
            jax.ShapeDtypeStruct((KERNEL, COLS), F32),
            jax.ShapeDtypeStruct((8, 128), F32),
        ],
        scratch_shapes=TOKEN_SCRATCH + [
            pltpu.VMEM((128, T), F32),
            pltpu.VMEM((T, T), F32),
            pltpu.VMEM((T, T), F32),
            pltpu.VMEM((T, T), F32),
            pltpu.VMEM((T, 128), F32),
            pltpu.VMEM((T, 128), F32),
            pltpu.VMEM((T, 128), F32),
            pltpu.VMEM((8, 128), F32),
        ],
        name="mixer_second",
    )(x, halo, weight, gate, grad, step_pad, params, docs, out_in, state)


def attention_kernel(q_ref, g_ref, docs_ref, *refs):
    blocks = REACH + 1
    kv_refs = refs[:blocks]
    dq_ref, own_ref = refs[blocks : blocks + 2]
    back_refs = refs[blocks + 2 : 2 * blocks + 1]
    neg_s = refs[2 * blocks + 1]
    docs = docs_ref[...].astype(F32)
    own = columns_of(docs[0:1])
    for gap in range(blocks):
        same = own == docs[gap : gap + 1]
        if gap == 0:
            same = same & (iota((T, T), 0) >= iota((T, T), 1))
        if gap == REACH:
            same = same & (iota((T, T), 1) > iota((T, T), 0))
        neg_s[gap] = jnp.where(same, 0.0, NEG)
    scale = HEAD_DIM ** (-0.5)
    for head in range(LOCAL_HEADS):
        start, stop = head * HEAD_DIM, (head + 1) * HEAD_DIM
        left, right = start // 128 * 128, -(-stop // 128) * 128
        window = slice(left, right)
        shared = start != left
        column = iota((T, right - left), 1) + left
        mine = (column >= start) & (column < stop)
        q = q_ref[:, window]
        g = g_ref[:, window]
        q = jnp.where(mine, q, jnp.zeros_like(q))
        g = jnp.where(mine, g, jnp.zeros_like(g))
        scores = []
        top = None
        for gap in range(blocks):
            s = dot(q, kv_refs[gap][0:T, window], NT) * scale + neg_s[gap]
            scores.append(s)
            peak = jnp.max(s, axis=1, keepdims=True)
            top = peak if top is None else jnp.maximum(top, peak)
        expos = [jnp.exp(s - top) for s in scores]
        total = sum(jnp.sum(e, axis=1, keepdims=True) for e in expos)
        inverse = 1.0 / jnp.maximum(total, 1.0)
        probs = [e * inverse for e in expos]
        halves = [p.astype(BF16) for p in probs]
        dprobs = [dot(g, kv_refs[gap][T : 2 * T, window], NT) for gap in range(blocks)]
        delta = sum(
            jnp.sum(h.astype(F32) * d, axis=1, keepdims=True) for h, d in zip(halves, dprobs)
        )
        dq = jnp.zeros((T, right - left), F32)

        def put(ref, rows, value):
            value = value.astype(ref.dtype)
            if shared:
                ref[rows, left : left + 128] += value[:, :128]
                ref[rows, left + 128 : right] = value[:, 128:]
            else:
                ref[rows, window] = value

        for gap in range(blocks):
            dscore = (probs[gap] * (dprobs[gap] - delta)).astype(BF16)
            dq = dq + dot(dscore, kv_refs[gap][0:T, window])
            ref = own_ref if gap == 0 else back_refs[gap - 1]
            put(ref, slice(0, T), dot(dscore, q, TN))
            put(ref, slice(T, 2 * T), dot(halves[gap], g, TN))
        put(dq_ref, slice(0, T), jnp.where(mine, dq * scale, 0.0))


def attention(queries, grads, docs, key_values):
    width = queries.shape[1]
    vmem = pl.BlockSpec(memory_space=pltpu.VMEM)
    both = jax.ShapeDtypeStruct((2 * T, width), BF16)
    return pl.pallas_call(
        attention_kernel,
        in_specs=[vmem] * (3 + REACH + 1),
        out_specs=[vmem] * (2 + REACH),
        out_shape=[
            jax.ShapeDtypeStruct((T, width), BF16),
            jax.ShapeDtypeStruct((2 * T, width), F32),
        ] + [both] * REACH,
        scratch_shapes=[pltpu.VMEM((REACH + 1, T, T), F32)],
        name="attention",
    )(queries, grads, docs, *key_values)


def passed_along(value, axis, steps):
    count = lax.axis_size(axis)
    initial, last = (max(0, -steps), min(count, count - steps))
    return lax.ppermute(value, axis, [(source, source + steps) for source in range(initial, last)])


def exchange(array, axis):
    return lax.all_to_all(array, axis, split_axis=0, concat_axis=0, tiled=True)


def from_everyone(array, axis):
    return exchange(jnp.broadcast_to(array, (lax.axis_size(axis), *array.shape)), axis)


def local(
    queries, keys, values, attn_grad, doc_ids, conv_input, conv_weight, step_raw, step_bias,
    rate_log, skip_gain, input_coeff, output_coeff, gate_input, mix_grad,
):
    heads = step_raw.shape[1]
    shard = lax.axis_index(SEQ)
    halo = passed_along(conv_input[T - 8 :], SEQ, 1)
    own = jnp.concatenate([keys, values], axis=0)
    key_values = [own] + [passed_along(own, SEQ, gap) for gap in range(1, REACH + 1)]

    doc_pad = jnp.concatenate([jnp.full((WINDOW,), -1, jnp.int32), doc_ids])
    doc_near = lax.dynamic_slice_in_dim(doc_pad, shard * T, WINDOW + T)
    docs = jnp.stack(
        [doc_near[WINDOW - T * gap : WINDOW - T * gap + T] for gap in range(REACH + 1)]
        + [doc_near[WINDOW - lag : WINDOW - lag + T] for lag in range(1, KERNEL)]
    )
    step_pad = jnp.pad(step_raw, ((0, 0), (0, 128 - heads)))
    params = jnp.pad(jnp.stack([step_bias, rate_log, skip_gain]), ((0, 5), (0, 128 - heads)))
    first = lax.axis_index("head") * heads < SSM_HEADS // GROUPS
    group_in = jnp.where(first, input_coeff[:, :STATE], input_coeff[:, STATE:])
    group_out = jnp.where(first, output_coeff[:, :STATE], output_coeff[:, STATE:])
    in_out = jnp.concatenate([group_in, group_out], axis=1)
    out_in = jnp.concatenate([group_out, group_in], axis=1)

    parts, through = mixer_first(
        conv_input, halo, conv_weight, gate_input, mix_grad, step_pad, params, docs, in_out
    )
    parts = jnp.concatenate(
        [
            parts.reshape(SHARDS, ROWS, 128),
            jnp.broadcast_to(through[None], (SHARDS, 8, 128)),
        ],
        axis=1,
    )
    slot = jnp.reshape(shard, (1,)).astype(jnp.int32)
    entering = exchange(chain(slot, exchange(parts, SEQ)), SEQ).reshape(COLS, 128)
    dx, tail, spill, dgate, dstep, coeff, dweight, small = mixer_second(
        conv_input, halo, conv_weight, gate_input, mix_grad, step_pad, params, docs, out_in,
        entering,
    )
    spilled = passed_along(spill, SEQ, -1)

    dq, own_grad, *back = attention(queries, attn_grad, docs, key_values)
    returned = [passed_along(piece, SEQ, -gap) for gap, piece in enumerate(back, 1)]

    coeffs = from_everyone(coeff, "head").astype(F32)
    low, high = coeffs[0] + coeffs[1], coeffs[2] + coeffs[3]
    sum_in = jnp.concatenate([low[:, STATE:], high[:, STATE:]], axis=1)
    sum_out = jnp.concatenate([low[:, :STATE], high[:, :STATE]], axis=1)

    bundle = jnp.concatenate([dweight.reshape(-1, 128).astype(BF16), small.astype(BF16)], axis=0)
    totals = jnp.sum(from_everyone(bundle, SEQ).astype(F32), axis=0)
    rows = KERNEL * COLS // 128
    grad_weight = totals[:rows].reshape(KERNEL, COLS)
    grad_bias, grad_rate, grad_skip = (
        totals[rows + 2 * n, :heads] + totals[rows + 2 * n + 1, :heads] for n in range(3)
    )

    tail = (tail + spilled).astype(BF16)
    grad_conv = lax.dynamic_update_slice_in_dim(dx, tail, T - 8, 0)

    total = own_grad
    for piece in returned:
        total = total + piece.astype(F32)
    grad_keys = (total[:T] * HEAD_DIM ** (-0.5)).astype(BF16)
    grad_values = total[T:].astype(BF16)
    return (
        dq, grad_keys, grad_values, grad_conv, dgate, dstep[:, :heads], sum_in, sum_out,
        grad_weight, grad_bias, grad_rate, grad_skip,
    )


def solution(mesh):
    finer = Mesh(
        mesh.devices.reshape(4, 2, 4, mesh.shape["head"]), ("seq_0", "seq_1", "seq_2", "head")
    )
    wide = P(SEQ, "head")
    return jax.shard_map(
        local,
        mesh=finer,
        in_specs=(
            wide, wide, wide, wide, P(), wide, P(None, "head"), wide, P("head"), P("head"),
            P("head"), P(SEQ, None), P(SEQ, None), wide, wide,
        ),
        out_specs=(
            wide, wide, wide, wide, wide, wide, P(SEQ, None), P(SEQ, None), P(None, "head"),
            P("head"), P("head"), P("head"),
        ),
        check_vma=False,
    )
```

```python
import jax
import jax.numpy as jnp
from jax import lax
from jax.experimental import pallas as pl
from jax.experimental.pallas import tpu as pltpu
from jax.sharding import Mesh
from jax.sharding import PartitionSpec as P

HEAD_DIM = 224
WINDOW = 1024
SSM_HEADS = 112
STATE = 64
GROUPS = 2
KERNEL = 4
SEQ = ("seq_0", "seq_1", "seq_2")
SHARDS = 32
T = 256
LOCAL_HEADS = 4
REACH = WINDOW // T
BLK = 256
HEADS_BLK = BLK // 64
COLS = 1792
STEPS = COLS // BLK
NEG = -1e30
F32 = jnp.float32
BF16 = jnp.bfloat16

NN = (((1,), (0,)), ((), ()))
NT = (((1,), (1,)), ((), ()))
TN = (((0,), (0,)), ((), ()))


def dot(a, b, dims=NN):
    return lax.dot_general(a, b, dims, preferred_element_type=F32)


def exact(a, b, dims=NN):
    return lax.dot_general(
        a, b, dims, preferred_element_type=F32, precision=lax.Precision.HIGHEST
    )


def split(a, pieces):
    parts = []
    for _ in range(pieces):
        part = a.astype(BF16)
        parts.append(part)
        a = a - part.astype(F32)
    return parts


def sigmoid(v):
    return 1.0 / (1.0 + jnp.exp(-v))


def iota(shape, dim):
    return lax.broadcasted_iota(jnp.int32, shape, dim)


def columns_of(row):
    return jnp.transpose(jnp.broadcast_to(row, (T, T)))


def whole(shape):
    return pl.BlockSpec(shape, lambda c: (0,) * len(shape))


def column_block(rows):
    return pl.BlockSpec((rows, BLK), lambda c: (0, c))


IN_SMEM = pl.BlockSpec(memory_space=pltpu.SMEM)
IN_VMEM = pl.BlockSpec(memory_space=pltpu.VMEM)


PARAM_ROWS = 3


def doc_rows(where_ref, docs_ref):
    shard = where_ref[0]
    own = docs_ref[pl.ds(shard, 1), :].astype(F32)
    before = docs_ref[pl.ds(jnp.maximum(shard - 1, 0), 1), :].astype(F32)
    return own, jnp.where(shard == 0, -1.0, before)


def group_halves(where_ref, coeff_ref):
    coeff = coeff_ref[...].astype(F32)
    turned = pltpu.roll(coeff, STATE, 1)
    first = where_ref[1] == 0
    low = iota((T, 128), 1) < STATE
    mine_low = jnp.where(low, jnp.where(first, coeff, turned), 0.0)
    mine_high = jnp.where(low, 0.0, jnp.where(first, turned, coeff))
    return mine_low.astype(BF16), mine_high.astype(BF16)


def padded_params(bias_ref, rate_ref, skip_ref, params_s):
    heads = bias_ref.shape[1]
    params_s[...] = jnp.zeros((8, 128), F32)
    for n, ref in enumerate((bias_ref, rate_ref, skip_ref)):
        params_s[n : n + 1, 0:heads] = ref[...]
    return params_s[...]


def raw_steps(step_ref):
    rows = step_ref.shape[0]
    filled = jnp.concatenate([step_ref[...], jnp.zeros((128 - rows, T), F32)], axis=0)
    return jnp.transpose(filled)


def step_and_decay(raw, params):
    step = jnp.maximum(raw, 0.0) + jnp.log1p(jnp.exp(-jnp.abs(raw)))
    return step, -step * jnp.exp(params[1:2])


def token_setup(where_ref, docs_ref, step_ref, params, cum_s, step_s, mask_s, prev_s, end_s):
    own_row, before_row = doc_rows(where_ref, docs_ref)
    own = columns_of(own_row)
    lane = iota((8, T), 1)
    own8 = jnp.broadcast_to(own_row, (8, T))
    before8 = jnp.broadcast_to(before_row, (8, T))
    for lag in range(1, KERNEL):
        lagged = jnp.where(lane < lag, pltpu.roll(before8, lag, 1), pltpu.roll(own8, lag, 1))
        mask_s[lag - 1] = jnp.where(own == columns_of(lagged[0:1]), 1.0, 0.0)
    prev_s[...] = jnp.where(own == before_row[:, T - 1 : T], 0.0, NEG)
    end_s[...] = jnp.where(own == own_row[:, T - 1 : T], 0.0, NEG)
    raw = raw_steps(step_ref) + params[0:1]
    step, decay = step_and_decay(raw, params)
    lower = jnp.where(iota((T, T), 0) >= iota((T, T), 1), 1.0, 0.0)
    cum = exact(lower, decay)
    for n, part in enumerate(split(cum, 3)):
        cum_s[n] = part
    for n, part in enumerate(split(step, 2)):
        step_s[n] = part
    return own, own_row, cum


def spread_of(step_id):
    head = iota((128, BLK), 0)
    owner = step_id * HEADS_BLK + iota((128, BLK), 1) // 64
    return jnp.where(head == owner, 1.0, 0.0).astype(BF16)


def block_gains(step_id, cum_s, step_s, prev_s, end_s):
    spread = spread_of(step_id)
    cum = dot(cum_s[0], spread) + dot(cum_s[1], spread) + dot(cum_s[2], spread)
    step = dot(step_s[0], spread) + dot(step_s[1], spread)
    enter = jnp.exp(cum + prev_s[...])
    to_end = jnp.exp(cum[T - 1 : T] - cum + end_s[...])
    return spread, cum, step, enter, to_end


def conv_pre(x, halo, weight, mask_s):
    extended = jnp.concatenate([halo.astype(F32), x.astype(F32)], axis=0)
    shifted = [extended[8:]]
    summed = weight[0:1] * shifted[0]
    for lag in range(1, KERNEL):
        moved = pltpu.roll(extended, lag, 0)[8:] * mask_s[lag - 1]
        shifted.append(moved)
        summed = summed + weight[lag : lag + 1] * moved
    return summed, shifted


ROWS = COLS // SHARDS
GROUPS8 = ROWS // 8
SLOT = ROWS + 8


def mixer_first_kernel(
    where_ref, x_ref, halo_ref, weight_ref, gate_ref, grad_ref, step_ref, bias_ref, rate_ref,
    skip_ref, docs_ref, in_ref, out_ref,
    parts_ref,
    cum_s, step_s, mask_s, prev_s, end_s, params_s, state_s, in_s, out_s,
):
    step_id = pl.program_id(0)

    @pl.when(step_id == 0)
    def _():
        params = padded_params(bias_ref, rate_ref, skip_ref, params_s)
        cum = token_setup(
            where_ref, docs_ref, step_ref, params, cum_s, step_s, mask_s, prev_s, end_s
        )[2]
        through = jnp.exp(cum[T - 1 : T] + prev_s[T - 1 : T, 0:1])
        high, low = split(through, 2)
        row = iota((8, 128), 0)
        both = jnp.where(row == 0, high.astype(F32), jnp.where(row == 1, low.astype(F32), 0.0))
        for shard in range(SHARDS):
            state_s[SLOT * shard + ROWS : SLOT * (shard + 1)] = both
        in_s[...] = group_halves(where_ref, in_ref)[0]
        out_s[...] = group_halves(where_ref, out_ref)[1]

    _, _, step, enter, to_end = block_gains(step_id, cum_s, step_s, prev_s, end_s)
    pre, _ = conv_pre(x_ref[...], halo_ref[...], weight_ref[...], mask_s)
    act = pre * sigmoid(pre)
    gate = gate_ref[...].astype(F32)
    out_grad = grad_ref[...].astype(F32) * gate * sigmoid(gate)
    ended = (act * step * to_end).astype(BF16)
    entered = (out_grad * enter).astype(BF16)
    state = dot(ended, in_s[...], TN) + dot(entered, out_s[...], TN)
    for part in range(BLK // 8):
        place = step_id * (BLK // 8) + part
        target = lax.div(place, GROUPS8)
        offset = SLOT * target + 8 * (place - GROUPS8 * target)
        state_s[pl.ds(pl.multiple_of(offset, 8), 8), :] = state[8 * part : 8 * part + 8]

    @pl.when(step_id == STEPS - 1)
    def _():
        parts_ref[...] = state_s[...].astype(BF16)


TOKEN_SCRATCH = [
    pltpu.VMEM((3, T, 128), BF16),
    pltpu.VMEM((2, T, 128), BF16),
    pltpu.VMEM((KERNEL - 1, T, BLK), F32),
    pltpu.VMEM((T, BLK), F32),
    pltpu.VMEM((T, BLK), F32),
    pltpu.VMEM((8, 128), F32),
]


def mixer_specs(heads):
    return [
        IN_SMEM, column_block(T), column_block(8), column_block(KERNEL), column_block(T),
        column_block(T), whole((heads, T)), whole((1, heads)), whole((1, heads)),
        whole((1, heads)), whole((SHARDS, T)), whole((T, 128)), whole((T, 128)),
    ]


def mixer_first(*arrays):
    heads = arrays[6].shape[0]
    return pl.pallas_call(
        mixer_first_kernel,
        grid=(STEPS,),
        in_specs=mixer_specs(heads),
        out_specs=whole((SHARDS * SLOT, 128)),
        out_shape=jax.ShapeDtypeStruct((SHARDS * SLOT, 128), BF16),
        scratch_shapes=TOKEN_SCRATCH + [
            pltpu.VMEM((SHARDS * SLOT, 128), F32),
            pltpu.VMEM((T, 128), BF16),
            pltpu.VMEM((T, 128), BF16),
        ],
        cost_estimate=pl.CostEstimate(flops=8 * 10**9, bytes_accessed=4 * 10**6, transcendentals=0),
        name="mixer_first",
    )(*arrays)


def chain_kernel(where_ref, parts_ref, out_ref, forward_s):
    slot = where_ref[0]
    owner = (slot * ROWS + iota((ROWS, 128), 0)) // 64
    choose = jnp.where(owner == iota((ROWS, 128), 1), 1.0, 0.0)
    lane = iota((ROWS, 128), 1)
    through = []
    carry = jnp.zeros((ROWS, 128), F32)
    for shard in range(SHARDS):
        row = parts_ref[shard, ROWS : ROWS + 1].astype(F32)
        row = row + parts_ref[shard, ROWS + 1 : ROWS + 2].astype(F32)
        gain = jnp.sum(choose * row, axis=1, keepdims=True)
        through.append(gain)
        forward_s[shard] = carry
        carry = gain * carry + parts_ref[shard, 0:ROWS].astype(F32)
    carry = jnp.zeros((ROWS, 128), F32)
    for shard in reversed(range(SHARDS)):
        out_ref[shard] = jnp.where(lane < STATE, forward_s[shard], carry).astype(BF16)
        carry = through[shard] * carry + parts_ref[shard, 0:ROWS].astype(F32)


def chain(where, parts):
    return pl.pallas_call(
        chain_kernel,
        in_specs=[IN_SMEM, IN_VMEM],
        out_specs=IN_VMEM,
        out_shape=jax.ShapeDtypeStruct((SHARDS, ROWS, 128), BF16),
        scratch_shapes=[pltpu.VMEM((SHARDS, ROWS, 128), F32)],
        cost_estimate=pl.CostEstimate(flops=2 * 10**9, bytes_accessed=10**6, transcendentals=0),
        name="chain",
    )(where, parts)


BUNDLE = KERNEL * COLS // 128
LANES_BLK = BLK // 128


def mixer_second_kernel(
    where_ref, x_ref, halo_ref, weight_ref, gate_ref, grad_ref, step_ref, bias_ref, rate_ref,
    skip_ref, docs_ref, in_ref, out_ref, state_ref,
    dx_ref, tail_ref, spill_ref, dgate_ref, dstep_ref, coeff_ref, bundle_ref,
    cum_s, step_s, mask_s, prev_s, end_s, params_s,
    cumt_s, pair_s, causal_s, dpair_s, coeff_s, row_s, dt_s, ends_s, bundle_s,
    in_low_s, in_high_s, out_low_s, out_high_s,
):
    step_id = pl.program_id(0)
    lane = iota((T, 128), 1)

    @pl.when(step_id == 0)
    def _():
        params = padded_params(bias_ref, rate_ref, skip_ref, params_s)
        own, own_row, cum = token_setup(
            where_ref, docs_ref, step_ref, params, cum_s, step_s, mask_s, prev_s, end_s
        )
        cumt_s[...] = jnp.transpose(cum)
        same = (own == own_row) & (iota((T, T), 0) >= iota((T, T), 1))
        causal_s[...] = jnp.where(same, 0.0, NEG)
        in_low_s[...], in_high_s[...] = group_halves(where_ref, in_ref)
        out_low_s[...], out_high_s[...] = group_halves(where_ref, out_ref)
        pair_s[...] = dot(out_low_s[...], in_low_s[...], NT)
        dpair_s[...] = jnp.zeros((T, T), F32)
        coeff_s[...] = jnp.zeros((T, 128), F32)
        row_s[...] = jnp.zeros((T, 128), F32)
        dt_s[...] = jnp.zeros((T, 128), F32)
        ends_s[...] = jnp.zeros((8, 128), F32)

    out_low = out_low_s[...]
    in_high = in_high_s[...]
    spread, cum, step, enter, to_end = block_gains(step_id, cum_s, step_s, prev_s, end_s)
    skip = sum(dot(part, spread) for part in split(params_s[...], 3))[2:3]
    weight = weight_ref[...]
    pre, shifted = conv_pre(x_ref[...], halo_ref[...], weight, mask_s)
    sig = sigmoid(pre)
    act = pre * sig
    gate = gate_ref[...].astype(F32)
    gate_sig = sigmoid(gate)
    mix_grad = grad_ref[...].astype(F32)
    out_grad = mix_grad * gate * gate_sig
    scaled = act * step
    scaled_half = scaled.astype(BF16)
    grad_half = out_grad.astype(BF16)

    block_head = iota((T, BLK), 1) // 64
    inner = jnp.zeros((T, BLK), F32)
    dscaled = jnp.zeros((T, BLK), F32)
    dpair = dpair_s[...]
    for k in range(HEADS_BLK):
        mine = block_head == k
        cum_col = jnp.broadcast_to(cum[:, 64 * k : 64 * k + 1], (T, T))
        cum_row = cumt_s[pl.ds(step_id * HEADS_BLK + k, 1), :]
        weights = jnp.exp(cum_col - cum_row + causal_s[...])
        mixing = (pair_s[...] * weights).astype(BF16)
        scaled_k = jnp.where(mine, scaled_half, jnp.zeros_like(scaled_half))
        grad_k = jnp.where(mine, grad_half, jnp.zeros_like(grad_half))
        inner = inner + dot(mixing, scaled_k)
        dscaled = dscaled + dot(mixing, grad_k, TN)
        dpair = dpair + dot(grad_k, scaled_half, NT) * weights
    dpair_s[...] = dpair

    state = state_ref[...]
    carried = dot(out_low, state, NT) * enter
    from_end = dot(in_high, state, NT) * to_end
    ssm_out = inner + carried
    dscaled = dscaled + from_end
    mixed_out = ssm_out + skip * act
    dgate_ref[...] = (
        mix_grad * mixed_out * gate_sig * (1.0 + gate * (1.0 - gate_sig))
    ).astype(BF16)

    gave_out = dot((out_grad * enter).astype(BF16), state)
    gave_in = dot((scaled * to_end).astype(BF16), state)
    coeff_s[...] += jnp.where(lane < STATE, gave_out, gave_in)

    grad_round = grad_half.astype(F32)
    scaled_round = scaled_half.astype(F32)
    balance = grad_round * ssm_out - scaled_round * dscaled
    row_s[...] += sum(dot(part, spread, NT) for part in split(balance, 3))
    dt_s[...] += sum(dot(part, spread, NT) for part in split(dscaled * act, 2))

    state_wide = state.astype(F32)
    product = state_wide * pltpu.roll(state_wide, STATE, 1)
    through = jnp.sum(jnp.where(iota((BLK, 128), 1) < STATE, product, 0.0), axis=1, keepdims=True)
    through_row = jnp.transpose(jnp.broadcast_to(through, (BLK, BLK)))[0:1]
    end_row = jnp.sum(scaled_round * from_end, axis=0, keepdims=True)
    end_row = end_row + through_row * enter[T - 1 : T]
    skip_row = jnp.sum(out_grad * act, axis=0, keepdims=True)
    row8 = iota((8, BLK), 0)
    both = jnp.where(row8 == 0, end_row, jnp.where(row8 == 1, skip_row, 0.0))
    ends_s[...] += sum(dot(part, spread, NT) for part in split(both, 3))

    dact = step * dscaled + skip * out_grad
    dpre = dact * sig * (1.0 + pre * (1.0 - sig))
    zeros = jnp.zeros((8, BLK), F32)
    dx = weight[0:1] * dpre
    spill = zeros
    for lag in range(KERNEL):
        tap = jnp.sum(dpre * shifted[lag], axis=0, keepdims=True)
        for m in range(LANES_BLK):
            place = lag * (COLS // 128) + step_id * LANES_BLK + m
            bundle_s[pl.ds(place, 1), :] = tap[:, 128 * m : 128 * (m + 1)]
        if lag == 0:
            continue
        masked = dpre * mask_s[lag - 1]
        later = pltpu.roll(jnp.concatenate([masked, zeros], axis=0), T + 8 - lag, 0)[:T]
        dx = dx + weight[lag : lag + 1] * later
        edge = pltpu.roll(jnp.concatenate([zeros, masked[:8]], axis=0), 16 - lag, 0)[:8]
        spill = spill + weight[lag : lag + 1] * edge
    dx_ref[...] = dx.astype(BF16)
    tail_ref[...] = dx[T - 8 :]
    spill_ref[...] = spill

    @pl.when(step_id == STEPS - 1)
    def _():
        params = params_s[...]
        raw = raw_steps(step_ref) + params[0:1]
        rate = jnp.exp(params[1:2])
        decay = step_and_decay(raw, params)[1]
        upper = jnp.where(iota((T, T), 1) >= iota((T, T), 0), 1.0, 0.0)
        ends = ends_s[...]
        ddecay = exact(upper, row_s[...]) + ends[0:1]
        dstep = (dt_s[...] - ddecay * rate) * sigmoid(raw)
        dstep_ref[...] = jnp.transpose(dstep)[: dstep_ref.shape[0]]
        dbias = jnp.sum(dstep, axis=0, keepdims=True)
        drate = jnp.sum(ddecay * decay, axis=0, keepdims=True)
        row = iota((8, 128), 0)
        small = jnp.zeros((8, 128), F32)
        for n, vector in enumerate((dbias, drate, ends[1:2])):
            for m, part in enumerate(split(vector, 2)):
                small = jnp.where(row == 2 * n + m, part.astype(F32), small)
        bundle_s[BUNDLE : BUNDLE + 8] = small
        bundle = bundle_s[...].astype(BF16)
        for shard in range(SHARDS):
            bundle_ref[shard] = bundle
        dpair_half = dpair.astype(BF16)
        total = coeff_s[...] + dot(dpair_half, in_low_s[...])
        total = (total + dot(dpair_half, out_high_s[...], TN)).astype(BF16)
        for peer in range(coeff_ref.shape[0]):
            coeff_ref[peer] = total


def mixer_second(*arrays):
    heads = arrays[6].shape[0]
    half = pltpu.VMEM((T, 128), BF16)
    return pl.pallas_call(
        mixer_second_kernel,
        grid=(STEPS,),
        in_specs=mixer_specs(heads) + [pl.BlockSpec((BLK, 128), lambda c: (c, 0))],
        out_specs=[
            column_block(T), column_block(8), column_block(8), column_block(T),
            whole((heads, T)), whole((LOCAL_HEADS, T, 128)), whole((SHARDS, BUNDLE + 8, 128)),
        ],
        out_shape=[
            jax.ShapeDtypeStruct((T, COLS), BF16),
            jax.ShapeDtypeStruct((8, COLS), F32),
            jax.ShapeDtypeStruct((8, COLS), F32),
            jax.ShapeDtypeStruct((T, COLS), BF16),
            jax.ShapeDtypeStruct((heads, T), F32),
            jax.ShapeDtypeStruct((LOCAL_HEADS, T, 128), BF16),
            jax.ShapeDtypeStruct((SHARDS, BUNDLE + 8, 128), BF16),
        ],
        scratch_shapes=TOKEN_SCRATCH + [
            pltpu.VMEM((128, T), F32),
            pltpu.VMEM((T, T), F32),
            pltpu.VMEM((T, T), F32),
            pltpu.VMEM((T, T), F32),
            pltpu.VMEM((T, 128), F32),
            pltpu.VMEM((T, 128), F32),
            pltpu.VMEM((T, 128), F32),
            pltpu.VMEM((8, 128), F32),
            pltpu.VMEM((BUNDLE + 8, 128), F32),
            half, half, half, half,
        ],
        cost_estimate=pl.CostEstimate(flops=18 * 10**9, bytes_accessed=8 * 10**6, transcendentals=0),
        name="mixer_second",
    )(*arrays)


def finish_kernel(bundle_ref, coeff_ref, weight_ref, bias_ref, rate_ref, skip_ref, in_ref, out_ref):
    total = bundle_ref[0].astype(F32)
    for shard in range(1, SHARDS):
        total = total + bundle_ref[shard].astype(F32)
    tiles = COLS // 128
    for lag in range(KERNEL):
        for m in range(tiles):
            weight_ref[lag : lag + 1, 128 * m : 128 * (m + 1)] = total[
                lag * tiles + m : lag * tiles + m + 1
            ]
    for n, ref in enumerate((bias_ref, rate_ref, skip_ref)):
        row = BUNDLE + 2 * n
        ref[...] = (total[row : row + 1] + total[row + 1 : row + 2])[:, : ref.shape[1]]
    low = coeff_ref[0].astype(F32) + coeff_ref[1].astype(F32)
    high = coeff_ref[2].astype(F32) + coeff_ref[3].astype(F32)
    left = iota((T, 128), 1) < STATE
    out_ref[...] = jnp.where(left, low, pltpu.roll(high, STATE, 1))
    in_ref[...] = jnp.where(left, pltpu.roll(low, STATE, 1), high)


def finish(bundle, coeff, heads):
    small = jax.ShapeDtypeStruct((1, heads), F32)
    wide = jax.ShapeDtypeStruct((T, 128), F32)
    return pl.pallas_call(
        finish_kernel,
        in_specs=[IN_VMEM] * 2,
        out_specs=[IN_VMEM] * 6,
        out_shape=[jax.ShapeDtypeStruct((KERNEL, COLS), F32), small, small, small, wide, wide],
        name="finish",
    )(bundle, coeff)


ROW = 4
K_AT, V_AT, Q_AT, G_AT = (slice(n * HEAD_DIM, (n + 1) * HEAD_DIM) for n in range(4))
KV_AT = slice(0, 2 * HEAD_DIM)


def pack_kernel(k_ref, v_ref, q_ref, g_ref, out_ref):
    for ref, place in ((k_ref, K_AT), (v_ref, V_AT), (q_ref, Q_AT), (g_ref, G_AT)):
        turned = jnp.transpose(ref[...])
        for head in range(LOCAL_HEADS):
            out_ref[head, place] = turned[head * HEAD_DIM : (head + 1) * HEAD_DIM]


def pack(keys, values, queries, grads):
    return pl.pallas_call(
        pack_kernel,
        in_specs=[IN_VMEM] * 4,
        out_specs=IN_VMEM,
        out_shape=jax.ShapeDtypeStruct((LOCAL_HEADS, 4 * HEAD_DIM, T), BF16),
        name="pack",
    )(keys, values, queries, grads)


def attention_kernel(
    where_ref, docs_ref, own_ref, far_ref, dq_ref, dkv_ref, back_ref, far_s
):
    first_block = where_ref[2] * ROW
    later = iota((T, T), 1) > iota((T, T), 0)
    scale = HEAD_DIM ** (-0.5)

    def doc_row(block):
        place = first_block + block
        row = docs_ref[pl.ds(jnp.maximum(place, 0), 1), :].astype(F32)
        return row if block >= 0 else jnp.where(place < 0, -1.0, row)

    rows = {block: doc_row(block) for block in range(-ROW, ROW)}
    for i in range(ROW):
        own_doc = columns_of(rows[i])
        qt, gt = own_ref[i, Q_AT], own_ref[i, G_AT]
        q, g = jnp.transpose(qt), jnp.transpose(gt)

        def part(gap, place):
            block = i - gap
            return own_ref[block, place] if block >= 0 else far_ref[block + ROW, place]

        scores = []
        top = None
        for gap in range(ROW + 1):
            same = own_doc == rows[i - gap]
            if gap == 0:
                same = same & jnp.logical_not(later)
            if gap == ROW:
                same = same & later
            s = jnp.where(same, dot(q, part(gap, K_AT)) * scale, NEG)
            scores.append(s)
            top = s if top is None else jnp.maximum(top, s)
        top = jnp.max(top, axis=1, keepdims=True)
        expos = [jnp.exp(s - top) for s in scores]
        total = jnp.sum(sum(expos), axis=1, keepdims=True)
        inverse = 1.0 / jnp.maximum(total, 1.0)
        probs = [e * inverse for e in expos]
        halves = [p.astype(BF16) for p in probs]
        dprobs = [dot(g, part(gap, V_AT)) for gap in range(ROW + 1)]
        delta = sum(h.astype(F32) * d for h, d in zip(halves, dprobs))
        delta = jnp.sum(delta, axis=1, keepdims=True)
        dq = jnp.zeros((HEAD_DIM, T), F32)
        for gap in range(ROW + 1):
            dscore = (probs[gap] * (dprobs[gap] - delta)).astype(BF16)
            dq = dq + dot(part(gap, K_AT), dscore, NT)
            block = i - gap
            ref, index = (dkv_ref, block) if block >= 0 else (far_s, block + ROW)
            dk, dv = dot(qt, dscore), dot(gt, halves[gap])
            if gap == 0 or (block < 0 and i == 0):
                ref[index, K_AT] = dk
                ref[index, V_AT] = dv
            else:
                ref[index, K_AT] += dk
                ref[index, V_AT] += dv
            if gap == ROW:
                back_ref[index] = far_s[index].astype(BF16)
        dq_ref[i] = (dq * scale).astype(BF16)


def attention(where, docs, own, far):
    pair = (ROW, 2 * HEAD_DIM, T)
    return pl.pallas_call(
        attention_kernel,
        in_specs=[IN_SMEM] + [IN_VMEM] * 3,
        out_specs=[IN_VMEM] * 3,
        out_shape=[
            jax.ShapeDtypeStruct((ROW, HEAD_DIM, T), BF16),
            jax.ShapeDtypeStruct(pair, F32),
            jax.ShapeDtypeStruct(pair, BF16),
        ],
        scratch_shapes=[pltpu.VMEM(pair, F32)],
        cost_estimate=pl.CostEstimate(flops=12 * 10**9, bytes_accessed=8 * 10**6, transcendentals=0),
        name="attention",
    )(where, docs, own, far)


def merge_kernel(dq_ref, dkv_ref, back_ref, out_ref):
    scale = HEAD_DIM ** (-0.5)
    total = dkv_ref[0] + back_ref[0].astype(F32)
    out_ref[0, K_AT] = (total[K_AT] * scale).astype(BF16)
    out_ref[0, V_AT] = total[V_AT].astype(BF16)
    out_ref[0, Q_AT] = dq_ref[0]


def merge(dq, dkv, back):
    def block(rows):
        return pl.BlockSpec((1, rows, T), lambda n: (n, 0, 0))

    return pl.pallas_call(
        merge_kernel,
        grid=(ROW,),
        in_specs=[block(HEAD_DIM), block(2 * HEAD_DIM), block(2 * HEAD_DIM)],
        out_specs=block(3 * HEAD_DIM),
        out_shape=jax.ShapeDtypeStruct((ROW, 3 * HEAD_DIM, T), BF16),
        name="merge",
    )(dq, dkv, back)


def unpack_kernel(parts_ref, dq_ref, dk_ref, dv_ref):
    for ref, place in ((dk_ref, K_AT), (dv_ref, V_AT), (dq_ref, Q_AT)):
        stacked = jnp.concatenate([parts_ref[h, place] for h in range(LOCAL_HEADS)], axis=0)
        ref[...] = jnp.transpose(stacked)


def unpack(parts):
    wide = jax.ShapeDtypeStruct((T, LOCAL_HEADS * HEAD_DIM), BF16)
    return pl.pallas_call(
        unpack_kernel,
        in_specs=[IN_VMEM],
        out_specs=[IN_VMEM] * 3,
        out_shape=[wide] * 3,
        name="unpack",
    )(parts)


def passed_along(value, axis, steps):
    count = lax.axis_size(axis)
    initial, last = (max(0, -steps), min(count, count - steps))
    return lax.ppermute(value, axis, [(source, source + steps) for source in range(initial, last)])


def exchange(array, axis):
    return lax.all_to_all(array, axis, split_axis=0, concat_axis=0, tiled=True)


def local(
    queries, keys, values, attn_grad, doc_ids, conv_input, conv_weight, step_raw, step_bias,
    rate_log, skip_gain, input_coeff, output_coeff, gate_input, mix_grad,
):
    heads = step_raw.shape[1]
    shard = lax.axis_index(SEQ)
    group = lax.axis_index("head") * heads // (SSM_HEADS // GROUPS)
    where = jnp.stack([shard, group, shard // ROW]).astype(jnp.int32)
    docs = doc_ids.reshape(SHARDS, T)
    halo = passed_along(conv_input[T - 8 :], SEQ, 1)

    own = exchange(pack(keys, values, queries, attn_grad), "seq_2")
    far = passed_along(own[:, KV_AT], SEQ, ROW)

    mixer_args = (
        where, conv_input, halo, conv_weight, gate_input, mix_grad, step_raw.T,
        step_bias.reshape(1, heads), rate_log.reshape(1, heads), skip_gain.reshape(1, heads),
        docs, input_coeff, output_coeff,
    )
    parts = mixer_first(*mixer_args).reshape(SHARDS, SLOT, 128)
    entering = exchange(chain(where, exchange(parts, SEQ)), SEQ).reshape(COLS, 128)

    dq, dkv, back = attention(where, docs, own, far)
    returned = passed_along(back, SEQ, -ROW)

    dx, tail, spill, dgate, dstep, coeff, bundle = mixer_second(*mixer_args, entering)
    spilled = passed_along(spill, SEQ, -1)

    dq, dk, dv = unpack(exchange(merge(dq, dkv, returned), "seq_2"))

    grad_weight, grad_bias, grad_rate, grad_skip, sum_in, sum_out = finish(
        exchange(bundle, SEQ), exchange(coeff, "head"), heads
    )
    tail = (tail + spilled).astype(BF16)
    grad_conv = lax.dynamic_update_slice_in_dim(dx, tail, T - 8, 0)
    return (
        dq, dk, dv, grad_conv, dgate, dstep.T, sum_in, sum_out, grad_weight,
        grad_bias.reshape(heads), grad_rate.reshape(heads), grad_skip.reshape(heads),
    )


def solution(mesh):
    finer = Mesh(
        mesh.devices.reshape(4, 2, 4, mesh.shape["head"]), ("seq_0", "seq_1", "seq_2", "head")
    )
    wide = P(SEQ, "head")
    return jax.shard_map(
        local,
        mesh=finer,
        in_specs=(
            wide, wide, wide, wide, P(), wide, P(None, "head"), wide, P("head"), P("head"),
            P("head"), P(SEQ, None), P(SEQ, None), wide, wide,
        ),
        out_specs=(
            wide, wide, wide, wide, wide, wide, P(SEQ, None), P(SEQ, None), P(None, "head"),
            P("head"), P("head"), P("head"),
        ),
        check_vma=False,
    )
```

```python
import jax
import jax.numpy as jnp
from jax import lax
from jax.experimental import pallas as pl
from jax.experimental.pallas import tpu as pltpu
from jax.sharding import Mesh
from jax.sharding import PartitionSpec as P


HEAD_DIM = 224
SSM_HEADS = 112
STATE = 64
GROUPS = 2
KERNEL = 4
SEQ = ("seq_0", "seq_1", "seq_2")
SHARDS = 32
T = 256
LOCAL_HEADS = 4
BLK = 256
HEADS_BLK = BLK // 64
COLS = 1792
STEPS = COLS // BLK
NEG = -1e30
F32 = jnp.float32
BF16 = jnp.bfloat16

NN = (((1,), (0,)), ((), ()))
NT = (((1,), (1,)), ((), ()))
TN = (((0,), (0,)), ((), ()))


def dot(a, b, dims=NN):
    return lax.dot_general(a, b, dims, preferred_element_type=F32)


def exact(a, b, dims=NN):
    return lax.dot_general(
        a, b, dims, preferred_element_type=F32, precision=lax.Precision.HIGHEST
    )


def split(a, pieces):
    parts = []
    for _ in range(pieces):
        part = a.astype(BF16)
        parts.append(part)
        a = a - part.astype(F32)
    return parts


def sigmoid(v):
    return 1.0 / (1.0 + jnp.exp(-v))


def iota(shape, dim):
    return lax.broadcasted_iota(jnp.int32, shape, dim)


def columns_of(row):
    return jnp.transpose(jnp.broadcast_to(row, (T, T)))


def whole(shape):
    return pl.BlockSpec(shape, lambda c: (0,) * len(shape))


def column_block(rows):
    return pl.BlockSpec((rows, BLK), lambda c: (0, c))


IN_SMEM = pl.BlockSpec(memory_space=pltpu.SMEM)
IN_VMEM = pl.BlockSpec(memory_space=pltpu.VMEM)


def doc_rows(where_ref, docs_ref):
    shard = where_ref[0]
    own = docs_ref[pl.ds(shard, 1), :].astype(F32)
    before = docs_ref[pl.ds(jnp.maximum(shard - 1, 0), 1), :].astype(F32)
    return own, jnp.where(shard == 0, -1.0, before)


def group_halves(where_ref, coeff_ref):
    coeff = coeff_ref[...].astype(F32)
    turned = pltpu.roll(coeff, STATE, 1)
    first = where_ref[1] == 0
    low = iota((T, 128), 1) < STATE
    mine_low = jnp.where(low, jnp.where(first, coeff, turned), 0.0)
    mine_high = jnp.where(low, 0.0, jnp.where(first, turned, coeff))
    return mine_low.astype(BF16), mine_high.astype(BF16)


def padded_params(bias_ref, rate_ref, skip_ref, params_s):
    heads = bias_ref.shape[1]
    params_s[...] = jnp.zeros((8, 128), F32)
    for n, ref in enumerate((bias_ref, rate_ref, skip_ref)):
        params_s[n : n + 1, 0:heads] = ref[...]
    return params_s[...]


def raw_steps(step_ref):
    rows = step_ref.shape[0]
    filled = jnp.concatenate([step_ref[...], jnp.zeros((128 - rows, T), F32)], axis=0)
    return jnp.transpose(filled)


def step_and_decay(raw, params):
    step = jnp.maximum(raw, 0.0) + jnp.log1p(jnp.exp(-jnp.abs(raw)))
    return step, -step * jnp.exp(params[1:2])


def token_setup(where_ref, docs_ref, step_ref, params, cum_s, step_s, mask_s, prev_s, end_s):
    own_row, before_row = doc_rows(where_ref, docs_ref)
    own = columns_of(own_row)
    lane = iota((8, T), 1)
    own8 = jnp.broadcast_to(own_row, (8, T))
    before8 = jnp.broadcast_to(before_row, (8, T))
    for lag in range(1, KERNEL):
        lagged = jnp.where(lane < lag, pltpu.roll(before8, lag, 1), pltpu.roll(own8, lag, 1))
        mask_s[lag - 1] = jnp.where(own == columns_of(lagged[0:1]), 1.0, 0.0)
    prev_s[...] = jnp.where(own == before_row[:, T - 1 : T], 0.0, NEG)
    end_s[...] = jnp.where(own == own_row[:, T - 1 : T], 0.0, NEG)
    raw = raw_steps(step_ref) + params[0:1]
    step, decay = step_and_decay(raw, params)
    lower = jnp.where(iota((T, T), 0) >= iota((T, T), 1), 1.0, 0.0)
    cum = exact(lower, decay)
    for n, part in enumerate(split(cum, 3)):
        cum_s[n] = part
    for n, part in enumerate(split(step, 2)):
        step_s[n] = part
    return own, own_row, cum


def spread_of(step_id):
    head = iota((128, BLK), 0)
    owner = step_id * HEADS_BLK + iota((128, BLK), 1) // 64
    return jnp.where(head == owner, 1.0, 0.0).astype(BF16)


def block_gains(step_id, cum_s, step_s, prev_s, end_s):
    spread = spread_of(step_id)
    cum = dot(cum_s[0], spread) + dot(cum_s[1], spread) + dot(cum_s[2], spread)
    step = dot(step_s[0], spread) + dot(step_s[1], spread)
    enter = jnp.exp(cum + prev_s[...])
    to_end = jnp.exp(cum[T - 1 : T] - cum + end_s[...])
    return spread, cum, step, enter, to_end


def conv_pre(x, halo, weight, mask_s):
    extended = jnp.concatenate([halo.astype(F32), x.astype(F32)], axis=0)
    shifted = [extended[8:]]
    summed = weight[0:1] * shifted[0]
    for lag in range(1, KERNEL):
        moved = pltpu.roll(extended, lag, 0)[8:] * mask_s[lag - 1]
        shifted.append(moved)
        summed = summed + weight[lag : lag + 1] * moved
    return summed, shifted


ROWS = COLS // SHARDS
GROUPS8 = ROWS // 8
SLOT = ROWS + 8


def mixer_first_kernel(
    where_ref, x_ref, halo_ref, weight_ref, gate_ref, grad_ref, step_ref, bias_ref, rate_ref,
    skip_ref, docs_ref, in_ref, out_ref,
    parts_ref,
    cum_s, step_s, mask_s, prev_s, end_s, params_s, state_s, in_s, out_s,
):
    step_id = pl.program_id(0)

    @pl.when(step_id == 0)
    def _():
        params = padded_params(bias_ref, rate_ref, skip_ref, params_s)
        cum = token_setup(
            where_ref, docs_ref, step_ref, params, cum_s, step_s, mask_s, prev_s, end_s
        )[2]
        through = jnp.exp(cum[T - 1 : T] + prev_s[T - 1 : T, 0:1])
        high, low = split(through, 2)
        row = iota((8, 128), 0)
        both = jnp.where(row == 0, high.astype(F32), jnp.where(row == 1, low.astype(F32), 0.0))
        for shard in range(SHARDS):
            state_s[SLOT * shard + ROWS : SLOT * (shard + 1)] = both
        in_s[...] = group_halves(where_ref, in_ref)[0]
        out_s[...] = group_halves(where_ref, out_ref)[1]

    _, _, step, enter, to_end = block_gains(step_id, cum_s, step_s, prev_s, end_s)
    pre, _ = conv_pre(x_ref[...], halo_ref[...], weight_ref[...], mask_s)
    act = pre * sigmoid(pre)
    gate = gate_ref[...].astype(F32)
    out_grad = grad_ref[...].astype(F32) * gate * sigmoid(gate)
    ended = (act * step * to_end).astype(BF16)
    entered = (out_grad * enter).astype(BF16)
    state = dot(ended, in_s[...], TN) + dot(entered, out_s[...], TN)
    for part in range(BLK // 8):
        place = step_id * (BLK // 8) + part
        target = lax.div(place, GROUPS8)
        offset = SLOT * target + 8 * (place - GROUPS8 * target)
        state_s[pl.ds(pl.multiple_of(offset, 8), 8), :] = state[8 * part : 8 * part + 8]

    @pl.when(step_id == STEPS - 1)
    def _():
        parts_ref[...] = state_s[...].astype(BF16)


TOKEN_SCRATCH = [
    pltpu.VMEM((3, T, 128), BF16),
    pltpu.VMEM((2, T, 128), BF16),
    pltpu.VMEM((KERNEL - 1, T, BLK), F32),
    pltpu.VMEM((T, BLK), F32),
    pltpu.VMEM((T, BLK), F32),
    pltpu.VMEM((8, 128), F32),
]


def mixer_specs(heads):
    return [
        IN_SMEM, column_block(T), column_block(8), column_block(KERNEL), column_block(T),
        column_block(T), whole((heads, T)), whole((1, heads)), whole((1, heads)),
        whole((1, heads)), whole((SHARDS, T)), whole((T, 128)), whole((T, 128)),
    ]


def mixer_first(*arrays):
    heads = arrays[6].shape[0]
    return pl.pallas_call(
        mixer_first_kernel,
        grid=(STEPS,),
        in_specs=mixer_specs(heads),
        out_specs=whole((SHARDS * SLOT, 128)),
        out_shape=jax.ShapeDtypeStruct((SHARDS * SLOT, 128), BF16),
        scratch_shapes=TOKEN_SCRATCH + [
            pltpu.VMEM((SHARDS * SLOT, 128), F32),
            pltpu.VMEM((T, 128), BF16),
            pltpu.VMEM((T, 128), BF16),
        ],
        cost_estimate=pl.CostEstimate(flops=8 * 10**9, bytes_accessed=4 * 10**6, transcendentals=0),
        name="mixer_first",
    )(*arrays)


def chain_kernel(where_ref, parts_ref, out_ref, forward_s):
    slot = where_ref[0]
    owner = (slot * ROWS + iota((ROWS, 128), 0)) // 64
    choose = jnp.where(owner == iota((ROWS, 128), 1), 1.0, 0.0)
    lane = iota((ROWS, 128), 1)
    through = []
    carry = jnp.zeros((ROWS, 128), F32)
    for shard in range(SHARDS):
        row = parts_ref[shard, ROWS : ROWS + 1].astype(F32)
        row = row + parts_ref[shard, ROWS + 1 : ROWS + 2].astype(F32)
        gain = jnp.sum(choose * row, axis=1, keepdims=True)
        through.append(gain)
        forward_s[shard] = carry
        carry = gain * carry + parts_ref[shard, 0:ROWS].astype(F32)
    carry = jnp.zeros((ROWS, 128), F32)
    for shard in reversed(range(SHARDS)):
        out_ref[shard] = jnp.where(lane < STATE, forward_s[shard], carry).astype(BF16)
        carry = through[shard] * carry + parts_ref[shard, 0:ROWS].astype(F32)


def chain(where, parts):
    return pl.pallas_call(
        chain_kernel,
        in_specs=[IN_SMEM, IN_VMEM],
        out_specs=IN_VMEM,
        out_shape=jax.ShapeDtypeStruct((SHARDS, ROWS, 128), BF16),
        scratch_shapes=[pltpu.VMEM((SHARDS, ROWS, 128), F32)],
        cost_estimate=pl.CostEstimate(flops=2 * 10**9, bytes_accessed=10**6, transcendentals=0),
        name="chain",
    )(where, parts)


BUNDLE = KERNEL * COLS // 128
LANES_BLK = BLK // 128


def mixer_second_kernel(
    where_ref, x_ref, halo_ref, weight_ref, gate_ref, grad_ref, step_ref, bias_ref, rate_ref,
    skip_ref, docs_ref, in_ref, out_ref, state_ref,
    dx_ref, tail_ref, spill_ref, dgate_ref, dstep_ref, coeff_ref, bundle_ref,
    cum_s, step_s, mask_s, prev_s, end_s, params_s,
    cumt_s, pair_s, causal_s, dpair_s, coeff_s, row_s, dt_s, ends_s, bundle_s,
    in_low_s, in_high_s, out_low_s, out_high_s,
):
    step_id = pl.program_id(0)
    lane = iota((T, 128), 1)

    @pl.when(step_id == 0)
    def _():
        params = padded_params(bias_ref, rate_ref, skip_ref, params_s)
        own, own_row, cum = token_setup(
            where_ref, docs_ref, step_ref, params, cum_s, step_s, mask_s, prev_s, end_s
        )
        cumt_s[...] = jnp.transpose(cum)
        same = (own == own_row) & (iota((T, T), 0) >= iota((T, T), 1))
        causal_s[...] = jnp.where(same, 0.0, NEG)
        in_low_s[...], in_high_s[...] = group_halves(where_ref, in_ref)
        out_low_s[...], out_high_s[...] = group_halves(where_ref, out_ref)
        pair_s[...] = dot(out_low_s[...], in_low_s[...], NT)
        dpair_s[...] = jnp.zeros((T, T), F32)
        coeff_s[...] = jnp.zeros((T, 128), F32)
        row_s[...] = jnp.zeros((T, 128), F32)
        dt_s[...] = jnp.zeros((T, 128), F32)
        ends_s[...] = jnp.zeros((8, 128), F32)

    out_low = out_low_s[...]
    in_high = in_high_s[...]
    spread, cum, step, enter, to_end = block_gains(step_id, cum_s, step_s, prev_s, end_s)
    skip = sum(dot(part, spread) for part in split(params_s[...], 3))[2:3]
    weight = weight_ref[...]
    pre, shifted = conv_pre(x_ref[...], halo_ref[...], weight, mask_s)
    sig = sigmoid(pre)
    act = pre * sig
    gate = gate_ref[...].astype(F32)
    gate_sig = sigmoid(gate)
    mix_grad = grad_ref[...].astype(F32)
    out_grad = mix_grad * gate * gate_sig
    scaled = act * step
    scaled_half = scaled.astype(BF16)
    grad_half = out_grad.astype(BF16)

    block_head = iota((T, BLK), 1) // 64
    inner = jnp.zeros((T, BLK), F32)
    dscaled = jnp.zeros((T, BLK), F32)
    dpair = dpair_s[...]
    for k in range(HEADS_BLK):
        mine = block_head == k
        cum_col = jnp.broadcast_to(cum[:, 64 * k : 64 * k + 1], (T, T))
        cum_row = cumt_s[pl.ds(step_id * HEADS_BLK + k, 1), :]
        weights = jnp.exp(cum_col - cum_row + causal_s[...])
        mixing = (pair_s[...] * weights).astype(BF16)
        scaled_k = jnp.where(mine, scaled_half, jnp.zeros_like(scaled_half))
        grad_k = jnp.where(mine, grad_half, jnp.zeros_like(grad_half))
        inner = inner + dot(mixing, scaled_k)
        dscaled = dscaled + dot(mixing, grad_k, TN)
        dpair = dpair + dot(grad_k, scaled_half, NT) * weights
    dpair_s[...] = dpair

    state = state_ref[...]
    carried = dot(out_low, state, NT) * enter
    from_end = dot(in_high, state, NT) * to_end
    ssm_out = inner + carried
    dscaled = dscaled + from_end
    mixed_out = ssm_out + skip * act
    dgate_ref[...] = (
        mix_grad * mixed_out * gate_sig * (1.0 + gate * (1.0 - gate_sig))
    ).astype(BF16)

    gave_out = dot((out_grad * enter).astype(BF16), state)
    gave_in = dot((scaled * to_end).astype(BF16), state)
    coeff_s[...] += jnp.where(lane < STATE, gave_out, gave_in)

    grad_round = grad_half.astype(F32)
    scaled_round = scaled_half.astype(F32)
    balance = grad_round * ssm_out - scaled_round * dscaled
    row_s[...] += sum(dot(part, spread, NT) for part in split(balance, 3))
    dt_s[...] += sum(dot(part, spread, NT) for part in split(dscaled * act, 2))

    state_wide = state.astype(F32)
    product = state_wide * pltpu.roll(state_wide, STATE, 1)
    through = jnp.sum(jnp.where(iota((BLK, 128), 1) < STATE, product, 0.0), axis=1, keepdims=True)
    through_row = jnp.transpose(jnp.broadcast_to(through, (BLK, BLK)))[0:1]
    end_row = jnp.sum(scaled_round * from_end, axis=0, keepdims=True)
    end_row = end_row + through_row * enter[T - 1 : T]
    skip_row = jnp.sum(out_grad * act, axis=0, keepdims=True)
    row8 = iota((8, BLK), 0)
    both = jnp.where(row8 == 0, end_row, jnp.where(row8 == 1, skip_row, 0.0))
    ends_s[...] += sum(dot(part, spread, NT) for part in split(both, 3))

    dact = step * dscaled + skip * out_grad
    dpre = dact * sig * (1.0 + pre * (1.0 - sig))
    zeros = jnp.zeros((8, BLK), F32)
    dx = weight[0:1] * dpre
    spill = zeros
    for lag in range(KERNEL):
        tap = jnp.sum(dpre * shifted[lag], axis=0, keepdims=True)
        for m in range(LANES_BLK):
            place = lag * (COLS // 128) + step_id * LANES_BLK + m
            bundle_s[pl.ds(place, 1), :] = tap[:, 128 * m : 128 * (m + 1)]
        if lag == 0:
            continue
        masked = dpre * mask_s[lag - 1]
        later = pltpu.roll(jnp.concatenate([masked, zeros], axis=0), T + 8 - lag, 0)[:T]
        dx = dx + weight[lag : lag + 1] * later
        edge = pltpu.roll(jnp.concatenate([zeros, masked[:8]], axis=0), 16 - lag, 0)[:8]
        spill = spill + weight[lag : lag + 1] * edge
    dx_ref[...] = dx.astype(BF16)
    tail_ref[...] = dx[T - 8 :]
    spill_ref[...] = spill

    @pl.when(step_id == STEPS - 1)
    def _():
        params = params_s[...]
        raw = raw_steps(step_ref) + params[0:1]
        rate = jnp.exp(params[1:2])
        decay = step_and_decay(raw, params)[1]
        upper = jnp.where(iota((T, T), 1) >= iota((T, T), 0), 1.0, 0.0)
        ends = ends_s[...]
        ddecay = exact(upper, row_s[...]) + ends[0:1]
        dstep = (dt_s[...] - ddecay * rate) * sigmoid(raw)
        dstep_ref[...] = jnp.transpose(dstep)[: dstep_ref.shape[0]]
        dbias = jnp.sum(dstep, axis=0, keepdims=True)
        drate = jnp.sum(ddecay * decay, axis=0, keepdims=True)
        row = iota((8, 128), 0)
        small = jnp.zeros((8, 128), F32)
        for n, vector in enumerate((dbias, drate, ends[1:2])):
            for m, part in enumerate(split(vector, 2)):
                small = jnp.where(row == 2 * n + m, part.astype(F32), small)
        bundle_s[BUNDLE : BUNDLE + 8] = small
        bundle = bundle_s[...].astype(BF16)
        for shard in range(SHARDS):
            bundle_ref[shard] = bundle
        dpair_half = dpair.astype(BF16)
        total = coeff_s[...] + dot(dpair_half, in_low_s[...])
        total = (total + dot(dpair_half, out_high_s[...], TN)).astype(BF16)
        for peer in range(coeff_ref.shape[0]):
            coeff_ref[peer] = total


def mixer_second(*arrays):
    heads = arrays[6].shape[0]
    half = pltpu.VMEM((T, 128), BF16)
    return pl.pallas_call(
        mixer_second_kernel,
        grid=(STEPS,),
        in_specs=mixer_specs(heads) + [pl.BlockSpec((BLK, 128), lambda c: (c, 0))],
        out_specs=[
            column_block(T), column_block(8), column_block(8), column_block(T),
            whole((heads, T)), whole((LOCAL_HEADS, T, 128)), whole((SHARDS, BUNDLE + 8, 128)),
        ],
        out_shape=[
            jax.ShapeDtypeStruct((T, COLS), BF16),
            jax.ShapeDtypeStruct((8, COLS), F32),
            jax.ShapeDtypeStruct((8, COLS), F32),
            jax.ShapeDtypeStruct((T, COLS), BF16),
            jax.ShapeDtypeStruct((heads, T), F32),
            jax.ShapeDtypeStruct((LOCAL_HEADS, T, 128), BF16),
            jax.ShapeDtypeStruct((SHARDS, BUNDLE + 8, 128), BF16),
        ],
        scratch_shapes=TOKEN_SCRATCH + [
            pltpu.VMEM((128, T), F32),
            pltpu.VMEM((T, T), F32),
            pltpu.VMEM((T, T), F32),
            pltpu.VMEM((T, T), F32),
            pltpu.VMEM((T, 128), F32),
            pltpu.VMEM((T, 128), F32),
            pltpu.VMEM((T, 128), F32),
            pltpu.VMEM((8, 128), F32),
            pltpu.VMEM((BUNDLE + 8, 128), F32),
            half, half, half, half,
        ],
        cost_estimate=pl.CostEstimate(flops=18 * 10**9, bytes_accessed=8 * 10**6, transcendentals=0),
        name="mixer_second",
    )(*arrays)


def finish_kernel(bundle_ref, coeff_ref, weight_ref, bias_ref, rate_ref, skip_ref, in_ref, out_ref):
    total = bundle_ref[0].astype(F32)
    for shard in range(1, SHARDS):
        total = total + bundle_ref[shard].astype(F32)
    tiles = COLS // 128
    for lag in range(KERNEL):
        for m in range(tiles):
            weight_ref[lag : lag + 1, 128 * m : 128 * (m + 1)] = total[
                lag * tiles + m : lag * tiles + m + 1
            ]
    for n, ref in enumerate((bias_ref, rate_ref, skip_ref)):
        row = BUNDLE + 2 * n
        ref[...] = (total[row : row + 1] + total[row + 1 : row + 2])[:, : ref.shape[1]]
    low = coeff_ref[0].astype(F32) + coeff_ref[1].astype(F32)
    high = coeff_ref[2].astype(F32) + coeff_ref[3].astype(F32)
    left = iota((T, 128), 1) < STATE
    out_ref[...] = jnp.where(left, low, pltpu.roll(high, STATE, 1))
    in_ref[...] = jnp.where(left, pltpu.roll(low, STATE, 1), high)


def finish(bundle, coeff, heads):
    small = jax.ShapeDtypeStruct((1, heads), F32)
    wide = jax.ShapeDtypeStruct((T, 128), F32)
    return pl.pallas_call(
        finish_kernel,
        in_specs=[IN_VMEM] * 2,
        out_specs=[IN_VMEM] * 6,
        out_shape=[jax.ShapeDtypeStruct((KERNEL, COLS), F32), small, small, small, wide, wide],
        name="finish",
    )(bundle, coeff)


ROW = 4
K_AT, V_AT, Q_AT, G_AT = (slice(n * HEAD_DIM, (n + 1) * HEAD_DIM) for n in range(4))
KV_AT = slice(0, 2 * HEAD_DIM)


def pack_kernel(k_ref, v_ref, q_ref, g_ref, out_ref):
    for ref, place in ((k_ref, K_AT), (v_ref, V_AT), (q_ref, Q_AT), (g_ref, G_AT)):
        turned = jnp.transpose(ref[...])
        for head in range(LOCAL_HEADS):
            out_ref[head, place] = turned[head * HEAD_DIM : (head + 1) * HEAD_DIM]


def pack(keys, values, queries, grads):
    return pl.pallas_call(
        pack_kernel,
        in_specs=[IN_VMEM] * 4,
        out_specs=IN_VMEM,
        out_shape=jax.ShapeDtypeStruct((LOCAL_HEADS, 4 * HEAD_DIM, T), BF16),
        name="pack",
    )(keys, values, queries, grads)


def attention_kernel(
    where_ref, docs_ref, own_ref, far_ref, dq_ref, dkv_ref, back_ref, far_s
):
    first_block = where_ref[2] * ROW
    later = iota((T, T), 1) > iota((T, T), 0)
    scale = HEAD_DIM ** (-0.5)

    def doc_row(block):
        place = first_block + block
        row = docs_ref[pl.ds(jnp.maximum(place, 0), 1), :].astype(F32)
        return row if block >= 0 else jnp.where(place < 0, -1.0, row)

    rows = {block: doc_row(block) for block in range(-ROW, ROW)}
    for i in range(ROW):
        own_doc = columns_of(rows[i])
        qt, gt = own_ref[i, Q_AT], own_ref[i, G_AT]
        q, g = jnp.transpose(qt), jnp.transpose(gt)

        def part(gap, place):
            block = i - gap
            return own_ref[block, place] if block >= 0 else far_ref[block + ROW, place]

        scores = []
        top = None
        for gap in range(ROW + 1):
            same = own_doc == rows[i - gap]
            if gap == 0:
                same = same & jnp.logical_not(later)
            if gap == ROW:
                same = same & later
            s = jnp.where(same, dot(q, part(gap, K_AT)) * scale, NEG)
            scores.append(s)
            top = s if top is None else jnp.maximum(top, s)
        top = jnp.max(top, axis=1, keepdims=True)
        expos = [jnp.exp(s - top) for s in scores]
        total = jnp.sum(sum(expos), axis=1, keepdims=True)
        inverse = 1.0 / jnp.maximum(total, 1.0)
        probs = [e * inverse for e in expos]
        halves = [p.astype(BF16) for p in probs]
        dprobs = [dot(g, part(gap, V_AT)) for gap in range(ROW + 1)]
        delta = sum(h.astype(F32) * d for h, d in zip(halves, dprobs))
        delta = jnp.sum(delta, axis=1, keepdims=True)
        dq = jnp.zeros((HEAD_DIM, T), F32)
        for gap in range(ROW + 1):
            dscore = (probs[gap] * (dprobs[gap] - delta)).astype(BF16)
            dq = dq + dot(part(gap, K_AT), dscore, NT)
            block = i - gap
            ref, index = (dkv_ref, block) if block >= 0 else (far_s, block + ROW)
            dk, dv = dot(qt, dscore), dot(gt, halves[gap])
            if gap == 0 or (block < 0 and i == 0):
                ref[index, K_AT] = dk
                ref[index, V_AT] = dv
            else:
                ref[index, K_AT] += dk
                ref[index, V_AT] += dv
            if gap == ROW:
                back_ref[index] = far_s[index].astype(BF16)
        dq_ref[i] = (dq * scale).astype(BF16)


def attention(where, docs, own, far):
    pair = (ROW, 2 * HEAD_DIM, T)
    return pl.pallas_call(
        attention_kernel,
        in_specs=[IN_SMEM] + [IN_VMEM] * 3,
        out_specs=[IN_VMEM] * 3,
        out_shape=[
            jax.ShapeDtypeStruct((ROW, HEAD_DIM, T), BF16),
            jax.ShapeDtypeStruct(pair, F32),
            jax.ShapeDtypeStruct(pair, BF16),
        ],
        scratch_shapes=[pltpu.VMEM(pair, F32)],
        cost_estimate=pl.CostEstimate(flops=12 * 10**9, bytes_accessed=8 * 10**6, transcendentals=0),
        name="attention",
    )(where, docs, own, far)


def merge_kernel(where_ref, dq_ref, dkv_ref, back_ref, *out_refs):
    scale = HEAD_DIM ** (-0.5)
    place = where_ref[3]
    for turn, out_ref in enumerate(out_refs):
        block = lax.rem(place + turn, ROW)
        total = dkv_ref[block] + back_ref[block].astype(F32)
        out_ref[K_AT] = (total[K_AT] * scale).astype(BF16)
        out_ref[V_AT] = total[V_AT].astype(BF16)
        out_ref[Q_AT] = dq_ref[block]


def merge(where, dq, dkv, back):
    return pl.pallas_call(
        merge_kernel,
        in_specs=[IN_SMEM] + [IN_VMEM] * 3,
        out_specs=[IN_VMEM] * ROW,
        out_shape=[jax.ShapeDtypeStruct((3 * HEAD_DIM, T), BF16)] * ROW,
        cost_estimate=pl.CostEstimate(flops=3 * 10**9, bytes_accessed=4 * 10**6, transcendentals=0),
        name="merge",
    )(where, dq, dkv, back)


def unpack_kernel(where_ref, *refs):
    parts, outs, stacked_s = refs[:ROW], refs[ROW : ROW + 3], refs[ROW + 3]
    place = where_ref[3]
    for turn, part in enumerate(parts):
        source = lax.rem(place - turn + ROW, ROW)
        for n, at in enumerate((Q_AT, K_AT, V_AT)):
            stacked_s[n, source] = part[at]
    for n, ref in enumerate(outs):
        stacked = jnp.concatenate([stacked_s[n, h] for h in range(LOCAL_HEADS)], axis=0)
        ref[...] = jnp.transpose(stacked)


def unpack(where, parts):
    wide = jax.ShapeDtypeStruct((T, LOCAL_HEADS * HEAD_DIM), BF16)
    return pl.pallas_call(
        unpack_kernel,
        in_specs=[IN_SMEM] + [IN_VMEM] * ROW,
        out_specs=[IN_VMEM] * 3,
        out_shape=[wide] * 3,
        scratch_shapes=[pltpu.VMEM((3, LOCAL_HEADS, HEAD_DIM, T), BF16)],
        name="unpack",
    )(where, *parts)


def passed_along(value, axis, steps):
    count = lax.axis_size(axis)
    initial, last = (max(0, -steps), min(count, count - steps))
    return lax.ppermute(value, axis, [(source, source + steps) for source in range(initial, last)])


def turned(value, axis, steps):
    count = lax.axis_size(axis)
    return lax.ppermute(value, axis, [(n, (n + steps) % count) for n in range(count)])


def exchange(array, axis):
    return lax.all_to_all(array, axis, split_axis=0, concat_axis=0, tiled=True)


def local(
    queries, keys, values, attn_grad, doc_ids, conv_input, conv_weight, step_raw, step_bias,
    rate_log, skip_gain, input_coeff, output_coeff, gate_input, mix_grad,
):
    heads = step_raw.shape[1]
    shard = lax.axis_index(SEQ)
    group = lax.axis_index("head") * heads // (SSM_HEADS // GROUPS)
    where = jnp.stack([shard, group, shard // ROW, lax.axis_index("seq_2")]).astype(jnp.int32)
    docs = doc_ids.reshape(SHARDS, T)
    halo = passed_along(conv_input[T - 8 :], SEQ, 1)
    packed = pack(keys, values, queries, attn_grad)
    own = exchange(packed, "seq_2")
    borrowed = own[:, KV_AT]
    far = passed_along(borrowed, SEQ, ROW)

    mixer_args = (
        where, conv_input, halo, conv_weight, gate_input, mix_grad, step_raw.T,
        step_bias.reshape(1, heads), rate_log.reshape(1, heads), skip_gain.reshape(1, heads),
        docs, input_coeff, output_coeff,
    )
    parts = mixer_first(*mixer_args).reshape(SHARDS, SLOT, 128)
    gathered = exchange(parts, SEQ)
    scanned = chain(where, gathered)
    entering = exchange(scanned, SEQ).reshape(COLS, 128)
    dq, dkv, back = attention(where, docs, own, far)
    returned = passed_along(back, SEQ, -ROW)
    dx, tail, spill, dgate, dstep, coeff, bundle = mixer_second(*mixer_args, entering)
    spilled = passed_along(spill, SEQ, -1)
    bundles = exchange(bundle, SEQ)
    coeffs = exchange(coeff, "head")
    kept, *leaving = merge(where, dq, dkv, returned)
    swapped = [kept] + [turned(part, "seq_2", n) for n, part in enumerate(leaving, 1)]
    grad_weight, grad_bias, grad_rate, grad_skip, sum_in, sum_out = finish(bundles, coeffs, heads)
    dq, dk, dv = unpack(where, swapped)
    tail = (tail + spilled).astype(BF16)
    grad_conv = lax.dynamic_update_slice_in_dim(dx, tail, T - 8, 0)
    return (
        dq, dk, dv, grad_conv, dgate, dstep.T, sum_in, sum_out, grad_weight,
        grad_bias.reshape(heads), grad_rate.reshape(heads), grad_skip.reshape(heads),
    )


def solution(mesh):
    finer = Mesh(
        mesh.devices.reshape(4, 2, 4, mesh.shape["head"]), ("seq_0", "seq_1", "seq_2", "head")
    )
    wide = P(SEQ, "head")
    return jax.shard_map(
        local,
        mesh=finer,
        in_specs=(
            wide, wide, wide, wide, P(), wide, P(None, "head"), wide, P("head"), P("head"),
            P("head"), P(SEQ, None), P(SEQ, None), wide, wide,
        ),
        out_specs=(
            wide, wide, wide, wide, wide, wide, P(SEQ, None), P(SEQ, None), P(None, "head"),
            P("head"), P("head"), P("head"),
        ),
        check_vma=False,
    )
```

```python
import jax
import jax.numpy as jnp
from jax import lax
from jax.experimental import pallas as pl
from jax.experimental.pallas import tpu as pltpu
from jax.sharding import Mesh
from jax.sharding import PartitionSpec as P


HEAD_DIM = 224
SSM_HEADS = 112
STATE = 64
GROUPS = 2
KERNEL = 4
SEQ = ("seq_0", "seq_1", "seq_2")
SHARDS = 32
T = 256
LOCAL_HEADS = 4
BLK = 256
HALF = T // 2
HEADS_BLK = BLK // 64
COLS = 1792
STEPS = COLS // BLK
NEG = -1e30
LOG2E = 1.4426950408889634
F32 = jnp.float32
BF16 = jnp.bfloat16

NN = (((1,), (0,)), ((), ()))
NT = (((1,), (1,)), ((), ()))
TN = (((0,), (0,)), ((), ()))


def dot(a, b, dims=NN):
    return lax.dot_general(a, b, dims, preferred_element_type=F32)


def exact(a, b, dims=NN):
    return lax.dot_general(
        a, b, dims, preferred_element_type=F32, precision=lax.Precision.HIGHEST
    )


def split(a, pieces):
    parts = []
    for _ in range(pieces):
        part = a.astype(BF16)
        parts.append(part)
        a = a - part.astype(F32)
    return parts


def sigmoid(v):
    return 0.5 + 0.5 * jnp.tanh(0.5 * v)


def iota(shape, dim):
    return lax.broadcasted_iota(jnp.int32, shape, dim)


def columns_of(row):
    return jnp.transpose(jnp.broadcast_to(row, (T, T)))


def whole(shape):
    return pl.BlockSpec(shape, lambda c: (0,) * len(shape))


def column_block(rows):
    return pl.BlockSpec((rows, BLK), lambda c: (0, c))


IN_SMEM = pl.BlockSpec(memory_space=pltpu.SMEM)
IN_VMEM = pl.BlockSpec(memory_space=pltpu.VMEM)


def doc_rows(where_ref, docs_ref):
    shard = where_ref[0]
    own = docs_ref[pl.ds(shard, 1), :].astype(F32)
    before = docs_ref[pl.ds(jnp.maximum(shard - 1, 0), 1), :].astype(F32)
    return own, jnp.where(shard == 0, -1.0, before)


def group_halves(where_ref, coeff_ref):
    coeff = coeff_ref[...].astype(F32)
    turned = pltpu.roll(coeff, STATE, 1)
    first = where_ref[1] == 0
    low = iota((T, 128), 1) < STATE
    mine_low = jnp.where(low, jnp.where(first, coeff, turned), 0.0)
    mine_high = jnp.where(low, 0.0, jnp.where(first, turned, coeff))
    return mine_low.astype(BF16), mine_high.astype(BF16)


def padded_params(bias_ref, rate_ref, skip_ref, params_s):
    heads = bias_ref.shape[1]
    params_s[...] = jnp.zeros((8, 128), F32)
    for n, ref in enumerate((bias_ref, rate_ref, skip_ref)):
        params_s[n : n + 1, 0:heads] = ref[...]
    return params_s[...]


def raw_steps(step_ref):
    rows = step_ref.shape[0]
    filled = jnp.concatenate([step_ref[...], jnp.zeros((128 - rows, T), F32)], axis=0)
    return jnp.transpose(filled)


def step_and_decay(raw, params):
    step = jnp.maximum(raw, 0.0) + jnp.log1p(jnp.exp(-jnp.abs(raw)))
    return step, -step * jnp.exp(params[1:2])


def token_setup(where_ref, docs_ref, step_ref, params, cum_s, step_s, mask_s, prev_s, end_s):
    own_row, before_row = doc_rows(where_ref, docs_ref)
    own = columns_of(own_row)
    lane = iota((8, T), 1)
    own8 = jnp.broadcast_to(own_row, (8, T))
    before8 = jnp.broadcast_to(before_row, (8, T))
    for lag in range(1, KERNEL):
        lagged = jnp.where(lane < lag, pltpu.roll(before8, lag, 1), pltpu.roll(own8, lag, 1))
        mask_s[lag - 1] = jnp.where(own == columns_of(lagged[0:1]), 1.0, 0.0)
    prev_s[...] = jnp.where(own == before_row[:, T - 1 : T], 0.0, NEG)
    end_s[...] = jnp.where(own == own_row[:, T - 1 : T], 0.0, NEG)
    raw = raw_steps(step_ref) + params[0:1]
    step, decay = step_and_decay(raw, params)
    lower = jnp.where(iota((T, T), 0) >= iota((T, T), 1), 1.0, 0.0)
    cum = exact(lower, decay) * LOG2E
    for n, part in enumerate(split(cum, 3)):
        cum_s[n] = part
    for n, part in enumerate(split(step, 2)):
        step_s[n] = part
    return own, own_row, cum


def spread_of(step_id):
    head = iota((128, BLK), 0)
    owner = step_id * HEADS_BLK + iota((128, BLK), 1) // 64
    return jnp.where(head == owner, 1.0, 0.0).astype(BF16)


def block_gains(step_id, cum_s, step_s, prev_s, end_s):
    spread = spread_of(step_id)
    cum = dot(cum_s[0], spread) + dot(cum_s[1], spread) + dot(cum_s[2], spread)
    step = dot(step_s[0], spread) + dot(step_s[1], spread)
    enter = jnp.exp2(cum + prev_s[...])
    to_end = jnp.exp2(cum[T - 1 : T] - cum + end_s[...])
    return spread, cum, step, enter, to_end


def conv_pre(x, halo, weight, mask_s):
    extended = jnp.concatenate([halo.astype(F32), x.astype(F32)], axis=0)
    shifted = [extended[8:]]
    summed = weight[0:1] * shifted[0]
    for lag in range(1, KERNEL):
        moved = pltpu.roll(extended, lag, 0)[8:] * mask_s[lag - 1]
        shifted.append(moved)
        summed = summed + weight[lag : lag + 1] * moved
    return summed, shifted


ROWS = COLS // SHARDS
GROUPS8 = ROWS // 8
SLOT = ROWS + 8


def mixer_first_kernel(
    where_ref, x_ref, halo_ref, weight_ref, gate_ref, grad_ref, step_ref, bias_ref, rate_ref,
    skip_ref, docs_ref, in_ref, out_ref,
    parts_ref,
    cum_s, step_s, mask_s, prev_s, end_s, params_s, state_s, in_s, out_s,
):
    step_id = pl.program_id(0)

    @pl.when(step_id == 0)
    def _():
        params = padded_params(bias_ref, rate_ref, skip_ref, params_s)
        cum = token_setup(
            where_ref, docs_ref, step_ref, params, cum_s, step_s, mask_s, prev_s, end_s
        )[2]
        through = jnp.exp2(cum[T - 1 : T] + prev_s[T - 1 : T, 0:1])
        high, low = split(through, 2)
        row = iota((8, 128), 0)
        both = jnp.where(row == 0, high.astype(F32), jnp.where(row == 1, low.astype(F32), 0.0))
        for shard in range(SHARDS):
            state_s[SLOT * shard + ROWS : SLOT * (shard + 1)] = both
        in_s[...] = group_halves(where_ref, in_ref)[0]
        out_s[...] = group_halves(where_ref, out_ref)[1]

    _, _, step, enter, to_end = block_gains(step_id, cum_s, step_s, prev_s, end_s)
    pre, _ = conv_pre(x_ref[...], halo_ref[...], weight_ref[...], mask_s)
    act = pre * sigmoid(pre)
    gate = gate_ref[...].astype(F32)
    out_grad = grad_ref[...].astype(F32) * gate * sigmoid(gate)
    ended = (act * step * to_end).astype(BF16)
    entered = (out_grad * enter).astype(BF16)
    state = dot(ended, in_s[...], TN) + dot(entered, out_s[...], TN)
    for part in range(BLK // 8):
        place = step_id * (BLK // 8) + part
        target = lax.div(place, GROUPS8)
        offset = SLOT * target + 8 * (place - GROUPS8 * target)
        state_s[pl.ds(pl.multiple_of(offset, 8), 8), :] = state[8 * part : 8 * part + 8]

    @pl.when(step_id == STEPS - 1)
    def _():
        parts_ref[...] = state_s[...].astype(BF16)


TOKEN_SCRATCH = [
    pltpu.VMEM((3, T, 128), BF16),
    pltpu.VMEM((2, T, 128), BF16),
    pltpu.VMEM((KERNEL - 1, T, BLK), F32),
    pltpu.VMEM((T, BLK), F32),
    pltpu.VMEM((T, BLK), F32),
    pltpu.VMEM((8, 128), F32),
]


def mixer_specs(heads):
    return [
        IN_SMEM, column_block(T), column_block(8), column_block(KERNEL), column_block(T),
        column_block(T), whole((heads, T)), whole((1, heads)), whole((1, heads)),
        whole((1, heads)), whole((SHARDS, T)), whole((T, 128)), whole((T, 128)),
    ]


def mixer_first(*arrays):
    heads = arrays[6].shape[0]
    return pl.pallas_call(
        mixer_first_kernel,
        grid=(STEPS,),
        in_specs=mixer_specs(heads),
        out_specs=whole((SHARDS * SLOT, 128)),
        out_shape=jax.ShapeDtypeStruct((SHARDS * SLOT, 128), BF16),
        scratch_shapes=TOKEN_SCRATCH + [
            pltpu.VMEM((SHARDS * SLOT, 128), F32),
            pltpu.VMEM((T, 128), BF16),
            pltpu.VMEM((T, 128), BF16),
        ],
        cost_estimate=pl.CostEstimate(flops=8 * 10**9, bytes_accessed=4 * 10**6, transcendentals=0),
        name="mixer_first",
    )(*arrays)


def chain_kernel(where_ref, parts_ref, out_ref, forward_s):
    slot = where_ref[0]
    owner = (slot * ROWS + iota((ROWS, 128), 0)) // 64
    choose = jnp.where(owner == iota((ROWS, 128), 1), 1.0, 0.0)
    lane = iota((ROWS, 128), 1)
    through = []
    carry = jnp.zeros((ROWS, 128), F32)
    for shard in range(SHARDS):
        row = parts_ref[shard, ROWS : ROWS + 1].astype(F32)
        row = row + parts_ref[shard, ROWS + 1 : ROWS + 2].astype(F32)
        gain = jnp.sum(choose * row, axis=1, keepdims=True)
        through.append(gain)
        forward_s[shard] = carry
        carry = gain * carry + parts_ref[shard, 0:ROWS].astype(F32)
    carry = jnp.zeros((ROWS, 128), F32)
    for shard in reversed(range(SHARDS)):
        out_ref[shard] = jnp.where(lane < STATE, forward_s[shard], carry).astype(BF16)
        carry = through[shard] * carry + parts_ref[shard, 0:ROWS].astype(F32)


def chain(where, parts):
    return pl.pallas_call(
        chain_kernel,
        in_specs=[IN_SMEM, IN_VMEM],
        out_specs=IN_VMEM,
        out_shape=jax.ShapeDtypeStruct((SHARDS, ROWS, 128), BF16),
        scratch_shapes=[pltpu.VMEM((SHARDS, ROWS, 128), F32)],
        cost_estimate=pl.CostEstimate(flops=2 * 10**9, bytes_accessed=10**6, transcendentals=0),
        name="chain",
    )(where, parts)


BUNDLE = KERNEL * COLS // 128
LANES_BLK = BLK // 128


def mixer_second_kernel(
    where_ref, x_ref, halo_ref, weight_ref, gate_ref, grad_ref, step_ref, bias_ref, rate_ref,
    skip_ref, docs_ref, in_ref, out_ref, state_ref,
    dx_ref, tail_ref, spill_ref, dgate_ref, dstep_ref, coeff_ref, bundle_ref,
    cum_s, step_s, mask_s, prev_s, end_s, params_s,
    cumt_s, pair_s, causal_s, dtop_s, dbottom_s, coeff_s, row_s, dt_s, ends_s, bundle_s,
    in_low_s, in_high_s, out_low_s, out_high_s,
):
    step_id = pl.program_id(0)
    lane = iota((T, 128), 1)

    @pl.when(step_id == 0)
    def _():
        params = padded_params(bias_ref, rate_ref, skip_ref, params_s)
        own, own_row, cum = token_setup(
            where_ref, docs_ref, step_ref, params, cum_s, step_s, mask_s, prev_s, end_s
        )
        cumt_s[...] = jnp.transpose(cum)
        same = (own == own_row) & (iota((T, T), 0) >= iota((T, T), 1))
        causal_s[...] = jnp.where(same, 0.0, NEG)
        in_low_s[...], in_high_s[...] = group_halves(where_ref, in_ref)
        out_low_s[...], out_high_s[...] = group_halves(where_ref, out_ref)
        pair_s[...] = dot(out_low_s[...], in_low_s[...], NT)
        dtop_s[...] = jnp.zeros((HALF, HALF), F32)
        dbottom_s[...] = jnp.zeros((HALF, T), F32)
        coeff_s[...] = jnp.zeros((T, 128), F32)
        row_s[...] = jnp.zeros((T, 128), F32)
        dt_s[...] = jnp.zeros((T, 128), F32)
        ends_s[...] = jnp.zeros((8, 128), F32)

    out_low = out_low_s[...]
    in_high = in_high_s[...]
    spread, cum, step, enter, to_end = block_gains(step_id, cum_s, step_s, prev_s, end_s)
    skip = sum(dot(part, spread) for part in split(params_s[...], 3))[2:3]
    weight = weight_ref[...]
    pre, shifted = conv_pre(x_ref[...], halo_ref[...], weight, mask_s)
    sig = sigmoid(pre)
    act = pre * sig
    gate = gate_ref[...].astype(F32)
    gate_sig = sigmoid(gate)
    mix_grad = grad_ref[...].astype(F32)
    out_grad = mix_grad * gate * gate_sig
    scaled = act * step
    scaled_half = scaled.astype(BF16)
    grad_half = out_grad.astype(BF16)

    block_head = iota((T, BLK), 1) // 64
    tops, bottoms, scaled_parts, grad_parts = [], [], [], []
    dtop, dbottom = dtop_s[...], dbottom_s[...]
    for k in range(HEADS_BLK):
        mine = block_head == k
        cum_col = cum[:, 64 * k : 64 * k + 1]
        cum_row = cumt_s[pl.ds(step_id * HEADS_BLK + k, 1), :]
        top = jnp.exp2(
            jnp.broadcast_to(cum_col[:HALF], (HALF, HALF)) - cum_row[:, :HALF]
            + causal_s[:HALF, :HALF]
        )
        bottom = jnp.exp2(
            jnp.broadcast_to(cum_col[HALF:], (HALF, T)) - cum_row + causal_s[HALF:, :]
        )
        tops.append((pair_s[:HALF, :HALF] * top).astype(BF16))
        bottoms.append((pair_s[HALF:, :] * bottom).astype(BF16))
        scaled_k = jnp.where(mine, scaled_half, jnp.zeros_like(scaled_half))
        grad_k = jnp.where(mine, grad_half, jnp.zeros_like(grad_half))
        scaled_parts.append(scaled_k)
        grad_parts.append(grad_k)
        dtop = dtop + dot(grad_k[:HALF], scaled_half[:HALF], NT) * top
        dbottom = dbottom + dot(grad_k[HALF:], scaled_half, NT) * bottom
    dtop_s[...] = dtop
    dbottom_s[...] = dbottom
    join = jnp.concatenate
    inner = join(
        [
            dot(join(tops, axis=1), join([v[:HALF] for v in scaled_parts], axis=0)),
            dot(join(bottoms, axis=1), join(scaled_parts, axis=0)),
        ],
        axis=0,
    )
    upper_part = dot(join(tops, axis=0), join([v[:HALF] for v in grad_parts], axis=0), TN)
    dscaled = dot(join(bottoms, axis=0), join([v[HALF:] for v in grad_parts], axis=0), TN)
    dscaled = join([dscaled[:HALF] + upper_part, dscaled[HALF:]], axis=0)

    state = state_ref[...]
    carried = dot(out_low, state, NT) * enter
    from_end = dot(in_high, state, NT) * to_end
    ssm_out = inner + carried
    dscaled = dscaled + from_end
    mixed_out = ssm_out + skip * act
    dgate_ref[...] = (
        mix_grad * mixed_out * gate_sig * (1.0 + gate * (1.0 - gate_sig))
    ).astype(BF16)

    gave_out = dot((out_grad * enter).astype(BF16), state)
    gave_in = dot((scaled * to_end).astype(BF16), state)
    coeff_s[...] += jnp.where(lane < STATE, gave_out, gave_in)

    grad_round = grad_half.astype(F32)
    scaled_round = scaled_half.astype(F32)
    balance = grad_round * ssm_out - scaled_round * dscaled
    row_s[...] += sum(dot(part, spread, NT) for part in split(balance, 2))
    dt_s[...] += dot((dscaled * act).astype(BF16), spread, NT)

    state_wide = state.astype(F32)
    product = state_wide * pltpu.roll(state_wide, STATE, 1)
    through = jnp.sum(jnp.where(iota((BLK, 128), 1) < STATE, product, 0.0), axis=1, keepdims=True)
    through_row = jnp.transpose(jnp.broadcast_to(through, (BLK, BLK)))[0:1]
    end_row = jnp.sum(scaled_round * from_end, axis=0, keepdims=True)
    end_row = end_row + through_row * enter[T - 1 : T]
    skip_row = jnp.sum(out_grad * act, axis=0, keepdims=True)
    row8 = iota((8, BLK), 0)
    both = jnp.where(row8 == 0, end_row, jnp.where(row8 == 1, skip_row, 0.0))
    ends_s[...] += sum(dot(part, spread, NT) for part in split(both, 3))

    dact = step * dscaled + skip * out_grad
    dpre = dact * sig * (1.0 + pre * (1.0 - sig))
    zeros = jnp.zeros((8, BLK), F32)
    dx = weight[0:1] * dpre
    spill = zeros
    for lag in range(KERNEL):
        tap = jnp.sum(dpre * shifted[lag], axis=0, keepdims=True)
        for m in range(LANES_BLK):
            place = lag * (COLS // 128) + step_id * LANES_BLK + m
            bundle_s[pl.ds(place, 1), :] = tap[:, 128 * m : 128 * (m + 1)]
        if lag == 0:
            continue
        masked = dpre * mask_s[lag - 1]
        later = pltpu.roll(jnp.concatenate([masked, zeros], axis=0), T + 8 - lag, 0)[:T]
        dx = dx + weight[lag : lag + 1] * later
        edge = pltpu.roll(jnp.concatenate([zeros, masked[:8]], axis=0), 16 - lag, 0)[:8]
        spill = spill + weight[lag : lag + 1] * edge
    dx_ref[...] = dx.astype(BF16)
    tail_ref[...] = dx[T - 8 :]
    spill_ref[...] = spill

    @pl.when(step_id == STEPS - 1)
    def _():
        params = params_s[...]
        raw = raw_steps(step_ref) + params[0:1]
        rate = jnp.exp(params[1:2])
        decay = step_and_decay(raw, params)[1]
        upper = jnp.where(iota((T, T), 1) >= iota((T, T), 0), 1.0, 0.0)
        ends = ends_s[...]
        ddecay = exact(upper, row_s[...]) + ends[0:1]
        dstep = (dt_s[...] - ddecay * rate) * sigmoid(raw)
        dstep_ref[...] = jnp.transpose(dstep)[: dstep_ref.shape[0]]
        dbias = jnp.sum(dstep, axis=0, keepdims=True)
        drate = jnp.sum(ddecay * decay, axis=0, keepdims=True)
        row = iota((8, 128), 0)
        small = jnp.zeros((8, 128), F32)
        for n, vector in enumerate((dbias, drate, ends[1:2])):
            for m, part in enumerate(split(vector, 2)):
                small = jnp.where(row == 2 * n + m, part.astype(F32), small)
        bundle_s[BUNDLE : BUNDLE + 8] = small
        bundle = bundle_s[...].astype(BF16)
        for shard in range(SHARDS):
            bundle_ref[shard] = bundle
        top_half, bottom_half = dtop.astype(BF16), dbottom.astype(BF16)
        in_low, out_high = in_low_s[...], out_high_s[...]
        out_part = join([dot(top_half, in_low[:HALF]), dot(bottom_half, in_low)], axis=0)
        in_part = dot(bottom_half, out_high[HALF:], TN)
        in_part = join(
            [in_part[:HALF] + dot(top_half, out_high[:HALF], TN), in_part[HALF:]], axis=0
        )
        coeff_ref[...] = (coeff_s[...] + out_part + in_part).astype(BF16)


def mixer_second(*arrays):
    heads = arrays[6].shape[0]
    half = pltpu.VMEM((T, 128), BF16)
    return pl.pallas_call(
        mixer_second_kernel,
        grid=(STEPS,),
        in_specs=mixer_specs(heads) + [pl.BlockSpec((BLK, 128), lambda c: (c, 0))],
        out_specs=[
            column_block(T), column_block(8), column_block(8), column_block(T),
            whole((heads, T)), whole((T, 128)), whole((SHARDS, BUNDLE + 8, 128)),
        ],
        out_shape=[
            jax.ShapeDtypeStruct((T, COLS), BF16),
            jax.ShapeDtypeStruct((8, COLS), F32),
            jax.ShapeDtypeStruct((8, COLS), F32),
            jax.ShapeDtypeStruct((T, COLS), BF16),
            jax.ShapeDtypeStruct((heads, T), F32),
            jax.ShapeDtypeStruct((T, 128), BF16),
            jax.ShapeDtypeStruct((SHARDS, BUNDLE + 8, 128), BF16),
        ],
        scratch_shapes=TOKEN_SCRATCH + [
            pltpu.VMEM((128, T), F32),
            pltpu.VMEM((T, T), F32),
            pltpu.VMEM((T, T), F32),
            pltpu.VMEM((HALF, HALF), F32),
            pltpu.VMEM((HALF, T), F32),
            pltpu.VMEM((T, 128), F32),
            pltpu.VMEM((T, 128), F32),
            pltpu.VMEM((T, 128), F32),
            pltpu.VMEM((8, 128), F32),
            pltpu.VMEM((BUNDLE + 8, 128), F32),
            half, half, half, half,
        ],
        cost_estimate=pl.CostEstimate(flops=18 * 10**9, bytes_accessed=8 * 10**6, transcendentals=0),
        name="mixer_second",
    )(*arrays)


def finish_kernel(
    where_ref, bundle_ref, *refs
):
    coeff_refs = refs[:LOCAL_HEADS]
    weight_ref, bias_ref, rate_ref, skip_ref, in_ref, out_ref, coeff_s = refs[LOCAL_HEADS:]
    for turn, ref in enumerate(coeff_refs):
        coeff_s[lax.rem(where_ref[4] - turn + LOCAL_HEADS, LOCAL_HEADS)] = ref[...].astype(F32)
    total = bundle_ref[0].astype(F32)
    for shard in range(1, SHARDS):
        total = total + bundle_ref[shard].astype(F32)
    tiles = COLS // 128
    for lag in range(KERNEL):
        for m in range(tiles):
            weight_ref[lag : lag + 1, 128 * m : 128 * (m + 1)] = total[
                lag * tiles + m : lag * tiles + m + 1
            ]
    for n, ref in enumerate((bias_ref, rate_ref, skip_ref)):
        row = BUNDLE + 2 * n
        ref[...] = (total[row : row + 1] + total[row + 1 : row + 2])[:, : ref.shape[1]]
    low, high = coeff_s[0] + coeff_s[1], coeff_s[2] + coeff_s[3]
    left = iota((T, 128), 1) < STATE
    out_ref[...] = jnp.where(left, low, pltpu.roll(high, STATE, 1))
    in_ref[...] = jnp.where(left, pltpu.roll(low, STATE, 1), high)


def finish(where, bundle, coeffs, heads):
    small = jax.ShapeDtypeStruct((1, heads), F32)
    wide = jax.ShapeDtypeStruct((T, 128), F32)
    return pl.pallas_call(
        finish_kernel,
        in_specs=[IN_SMEM] + [IN_VMEM] * (1 + LOCAL_HEADS),
        out_specs=[IN_VMEM] * 6,
        out_shape=[jax.ShapeDtypeStruct((KERNEL, COLS), F32), small, small, small, wide, wide],
        scratch_shapes=[pltpu.VMEM((LOCAL_HEADS, T, 128), F32)],
        name="finish",
    )(where, bundle, *coeffs)


ROW = 4
K_AT, V_AT, Q_AT = (slice(n * HEAD_DIM, (n + 1) * HEAD_DIM) for n in range(3))


def pack_kernel(where_ref, k_ref, v_ref, q_ref, g_ref, *refs):
    out_refs, turned_s = refs[: 2 * ROW], refs[2 * ROW]
    for n, ref in enumerate((k_ref, v_ref, q_ref, g_ref)):
        half = slice((n % 2) * HEAD_DIM, (n % 2 + 1) * HEAD_DIM)
        turned_part = jnp.transpose(ref[...])
        for head in range(LOCAL_HEADS):
            turned_s[n // 2, head, half] = turned_part[head * HEAD_DIM : (head + 1) * HEAD_DIM]
    for turn in range(ROW):
        head = lax.rem(where_ref[3] + turn, ROW)
        out_refs[turn][...] = turned_s[0, head]
        out_refs[ROW + turn][...] = turned_s[1, head]


def pack(where, keys, values, queries, grads):
    outs = pl.pallas_call(
        pack_kernel,
        in_specs=[IN_SMEM] + [IN_VMEM] * 4,
        out_specs=[IN_VMEM] * (2 * ROW),
        out_shape=[jax.ShapeDtypeStruct((2 * HEAD_DIM, T), BF16)] * (2 * ROW),
        scratch_shapes=[pltpu.VMEM((2, LOCAL_HEADS, 2 * HEAD_DIM, T), BF16)],
        name="pack",
    )(where, keys, values, queries, grads)
    return outs[:ROW], outs[ROW:]


def attention_kernel(where_ref, docs_ref, *refs):
    arrived, (dq_ref, dkv_ref, back_ref, far_s, kv_s, qg_s) = refs[: 3 * ROW], refs[3 * ROW :]
    for turn in range(ROW):
        block = lax.rem(where_ref[3] - turn + ROW, ROW)
        qg_s[block] = arrived[turn][...]
        kv_s[ROW + block] = arrived[ROW + turn][...]
        kv_s[block] = arrived[2 * ROW + turn][...]
    first_block = where_ref[2] * ROW
    later = iota((T, T), 1) > iota((T, T), 0)
    scale = HEAD_DIM ** (-0.5)

    def doc_row(block):
        place = first_block + block
        row = docs_ref[pl.ds(jnp.maximum(place, 0), 1), :].astype(F32)
        return row if block >= 0 else jnp.where(place < 0, -1.0, row)

    rows = {block: doc_row(block) for block in range(-ROW, ROW)}
    for i in range(ROW):
        own_doc = columns_of(rows[i])
        qt, gt = qg_s[i, K_AT], qg_s[i, V_AT]
        q, g = jnp.transpose(qt), jnp.transpose(gt)

        def part(gap, place):
            return kv_s[ROW + i - gap, place]

        scores = []
        top = None
        for gap in range(ROW + 1):
            same = own_doc == rows[i - gap]
            if gap == 0:
                same = same & jnp.logical_not(later)
            if gap == ROW:
                same = same & later
            s = jnp.where(same, dot(q, part(gap, K_AT)) * (scale * LOG2E), NEG)
            scores.append(s)
            top = s if top is None else jnp.maximum(top, s)
        top = jnp.max(top, axis=1, keepdims=True)
        expos = [jnp.exp2(s - top) for s in scores]
        total = jnp.sum(sum(expos), axis=1, keepdims=True)
        inverse = 1.0 / jnp.maximum(total, 1.0)
        probs = [e * inverse for e in expos]
        halves = [p.astype(BF16) for p in probs]
        dprobs = [dot(g, part(gap, V_AT)) for gap in range(ROW + 1)]
        delta = sum(h.astype(F32) * d for h, d in zip(halves, dprobs))
        delta = jnp.sum(delta, axis=1, keepdims=True)
        dq = jnp.zeros((HEAD_DIM, T), F32)
        for gap in range(ROW + 1):
            dscore = (probs[gap] * (dprobs[gap] - delta)).astype(BF16)
            dq = dq + dot(part(gap, K_AT), dscore, NT)
            block = i - gap
            ref, index = (dkv_ref, block) if block >= 0 else (far_s, block + ROW)
            dk, dv = dot(qt, dscore), dot(gt, halves[gap])
            if gap == 0 or (block < 0 and i == 0):
                ref[index, K_AT] = dk
                ref[index, V_AT] = dv
            else:
                ref[index, K_AT] += dk
                ref[index, V_AT] += dv
            if gap == ROW:
                back_ref[index] = far_s[index].astype(BF16)
        dq_ref[i] = (dq * scale).astype(BF16)


def attention(where, docs, qg, kv, far):
    pair = (ROW, 2 * HEAD_DIM, T)
    return pl.pallas_call(
        attention_kernel,
        in_specs=[IN_SMEM] + [IN_VMEM] * (1 + 3 * ROW),
        out_specs=[IN_VMEM] * 3,
        out_shape=[
            jax.ShapeDtypeStruct((ROW, HEAD_DIM, T), BF16),
            jax.ShapeDtypeStruct(pair, F32),
            jax.ShapeDtypeStruct(pair, BF16),
        ],
        scratch_shapes=[
            pltpu.VMEM(pair, F32),
            pltpu.VMEM((2 * ROW, 2 * HEAD_DIM, T), BF16),
            pltpu.VMEM(pair, BF16),
        ],
        cost_estimate=pl.CostEstimate(flops=12 * 10**9, bytes_accessed=8 * 10**6, transcendentals=0),
        name="attention",
    )(where, docs, *qg, *kv, *far)


def merge_kernel(where_ref, dq_ref, dkv_ref, back_ref, *out_refs):
    scale = HEAD_DIM ** (-0.5)
    place = where_ref[3]
    for turn, out_ref in enumerate(out_refs):
        block = lax.rem(place + turn, ROW)
        total = dkv_ref[block] + back_ref[block].astype(F32)
        out_ref[K_AT] = (total[K_AT] * scale).astype(BF16)
        out_ref[V_AT] = total[V_AT].astype(BF16)
        out_ref[Q_AT] = dq_ref[block]


def merge(where, dq, dkv, back):
    return pl.pallas_call(
        merge_kernel,
        in_specs=[IN_SMEM] + [IN_VMEM] * 3,
        out_specs=[IN_VMEM] * ROW,
        out_shape=[jax.ShapeDtypeStruct((3 * HEAD_DIM, T), BF16)] * ROW,
        cost_estimate=pl.CostEstimate(flops=3 * 10**9, bytes_accessed=4 * 10**6, transcendentals=0),
        name="merge",
    )(where, dq, dkv, back)


def unpack_kernel(where_ref, *refs):
    parts, outs, stacked_s = refs[:ROW], refs[ROW : ROW + 3], refs[ROW + 3]
    place = where_ref[3]
    for turn, part in enumerate(parts):
        source = lax.rem(place - turn + ROW, ROW)
        for n, at in enumerate((Q_AT, K_AT, V_AT)):
            stacked_s[n, source] = part[at]
    for n, ref in enumerate(outs):
        stacked = jnp.concatenate([stacked_s[n, h] for h in range(LOCAL_HEADS)], axis=0)
        ref[...] = jnp.transpose(stacked)


def unpack(where, parts):
    wide = jax.ShapeDtypeStruct((T, LOCAL_HEADS * HEAD_DIM), BF16)
    return pl.pallas_call(
        unpack_kernel,
        in_specs=[IN_SMEM] + [IN_VMEM] * ROW,
        out_specs=[IN_VMEM] * 3,
        out_shape=[wide] * 3,
        scratch_shapes=[pltpu.VMEM((3, LOCAL_HEADS, HEAD_DIM, T), BF16)],
        name="unpack",
    )(where, *parts)


def passed_along(value, axis, steps):
    count = lax.axis_size(axis)
    initial, last = (max(0, -steps), min(count, count - steps))
    return lax.ppermute(value, axis, [(source, source + steps) for source in range(initial, last)])


def turns(parts, axis):
    count = lax.axis_size(axis)
    return [parts[0]] + [
        lax.ppermute(part, axis, [(n, (n + turn) % count) for n in range(count)])
        for turn, part in enumerate(parts[1:], 1)
    ]


def exchange(array, axis):
    return lax.all_to_all(array, axis, split_axis=0, concat_axis=0, tiled=True)


def local(
    queries, keys, values, attn_grad, doc_ids, conv_input, conv_weight, step_raw, step_bias,
    rate_log, skip_gain, input_coeff, output_coeff, gate_input, mix_grad,
):
    heads = step_raw.shape[1]
    shard = lax.axis_index(SEQ)
    group = lax.axis_index("head") * heads // (SSM_HEADS // GROUPS)
    where = jnp.stack([shard, group, shard // ROW, lax.axis_index("seq_2"), lax.axis_index("head")]).astype(jnp.int32)
    docs = doc_ids.reshape(SHARDS, T)
    halo = passed_along(conv_input[T - 8 :], SEQ, 1)
    kv_parts, qg_parts = pack(where, keys, values, queries, attn_grad)
    kv = turns(kv_parts, "seq_2")
    qg = turns(qg_parts, "seq_2")
    far = [passed_along(kv[0], SEQ, ROW)]
    far = far + [passed_along(part, SEQ, ROW) for part in kv[1:]]

    mixer_args = (
        where, conv_input, halo, conv_weight, gate_input, mix_grad, step_raw.T,
        step_bias.reshape(1, heads), rate_log.reshape(1, heads), skip_gain.reshape(1, heads),
        docs, input_coeff, output_coeff,
    )
    parts = mixer_first(*mixer_args).reshape(SHARDS, SLOT, 128)
    gathered = exchange(parts, SEQ)
    scanned = chain(where, gathered)
    entering = exchange(scanned, SEQ).reshape(COLS, 128)
    dq, dkv, back = attention(where, docs, qg, kv, far)
    returned = passed_along(back, SEQ, -ROW)
    dx, tail, spill, dgate, dstep, coeff, bundle = mixer_second(*mixer_args, entering)
    spilled = passed_along(spill, SEQ, -1)
    bundles = exchange(bundle, SEQ)
    coeffs = turns([coeff] * LOCAL_HEADS, "head")
    leaving = merge(where, dq, dkv, returned)
    swapped = turns(leaving, "seq_2")
    grad_weight, grad_bias, grad_rate, grad_skip, sum_in, sum_out = finish(
        where, bundles, coeffs, heads
    )
    dq, dk, dv = unpack(where, swapped)
    tail = (tail + spilled).astype(BF16)
    grad_conv = lax.dynamic_update_slice_in_dim(dx, tail, T - 8, 0)
    return (
        dq, dk, dv, grad_conv, dgate, dstep.T, sum_in, sum_out, grad_weight,
        grad_bias.reshape(heads), grad_rate.reshape(heads), grad_skip.reshape(heads),
    )


def solution(mesh):
    finer = Mesh(
        mesh.devices.reshape(4, 2, 4, mesh.shape["head"]), ("seq_0", "seq_1", "seq_2", "head")
    )
    wide = P(SEQ, "head")
    return jax.shard_map(
        local,
        mesh=finer,
        in_specs=(
            wide, wide, wide, wide, P(), wide, P(None, "head"), wide, P("head"), P("head"),
            P("head"), P(SEQ, None), P(SEQ, None), wide, wide,
        ),
        out_specs=(
            wide, wide, wide, wide, wide, wide, P(SEQ, None), P(SEQ, None), P(None, "head"),
            P("head"), P("head"), P("head"),
        ),
        check_vma=False,
    )
```

```python
import jax
import jax.numpy as jnp
from jax import lax
from jax.experimental import pallas as pl
from jax.experimental.pallas import tpu as pltpu
from jax.sharding import Mesh
from jax.sharding import PartitionSpec as P


HEAD_DIM = 224
STATE = 64
KERNEL = 4
SEQ = ("seq_0", "seq_1", "seq_2")
SHARDS = 32
T = 256
LOCAL_HEADS = 4
BLK = 256
HALF = T // 2
HEADS_BLK = BLK // 64
COLS = 1792
STEPS = COLS // BLK
NEG = -1e30
LOG2E = 1.4426950408889634
F32 = jnp.float32
BF16 = jnp.bfloat16

NN = (((1,), (0,)), ((), ()))
NT = (((1,), (1,)), ((), ()))
TN = (((0,), (0,)), ((), ()))


def dot(a, b, dims=NN):
    return lax.dot_general(a, b, dims, preferred_element_type=F32)


def exact(a, b, dims=NN):
    return lax.dot_general(
        a, b, dims, preferred_element_type=F32, precision=lax.Precision.HIGHEST
    )


def split(a, pieces):
    parts = []
    for _ in range(pieces):
        part = a.astype(BF16)
        parts.append(part)
        a = a - part.astype(F32)
    return parts


def sigmoid(v):
    return 0.5 + 0.5 * jnp.tanh(0.5 * v)


def iota(shape, dim):
    return lax.broadcasted_iota(jnp.int32, shape, dim)


def columns_of(row):
    return jnp.transpose(jnp.broadcast_to(row, (T, T)))


def whole(shape):
    return pl.BlockSpec(shape, lambda c: (0,) * len(shape))


def column_block(rows):
    return pl.BlockSpec((rows, BLK), lambda c: (0, c))


IN_SMEM = pl.BlockSpec(memory_space=pltpu.SMEM)
IN_VMEM = pl.BlockSpec(memory_space=pltpu.VMEM)


def seq_index():
    index = 0
    for axis in SEQ:
        index = index * lax.axis_size(axis) + lax.axis_index(axis)
    return index


def row_place():
    return lax.axis_index(SEQ[-1])


def doc_row_of(docs_ref, shard):
    return jnp.concatenate(
        [docs_ref[pl.ds(2 * shard + part, 1), :] for part in range(2)], axis=1
    ).astype(F32)


def doc_rows(docs_ref):
    shard = seq_index()
    own = doc_row_of(docs_ref, shard)
    before = doc_row_of(docs_ref, jnp.maximum(shard - 1, 0))
    return own, jnp.where(shard == 0, -1.0, before)


def group_halves(coeff_ref):
    coeff = coeff_ref[...].astype(F32)
    turned = pltpu.roll(coeff, STATE, 1)
    first = lax.axis_index("head") < 2
    low = iota((T, 128), 1) < STATE
    mine_low = jnp.where(low, jnp.where(first, coeff, turned), 0.0)
    mine_high = jnp.where(low, 0.0, jnp.where(first, turned, coeff))
    return mine_low.astype(BF16), mine_high.astype(BF16)


def padded_params(bias_ref, rate_ref, skip_ref, params_s):
    heads = bias_ref.shape[1]
    params_s[...] = jnp.zeros((8, 128), F32)
    for n, ref in enumerate((bias_ref, rate_ref, skip_ref)):
        params_s[n : n + 1, 0:heads] = ref[...]
    return params_s[...]


def raw_steps(step_ref):
    rows = step_ref.shape[0]
    filled = jnp.concatenate([step_ref[...], jnp.zeros((128 - rows, T), F32)], axis=0)
    return jnp.transpose(filled)


def step_and_decay(raw, params):
    step = jnp.maximum(raw, 0.0) + jnp.log1p(jnp.exp(-jnp.abs(raw)))
    return step, -step * jnp.exp(params[1:2])


def token_setup(docs_ref, step_ref, params, cum_s, step_s, mask_s, prev_s, end_s):
    own_row, before_row = doc_rows(docs_ref)
    own = columns_of(own_row)
    lane = iota((8, T), 1)
    own8 = jnp.broadcast_to(own_row, (8, T))
    before8 = jnp.broadcast_to(before_row, (8, T))
    for lag in range(1, KERNEL):
        lagged = jnp.where(lane < lag, pltpu.roll(before8, lag, 1), pltpu.roll(own8, lag, 1))
        mask_s[lag - 1] = jnp.where(own == columns_of(lagged[0:1]), 1.0, 0.0)
    prev_s[...] = jnp.where(own == before_row[:, T - 1 : T], 0.0, NEG)
    end_s[...] = jnp.where(own == own_row[:, T - 1 : T], 0.0, NEG)
    raw = raw_steps(step_ref) + params[0:1]
    step, decay = step_and_decay(raw, params)
    lower = jnp.where(iota((T, T), 0) >= iota((T, T), 1), 1.0, 0.0)
    cum = exact(lower, decay) * LOG2E
    for n, part in enumerate(split(cum, 3)):
        cum_s[n] = part
    for n, part in enumerate(split(step, 2)):
        step_s[n] = part
    return own, own_row, cum


def spread_of(step_id):
    head = iota((128, BLK), 0)
    owner = step_id * HEADS_BLK + iota((128, BLK), 1) // 64
    return jnp.where(head == owner, 1.0, 0.0).astype(BF16)


def block_gains(step_id, cum_s, step_s, prev_s, end_s):
    spread = spread_of(step_id)
    cum = dot(cum_s[0], spread) + dot(cum_s[1], spread) + dot(cum_s[2], spread)
    step = dot(step_s[0], spread) + dot(step_s[1], spread)
    enter = jnp.exp2(cum + prev_s[...])
    to_end = jnp.exp2(cum[T - 1 : T] - cum + end_s[...])
    return spread, cum, step, enter, to_end


def conv_pre(x, halo, weight, mask_s):
    extended = jnp.concatenate([halo.astype(F32), x.astype(F32)], axis=0)
    shifted = [extended[8:]]
    summed = weight[0:1] * shifted[0]
    for lag in range(1, KERNEL):
        moved = pltpu.roll(extended, lag, 0)[8:] * mask_s[lag - 1]
        shifted.append(moved)
        summed = summed + weight[lag : lag + 1] * moved
    return summed, shifted


ROWS = COLS // SHARDS
GROUPS8 = ROWS // 8
SLOT = ROWS + 8


def mixer_first_kernel(
    x_ref, halo_ref, weight_ref, gate_ref, grad_ref, step_ref, bias_ref, rate_ref,
    skip_ref, docs_ref, in_ref, out_ref,
    parts_ref,
    cum_s, step_s, mask_s, prev_s, end_s, params_s, state_s, in_s, out_s,
):
    step_id = pl.program_id(0)

    @pl.when(step_id == 0)
    def _():
        params = padded_params(bias_ref, rate_ref, skip_ref, params_s)
        cum = token_setup(
            docs_ref, step_ref, params, cum_s, step_s, mask_s, prev_s, end_s
        )[2]
        through = jnp.exp2(cum[T - 1 : T] + prev_s[T - 1 : T, 0:1])
        high, low = split(through, 2)
        row = iota((8, 128), 0)
        both = jnp.where(row == 0, high.astype(F32), jnp.where(row == 1, low.astype(F32), 0.0))
        for shard in range(SHARDS):
            state_s[SLOT * shard + ROWS : SLOT * (shard + 1)] = both
        in_s[...] = group_halves(in_ref)[0]
        out_s[...] = group_halves(out_ref)[1]

    _, _, step, enter, to_end = block_gains(step_id, cum_s, step_s, prev_s, end_s)
    pre, _ = conv_pre(x_ref[...], halo_ref[...], weight_ref[...], mask_s)
    act = pre * sigmoid(pre)
    gate = gate_ref[...].astype(F32)
    out_grad = grad_ref[...].astype(F32) * gate * sigmoid(gate)
    ended = (act * step * to_end).astype(BF16)
    entered = (out_grad * enter).astype(BF16)
    state = dot(ended, in_s[...], TN) + dot(entered, out_s[...], TN)
    for part in range(BLK // 8):
        place = step_id * (BLK // 8) + part
        target = lax.div(place, GROUPS8)
        offset = SLOT * target + 8 * (place - GROUPS8 * target)
        state_s[pl.ds(pl.multiple_of(offset, 8), 8), :] = state[8 * part : 8 * part + 8]

    @pl.when(step_id == STEPS - 1)
    def _():
        parts_ref[...] = state_s[...].astype(BF16)


TOKEN_SCRATCH = [
    pltpu.VMEM((3, T, 128), BF16),
    pltpu.VMEM((2, T, 128), BF16),
    pltpu.VMEM((KERNEL - 1, T, BLK), F32),
    pltpu.VMEM((T, BLK), F32),
    pltpu.VMEM((T, BLK), F32),
    pltpu.VMEM((8, 128), F32),
]


def mixer_specs(heads):
    return [
        column_block(T), column_block(8), column_block(KERNEL), column_block(T),
        column_block(T), whole((heads, T)), whole((1, heads)), whole((1, heads)),
        whole((1, heads)), whole((SHARDS * T // 128, 128)), whole((T, 128)), whole((T, 128)),
    ]


def mixer_first(*arrays):
    heads = arrays[5].shape[0]
    return pl.pallas_call(
        mixer_first_kernel,
        grid=(STEPS,),
        in_specs=mixer_specs(heads),
        out_specs=whole((SHARDS * SLOT, 128)),
        out_shape=jax.ShapeDtypeStruct((SHARDS * SLOT, 128), BF16),
        scratch_shapes=TOKEN_SCRATCH + [
            pltpu.VMEM((SHARDS * SLOT, 128), F32),
            pltpu.VMEM((T, 128), BF16),
            pltpu.VMEM((T, 128), BF16),
        ],
        cost_estimate=pl.CostEstimate(flops=8 * 10**9, bytes_accessed=4 * 10**6, transcendentals=0),
        name="mixer_first",
    )(*arrays)


def chain_kernel(parts_ref, out_ref, forward_s):
    slot = seq_index()
    owner = (slot * ROWS + iota((ROWS, 128), 0)) // 64
    choose = jnp.where(owner == iota((ROWS, 128), 1), 1.0, 0.0)
    lane = iota((ROWS, 128), 1)
    through = []
    carry = jnp.zeros((ROWS, 128), F32)
    for shard in range(SHARDS):
        row = parts_ref[shard, ROWS : ROWS + 1].astype(F32)
        row = row + parts_ref[shard, ROWS + 1 : ROWS + 2].astype(F32)
        gain = jnp.sum(choose * row, axis=1, keepdims=True)
        through.append(gain)
        forward_s[shard] = carry
        carry = gain * carry + parts_ref[shard, 0:ROWS].astype(F32)
    carry = jnp.zeros((ROWS, 128), F32)
    for shard in reversed(range(SHARDS)):
        out_ref[shard] = jnp.where(lane < STATE, forward_s[shard], carry).astype(BF16)
        carry = through[shard] * carry + parts_ref[shard, 0:ROWS].astype(F32)


def chain(parts):
    return pl.pallas_call(
        chain_kernel,
        in_specs=[IN_VMEM],
        out_specs=IN_VMEM,
        out_shape=jax.ShapeDtypeStruct((SHARDS, ROWS, 128), BF16),
        scratch_shapes=[pltpu.VMEM((SHARDS, ROWS, 128), F32)],
        cost_estimate=pl.CostEstimate(flops=2 * 10**9, bytes_accessed=10**6, transcendentals=0),
        name="chain",
    )(parts)


BUNDLE = KERNEL * COLS // 128
LANES_BLK = BLK // 128


def mixer_second_kernel(
    x_ref, halo_ref, weight_ref, gate_ref, grad_ref, step_ref, bias_ref, rate_ref,
    skip_ref, docs_ref, in_ref, out_ref, state_ref,
    dx_ref, tail_ref, spill_ref, dgate_ref, dstep_ref, coeff_ref, bundle_ref,
    cum_s, step_s, mask_s, prev_s, end_s, params_s,
    cumt_s, pair_s, causal_s, dtop_s, dbottom_s, coeff_s, row_s, dt_s, ends_s, bundle_s,
    in_low_s, in_high_s, out_low_s, out_high_s,
):
    step_id = pl.program_id(0)
    lane = iota((T, 128), 1)

    @pl.when(step_id == 0)
    def _():
        params = padded_params(bias_ref, rate_ref, skip_ref, params_s)
        own, own_row, cum = token_setup(
            docs_ref, step_ref, params, cum_s, step_s, mask_s, prev_s, end_s
        )
        cumt_s[...] = jnp.transpose(cum)
        same = (own == own_row) & (iota((T, T), 0) >= iota((T, T), 1))
        causal_s[...] = jnp.where(same, 0.0, NEG)
        in_low_s[...], in_high_s[...] = group_halves(in_ref)
        out_low_s[...], out_high_s[...] = group_halves(out_ref)
        pair_s[...] = dot(out_low_s[...], in_low_s[...], NT)
        dtop_s[...] = jnp.zeros((HALF, HALF), F32)
        dbottom_s[...] = jnp.zeros((HALF, T), F32)
        coeff_s[...] = jnp.zeros((T, 128), F32)
        row_s[...] = jnp.zeros((T, 128), F32)
        dt_s[...] = jnp.zeros((T, 128), F32)
        ends_s[...] = jnp.zeros((8, 128), F32)

    out_low = out_low_s[...]
    in_high = in_high_s[...]
    spread, cum, step, enter, to_end = block_gains(step_id, cum_s, step_s, prev_s, end_s)
    skip = sum(dot(part, spread) for part in split(params_s[...], 3))[2:3]
    weight = weight_ref[...]
    pre, shifted = conv_pre(x_ref[...], halo_ref[...], weight, mask_s)
    sig = sigmoid(pre)
    act = pre * sig
    gate = gate_ref[...].astype(F32)
    gate_sig = sigmoid(gate)
    mix_grad = grad_ref[...].astype(F32)
    out_grad = mix_grad * gate * gate_sig
    scaled = act * step
    scaled_half = scaled.astype(BF16)
    grad_half = out_grad.astype(BF16)

    block_head = iota((T, BLK), 1) // 64
    tops, bottoms, scaled_parts, grad_parts = [], [], [], []
    dtop, dbottom = dtop_s[...], dbottom_s[...]
    for k in range(HEADS_BLK):
        mine = block_head == k
        cum_col = cum[:, 64 * k : 64 * k + 1]
        cum_row = cumt_s[pl.ds(step_id * HEADS_BLK + k, 1), :]
        top = jnp.exp2(
            jnp.broadcast_to(cum_col[:HALF], (HALF, HALF)) - cum_row[:, :HALF]
            + causal_s[:HALF, :HALF]
        )
        bottom = jnp.exp2(
            jnp.broadcast_to(cum_col[HALF:], (HALF, T)) - cum_row + causal_s[HALF:, :]
        )
        tops.append((pair_s[:HALF, :HALF] * top).astype(BF16))
        bottoms.append((pair_s[HALF:, :] * bottom).astype(BF16))
        scaled_k = jnp.where(mine, scaled_half, jnp.zeros_like(scaled_half))
        grad_k = jnp.where(mine, grad_half, jnp.zeros_like(grad_half))
        scaled_parts.append(scaled_k)
        grad_parts.append(grad_k)
        dtop = dtop + dot(grad_k[:HALF], scaled_half[:HALF], NT) * top
        dbottom = dbottom + dot(grad_k[HALF:], scaled_half, NT) * bottom
    dtop_s[...] = dtop
    dbottom_s[...] = dbottom
    join = jnp.concatenate
    inner = join(
        [
            dot(join(tops, axis=1), join([v[:HALF] for v in scaled_parts], axis=0)),
            dot(join(bottoms, axis=1), join(scaled_parts, axis=0)),
        ],
        axis=0,
    )
    upper_part = dot(join(tops, axis=0), join([v[:HALF] for v in grad_parts], axis=0), TN)
    dscaled = dot(join(bottoms, axis=0), join([v[HALF:] for v in grad_parts], axis=0), TN)
    dscaled = join([dscaled[:HALF] + upper_part, dscaled[HALF:]], axis=0)

    state = state_ref[...]
    carried = dot(out_low, state, NT) * enter
    from_end = dot(in_high, state, NT) * to_end
    ssm_out = inner + carried
    dscaled = dscaled + from_end
    mixed_out = ssm_out + skip * act
    dgate_ref[...] = (
        mix_grad * mixed_out * gate_sig * (1.0 + gate * (1.0 - gate_sig))
    ).astype(BF16)

    gave_out = dot((out_grad * enter).astype(BF16), state)
    gave_in = dot((scaled * to_end).astype(BF16), state)
    coeff_s[...] += jnp.where(lane < STATE, gave_out, gave_in)

    grad_round = grad_half.astype(F32)
    scaled_round = scaled_half.astype(F32)
    balance = grad_round * ssm_out - scaled_round * dscaled
    row_s[...] += sum(dot(part, spread, NT) for part in split(balance, 2))
    dt_s[...] += dot((dscaled * act).astype(BF16), spread, NT)

    state_wide = state.astype(F32)
    product = state_wide * pltpu.roll(state_wide, STATE, 1)
    through = jnp.sum(jnp.where(iota((BLK, 128), 1) < STATE, product, 0.0), axis=1, keepdims=True)
    through_row = jnp.transpose(jnp.broadcast_to(through, (BLK, BLK)))[0:1]
    end_row = jnp.sum(scaled_round * from_end, axis=0, keepdims=True)
    end_row = end_row + through_row * enter[T - 1 : T]
    skip_row = jnp.sum(out_grad * act, axis=0, keepdims=True)
    row8 = iota((8, BLK), 0)
    both = jnp.where(row8 == 0, end_row, jnp.where(row8 == 1, skip_row, 0.0))
    ends_s[...] += sum(dot(part, spread, NT) for part in split(both, 3))

    dact = step * dscaled + skip * out_grad
    dpre = dact * sig * (1.0 + pre * (1.0 - sig))
    zeros = jnp.zeros((8, BLK), F32)
    dx = weight[0:1] * dpre
    spill = zeros
    for lag in range(KERNEL):
        tap = jnp.sum(dpre * shifted[lag], axis=0, keepdims=True)
        for m in range(LANES_BLK):
            place = lag * (COLS // 128) + step_id * LANES_BLK + m
            bundle_s[pl.ds(place, 1), :] = tap[:, 128 * m : 128 * (m + 1)]
        if lag == 0:
            continue
        masked = dpre * mask_s[lag - 1]
        later = pltpu.roll(jnp.concatenate([masked, zeros], axis=0), T + 8 - lag, 0)[:T]
        dx = dx + weight[lag : lag + 1] * later
        edge = pltpu.roll(jnp.concatenate([zeros, masked[:8]], axis=0), 16 - lag, 0)[:8]
        spill = spill + weight[lag : lag + 1] * edge
    dx_ref[...] = dx.astype(BF16)
    tail_ref[...] = dx[T - 8 :]
    spill_ref[...] = spill

    @pl.when(step_id == STEPS - 1)
    def _():
        params = params_s[...]
        raw = raw_steps(step_ref) + params[0:1]
        rate = jnp.exp(params[1:2])
        decay = step_and_decay(raw, params)[1]
        upper = jnp.where(iota((T, T), 1) >= iota((T, T), 0), 1.0, 0.0)
        ends = ends_s[...]
        ddecay = exact(upper, row_s[...]) + ends[0:1]
        dstep = (dt_s[...] - ddecay * rate) * sigmoid(raw)
        dstep_ref[...] = jnp.transpose(dstep)[: dstep_ref.shape[0]]
        dbias = jnp.sum(dstep, axis=0, keepdims=True)
        drate = jnp.sum(ddecay * decay, axis=0, keepdims=True)
        row = iota((8, 128), 0)
        small = jnp.zeros((8, 128), F32)
        for n, vector in enumerate((dbias, drate, ends[1:2])):
            for m, part in enumerate(split(vector, 2)):
                small = jnp.where(row == 2 * n + m, part.astype(F32), small)
        bundle_s[BUNDLE : BUNDLE + 8] = small
        bundle = bundle_s[...].astype(BF16)
        for shard in range(SHARDS):
            bundle_ref[shard] = bundle
        top_half, bottom_half = dtop.astype(BF16), dbottom.astype(BF16)
        in_low, out_high = in_low_s[...], out_high_s[...]
        out_part = join([dot(top_half, in_low[:HALF]), dot(bottom_half, in_low)], axis=0)
        in_part = dot(bottom_half, out_high[HALF:], TN)
        in_part = join(
            [in_part[:HALF] + dot(top_half, out_high[:HALF], TN), in_part[HALF:]], axis=0
        )
        coeff_ref[...] = (coeff_s[...] + out_part + in_part).astype(BF16)


def mixer_second(*arrays):
    heads = arrays[5].shape[0]
    half = pltpu.VMEM((T, 128), BF16)
    return pl.pallas_call(
        mixer_second_kernel,
        grid=(STEPS,),
        in_specs=mixer_specs(heads) + [pl.BlockSpec((BLK, 128), lambda c: (c, 0))],
        out_specs=[
            column_block(T), column_block(8), column_block(8), column_block(T),
            whole((heads, T)), whole((T, 128)), whole((SHARDS, BUNDLE + 8, 128)),
        ],
        out_shape=[
            jax.ShapeDtypeStruct((T, COLS), BF16),
            jax.ShapeDtypeStruct((8, COLS), F32),
            jax.ShapeDtypeStruct((8, COLS), F32),
            jax.ShapeDtypeStruct((T, COLS), BF16),
            jax.ShapeDtypeStruct((heads, T), F32),
            jax.ShapeDtypeStruct((T, 128), BF16),
            jax.ShapeDtypeStruct((SHARDS, BUNDLE + 8, 128), BF16),
        ],
        scratch_shapes=TOKEN_SCRATCH + [
            pltpu.VMEM((128, T), F32),
            pltpu.VMEM((T, T), F32),
            pltpu.VMEM((T, T), F32),
            pltpu.VMEM((HALF, HALF), F32),
            pltpu.VMEM((HALF, T), F32),
            pltpu.VMEM((T, 128), F32),
            pltpu.VMEM((T, 128), F32),
            pltpu.VMEM((T, 128), F32),
            pltpu.VMEM((8, 128), F32),
            pltpu.VMEM((BUNDLE + 8, 128), F32),
            half, half, half, half,
        ],
        cost_estimate=pl.CostEstimate(flops=18 * 10**9, bytes_accessed=8 * 10**6, transcendentals=0),
        name="mixer_second",
    )(*arrays)


def finish_kernel(bundle_ref, *refs):
    coeff_refs = refs[:LOCAL_HEADS]
    weight_ref, bias_ref, rate_ref, skip_ref, in_ref, out_ref, coeff_s = refs[LOCAL_HEADS:]
    for turn, ref in enumerate(coeff_refs):
        coeff_s[lax.rem(lax.axis_index("head") - turn + LOCAL_HEADS, LOCAL_HEADS)] = ref[...].astype(F32)
    total = bundle_ref[0].astype(F32)
    for shard in range(1, SHARDS):
        total = total + bundle_ref[shard].astype(F32)
    tiles = COLS // 128
    for lag in range(KERNEL):
        for m in range(tiles):
            weight_ref[lag : lag + 1, 128 * m : 128 * (m + 1)] = total[
                lag * tiles + m : lag * tiles + m + 1
            ]
    for n, ref in enumerate((bias_ref, rate_ref, skip_ref)):
        row = BUNDLE + 2 * n
        ref[...] = (total[row : row + 1] + total[row + 1 : row + 2])[:, : ref.shape[1]]
    low, high = coeff_s[0] + coeff_s[1], coeff_s[2] + coeff_s[3]
    left = iota((T, 128), 1) < STATE
    out_ref[...] = jnp.where(left, low, pltpu.roll(high, STATE, 1))
    in_ref[...] = jnp.where(left, pltpu.roll(low, STATE, 1), high)


def finish(bundle, coeffs, heads):
    small = jax.ShapeDtypeStruct((1, heads), F32)
    wide = jax.ShapeDtypeStruct((T, 128), F32)
    return pl.pallas_call(
        finish_kernel,
        in_specs=[IN_VMEM] * (1 + LOCAL_HEADS),
        out_specs=[IN_VMEM] * 6,
        out_shape=[jax.ShapeDtypeStruct((KERNEL, COLS), F32), small, small, small, wide, wide],
        scratch_shapes=[pltpu.VMEM((LOCAL_HEADS, T, 128), F32)],
        name="finish",
    )(bundle, *coeffs)


ROW = 4
K_AT, V_AT, Q_AT, G_AT = (slice(n * HEAD_DIM, (n + 1) * HEAD_DIM) for n in range(4))
PAIR = (2 * HEAD_DIM, T)


def pack_kernel(k_ref, v_ref, q_ref, g_ref, *refs):
    own_refs, far_refs, turned_s = refs[:ROW], refs[ROW : 2 * ROW], refs[2 * ROW]
    for ref, place in ((k_ref, K_AT), (v_ref, V_AT), (q_ref, Q_AT), (g_ref, G_AT)):
        turned_part = jnp.transpose(ref[...])
        for head in range(LOCAL_HEADS):
            turned_s[head, place] = turned_part[head * HEAD_DIM : (head + 1) * HEAD_DIM]
    for turn in range(ROW):
        head = lax.rem(row_place() + turn, ROW)
        own_refs[turn][...] = turned_s[head]
        far_refs[turn][...] = turned_s[head, : PAIR[0]]


def pack(keys, values, queries, grads):
    outs = pl.pallas_call(
        pack_kernel,
        in_specs=[IN_VMEM] * 4,
        out_specs=[IN_VMEM] * (2 * ROW),
        out_shape=[jax.ShapeDtypeStruct((4 * HEAD_DIM, T), BF16)] * ROW
        + [jax.ShapeDtypeStruct(PAIR, BF16)] * ROW,
        scratch_shapes=[pltpu.VMEM((LOCAL_HEADS, 4 * HEAD_DIM, T), BF16)],
        name="pack",
    )(keys, values, queries, grads)
    return outs[:ROW], outs[ROW:]


def attention_kernel(docs_ref, *refs):
    arrived, outs = refs[: 2 * ROW], refs[2 * ROW :]
    out_ref, back_refs, (own_s, far_s, qg_s, kv_s) = outs[0], outs[1 : ROW + 1], outs[ROW + 1 :]
    for turn in range(ROW):
        block = lax.rem(row_place() - turn + ROW, ROW)
        kv_s[ROW + block] = arrived[turn][: PAIR[0]]
        qg_s[block] = arrived[turn][PAIR[0] :]
        kv_s[block] = arrived[ROW + turn][...]
    first_block = lax.div(seq_index(), ROW) * ROW
    later = iota((T, T), 1) > iota((T, T), 0)
    scale = HEAD_DIM ** (-0.5)

    def doc_row(block):
        place = first_block + block
        row = doc_row_of(docs_ref, jnp.maximum(place, 0))
        return row if block >= 0 else jnp.where(place < 0, -1.0, row)

    rows = {block: doc_row(block) for block in range(-ROW, ROW)}
    for i in range(ROW):
        own_doc = columns_of(rows[i])
        qt, gt = qg_s[i, K_AT], qg_s[i, V_AT]
        q, g = jnp.transpose(qt), jnp.transpose(gt)

        def part(gap, place):
            return kv_s[ROW + i - gap, place]

        scores = []
        top = None
        for gap in range(ROW + 1):
            same = own_doc == rows[i - gap]
            if gap == 0:
                same = same & jnp.logical_not(later)
            if gap == ROW:
                same = same & later
            s = jnp.where(same, dot(q, part(gap, K_AT)) * (scale * LOG2E), NEG)
            scores.append(s)
            top = s if top is None else jnp.maximum(top, s)
        top = jnp.max(top, axis=1, keepdims=True)
        expos = [jnp.exp2(s - top) for s in scores]
        total = jnp.sum(sum(expos), axis=1, keepdims=True)
        inverse = 1.0 / jnp.maximum(total, 1.0)
        probs = [e * inverse for e in expos]
        halves = [p.astype(BF16) for p in probs]
        dprobs = [dot(g, part(gap, V_AT)) for gap in range(ROW + 1)]
        delta = sum(h.astype(F32) * d for h, d in zip(halves, dprobs))
        delta = jnp.sum(delta, axis=1, keepdims=True)
        dq = jnp.zeros((HEAD_DIM, T), F32)
        for gap in range(ROW + 1):
            dscore = (probs[gap] * (dprobs[gap] - delta)).astype(BF16)
            dq = dq + dot(part(gap, K_AT), dscore, NT)
            block = i - gap
            ref, index = (own_s, block) if block >= 0 else (far_s, block + ROW)
            dk, dv = dot(qt, dscore), dot(gt, halves[gap])
            if gap == 0 or (block < 0 and i == 0):
                ref[index, K_AT] = dk
                ref[index, V_AT] = dv
            else:
                ref[index, K_AT] += dk
                ref[index, V_AT] += dv
        out_ref[i, Q_AT] = (dq * scale).astype(BF16)
    for block in range(ROW):
        out_ref[block, : PAIR[0]] = own_s[block].astype(BF16)
    for turn in range(ROW):
        block = lax.rem(row_place() + turn, ROW)
        back_refs[turn][...] = far_s[block].astype(BF16)


def attention(docs, own, far):
    outs = pl.pallas_call(
        attention_kernel,
        in_specs=[IN_VMEM] * (1 + 2 * ROW),
        out_specs=[IN_VMEM] * (1 + ROW),
        out_shape=[jax.ShapeDtypeStruct((ROW, 3 * HEAD_DIM, T), BF16)]
        + [jax.ShapeDtypeStruct(PAIR, BF16)] * ROW,
        scratch_shapes=[
            pltpu.VMEM((ROW, *PAIR), F32),
            pltpu.VMEM((ROW, *PAIR), F32),
            pltpu.VMEM((ROW, *PAIR), BF16),
            pltpu.VMEM((2 * ROW, *PAIR), BF16),
        ],
        cost_estimate=pl.CostEstimate(flops=12 * 10**9, bytes_accessed=8 * 10**6, transcendentals=0),
        name="attention",
    )(docs, *own, *far)
    return outs[0], outs[1:]


def unpack_kernel(own_ref, *refs):
    back_refs, (dq_ref, dk_ref, dv_ref, back_s) = refs[:ROW], refs[ROW:]
    for turn, ref in enumerate(back_refs):
        back_s[lax.rem(row_place() - turn + ROW, ROW)] = ref[...]
    join = jnp.concatenate
    heads = range(LOCAL_HEADS)
    dq_ref[...] = jnp.transpose(join([own_ref[h, Q_AT] for h in heads], axis=0))
    for ref, place, scale in ((dk_ref, K_AT, HEAD_DIM ** (-0.5)), (dv_ref, V_AT, 1.0)):
        own = join([own_ref[h, place] for h in heads], axis=0).astype(F32)
        back = join([back_s[h, place] for h in heads], axis=0).astype(F32)
        ref[...] = jnp.transpose(((own + back) * scale).astype(BF16))


def unpack(own, back):
    wide = jax.ShapeDtypeStruct((T, LOCAL_HEADS * HEAD_DIM), BF16)
    return pl.pallas_call(
        unpack_kernel,
        in_specs=[IN_VMEM] * (1 + ROW),
        out_specs=[IN_VMEM] * 3,
        out_shape=[wide] * 3,
        scratch_shapes=[pltpu.VMEM((ROW, *PAIR), BF16)],
        cost_estimate=pl.CostEstimate(flops=2 * 10**9, bytes_accessed=4 * 10**6, transcendentals=0),
        name="unpack",
    )(own, *back)


def passed_along(value, axis, steps):
    count = lax.axis_size(axis)
    initial, last = (max(0, -steps), min(count, count - steps))
    return lax.ppermute(value, axis, [(source, source + steps) for source in range(initial, last)])


def turns(parts, axis):
    count = lax.axis_size(axis)
    return [parts[0]] + [
        lax.ppermute(part, axis, [(n, (n + turn) % count) for n in range(count)])
        for turn, part in enumerate(parts[1:], 1)
    ]


def to_row(part, rows, turn):
    pairs = []
    for shard in range(SHARDS):
        row, place = shard // ROW + rows, (shard + turn) % ROW
        if 0 <= row < SHARDS // ROW:
            pairs.append((shard, row * ROW + place))
    return lax.ppermute(part, SEQ, pairs)


def exchange(array, axis):
    return lax.all_to_all(array, axis, split_axis=0, concat_axis=0, tiled=True)


def local(
    queries, keys, values, attn_grad, doc_ids, conv_input, conv_weight, step_raw, step_bias,
    rate_log, skip_gain, input_coeff, output_coeff, gate_input, mix_grad,
):
    heads = step_raw.shape[1]
    docs = doc_ids.reshape(SHARDS * T // 128, 128)
    halo = passed_along(conv_input[T - 8 :], SEQ, 1)
    own_parts, far_parts = pack(keys, values, queries, attn_grad)
    own = turns(own_parts, "seq_2")
    far = [to_row(part, 1, turn) for turn, part in enumerate(far_parts)]

    mixer_args = (
        conv_input, halo, conv_weight, gate_input, mix_grad, step_raw.T,
        step_bias.reshape(1, heads), rate_log.reshape(1, heads), skip_gain.reshape(1, heads),
        docs, input_coeff, output_coeff,
    )
    parts = mixer_first(*mixer_args).reshape(SHARDS, SLOT, 128)
    gathered = exchange(parts, SEQ)
    scanned = chain(gathered)
    entering = exchange(scanned, SEQ).reshape(COLS, 128)
    out, back = attention(docs, own, far)
    swapped = exchange(out, "seq_2")
    returned = [to_row(part, -1, turn) for turn, part in enumerate(back)]
    dx, tail, spill, dgate, dstep, coeff, bundle = mixer_second(*mixer_args, entering)
    spilled = passed_along(spill, SEQ, -1)
    bundles = exchange(bundle, SEQ)
    coeffs = turns([coeff] * LOCAL_HEADS, "head")
    dq, dk, dv = unpack(swapped, returned)
    grad_weight, grad_bias, grad_rate, grad_skip, sum_in, sum_out = finish(bundles, coeffs, heads)
    tail = (tail + spilled).astype(BF16)
    grad_conv = lax.dynamic_update_slice_in_dim(dx, tail, T - 8, 0)
    return (
        dq, dk, dv, grad_conv, dgate, dstep.T, sum_in, sum_out, grad_weight,
        grad_bias.reshape(heads), grad_rate.reshape(heads), grad_skip.reshape(heads),
    )


def solution(mesh):
    finer = Mesh(
        mesh.devices.reshape(4, 2, 4, mesh.shape["head"]), ("seq_0", "seq_1", "seq_2", "head")
    )
    wide = P(SEQ, "head")
    return jax.shard_map(
        local,
        mesh=finer,
        in_specs=(
            wide, wide, wide, wide, P(), wide, P(None, "head"), wide, P("head"), P("head"),
            P("head"), P(SEQ, None), P(SEQ, None), wide, wide,
        ),
        out_specs=(
            wide, wide, wide, wide, wide, wide, P(SEQ, None), P(SEQ, None), P(None, "head"),
            P("head"), P("head"), P("head"),
        ),
        check_vma=False,
    )
```

```python
import jax
import jax.numpy as jnp
from jax import lax
from jax.experimental import pallas as pl
from jax.experimental.pallas import tpu as pltpu
from jax.sharding import Mesh
from jax.sharding import PartitionSpec as P


HEAD_DIM = 224
STATE = 64
KERNEL = 4
SEQ = ("seq_0", "seq_1", "seq_2")
SHARDS = 32
T = 256
LOCAL_HEADS = 4
BLK = 256
HALF = T // 2
HEADS_BLK = BLK // 64
COLS = 1792
STEPS = COLS // BLK
NEG = -1e30
LOG2E = 1.4426950408889634
F32 = jnp.float32
BF16 = jnp.bfloat16

NN = (((1,), (0,)), ((), ()))
NT = (((1,), (1,)), ((), ()))
TN = (((0,), (0,)), ((), ()))


def dot(a, b, dims=NN):
    return lax.dot_general(a, b, dims, preferred_element_type=F32)


def exact(a, b, dims=NN):
    return lax.dot_general(
        a, b, dims, preferred_element_type=F32, precision=lax.Precision.HIGHEST
    )


def split(a, pieces):
    parts = []
    for _ in range(pieces):
        part = a.astype(BF16)
        parts.append(part)
        a = a - part.astype(F32)
    return parts


def sigmoid(v):
    return 0.5 + 0.5 * jnp.tanh(0.5 * v)


def iota(shape, dim):
    return lax.broadcasted_iota(jnp.int32, shape, dim)


def columns_of(row):
    return jnp.transpose(jnp.broadcast_to(row, (T, T)))


def whole(shape):
    return pl.BlockSpec(shape, lambda c: (0,) * len(shape))


def column_block(rows):
    return pl.BlockSpec((rows, BLK), lambda c: (0, c))


IN_SMEM = pl.BlockSpec(memory_space=pltpu.SMEM)
IN_VMEM = pl.BlockSpec(memory_space=pltpu.VMEM)


def seq_index():
    index = 0
    for axis in SEQ:
        index = index * lax.axis_size(axis) + lax.axis_index(axis)
    return index


def row_place():
    return lax.axis_index(SEQ[-1])


def doc_row_of(docs_ref, shard):
    return jnp.concatenate(
        [docs_ref[pl.ds(2 * shard + part, 1), :] for part in range(2)], axis=1
    ).astype(F32)


def doc_rows(docs_ref):
    shard = seq_index()
    own = doc_row_of(docs_ref, shard)
    before = doc_row_of(docs_ref, jnp.maximum(shard - 1, 0))
    return own, jnp.where(shard == 0, -1.0, before)


def group_halves(coeff_ref):
    coeff = coeff_ref[...].astype(F32)
    turned = pltpu.roll(coeff, STATE, 1)
    first = lax.axis_index("head") < 2
    low = iota((T, 128), 1) < STATE
    mine_low = jnp.where(low, jnp.where(first, coeff, turned), 0.0)
    mine_high = jnp.where(low, 0.0, jnp.where(first, turned, coeff))
    return mine_low.astype(BF16), mine_high.astype(BF16)


def padded_params(bias_ref, rate_ref, skip_ref, params_s):
    heads = bias_ref.shape[1]
    params_s[...] = jnp.zeros((8, 128), F32)
    for n, ref in enumerate((bias_ref, rate_ref, skip_ref)):
        params_s[n : n + 1, 0:heads] = ref[...]
    return params_s[...]


def raw_steps(step_ref):
    rows = step_ref.shape[0]
    filled = jnp.concatenate([step_ref[...], jnp.zeros((128 - rows, T), F32)], axis=0)
    return jnp.transpose(filled)


def step_and_decay(raw, params):
    step = jnp.maximum(raw, 0.0) + jnp.log1p(jnp.exp(-jnp.abs(raw)))
    return step, -step * jnp.exp(params[1:2])


def token_setup(docs_ref, step_ref, params, cum_s, step_s, mask_s, prev_s, end_s):
    own_row, before_row = doc_rows(docs_ref)
    own = columns_of(own_row)
    lane = iota((8, T), 1)
    own8 = jnp.broadcast_to(own_row, (8, T))
    before8 = jnp.broadcast_to(before_row, (8, T))
    for lag in range(1, KERNEL):
        lagged = jnp.where(lane < lag, pltpu.roll(before8, lag, 1), pltpu.roll(own8, lag, 1))
        mask_s[lag - 1] = jnp.where(own == columns_of(lagged[0:1]), 1.0, 0.0)
    prev_s[...] = jnp.where(own == before_row[:, T - 1 : T], 0.0, NEG)
    end_s[...] = jnp.where(own == own_row[:, T - 1 : T], 0.0, NEG)
    raw = raw_steps(step_ref) + params[0:1]
    step, decay = step_and_decay(raw, params)
    lower = jnp.where(iota((T, T), 0) >= iota((T, T), 1), 1.0, 0.0)
    cum = exact(lower, decay) * LOG2E
    for n, part in enumerate(split(cum, 3)):
        cum_s[n] = part
    for n, part in enumerate(split(step, 2)):
        step_s[n] = part
    return own, own_row, cum


def spread_of(step_id):
    head = iota((128, BLK), 0)
    owner = step_id * HEADS_BLK + iota((128, BLK), 1) // 64
    return jnp.where(head == owner, 1.0, 0.0).astype(BF16)


def block_gains(step_id, cum_s, step_s, prev_s, end_s):
    spread = spread_of(step_id)
    cum = dot(cum_s[0], spread) + dot(cum_s[1], spread) + dot(cum_s[2], spread)
    step = dot(step_s[0], spread) + dot(step_s[1], spread)
    enter = jnp.exp2(cum + prev_s[...])
    to_end = jnp.exp2(cum[T - 1 : T] - cum + end_s[...])
    return spread, cum, step, enter, to_end


def conv_pre(x, halo, weight, mask_s):
    extended = jnp.concatenate([halo.astype(F32), x.astype(F32)], axis=0)
    shifted = [extended[8:]]
    summed = weight[0:1] * shifted[0]
    for lag in range(1, KERNEL):
        moved = pltpu.roll(extended, lag, 0)[8:] * mask_s[lag - 1]
        shifted.append(moved)
        summed = summed + weight[lag : lag + 1] * moved
    return summed, shifted


ROWS = COLS // SHARDS
GROUPS8 = ROWS // 8
SLOT = ROWS + 8


def mixer_first_kernel(
    x_ref, halo_ref, weight_ref, gate_ref, grad_ref, step_ref, bias_ref, rate_ref,
    skip_ref, docs_ref, in_ref, out_ref,
    parts_ref,
    cum_s, step_s, mask_s, prev_s, end_s, params_s, state_s, in_s, out_s,
):
    step_id = pl.program_id(0)

    @pl.when(step_id == 0)
    def _():
        params = padded_params(bias_ref, rate_ref, skip_ref, params_s)
        cum = token_setup(
            docs_ref, step_ref, params, cum_s, step_s, mask_s, prev_s, end_s
        )[2]
        through = jnp.exp2(cum[T - 1 : T] + prev_s[T - 1 : T, 0:1])
        high, low = split(through, 2)
        row = iota((8, 128), 0)
        both = jnp.where(row == 0, high.astype(F32), jnp.where(row == 1, low.astype(F32), 0.0))
        for shard in range(SHARDS):
            state_s[SLOT * shard + ROWS : SLOT * (shard + 1)] = both
        in_s[...] = group_halves(in_ref)[0]
        out_s[...] = group_halves(out_ref)[1]

    _, _, step, enter, to_end = block_gains(step_id, cum_s, step_s, prev_s, end_s)
    pre, _ = conv_pre(x_ref[...], halo_ref[...], weight_ref[...], mask_s)
    act = pre * sigmoid(pre)
    gate = gate_ref[...].astype(F32)
    out_grad = grad_ref[...].astype(F32) * gate * sigmoid(gate)
    ended = (act * step * to_end).astype(BF16)
    entered = (out_grad * enter).astype(BF16)
    state = dot(ended, in_s[...], TN) + dot(entered, out_s[...], TN)
    for part in range(BLK // 8):
        place = step_id * (BLK // 8) + part
        target = lax.div(place, GROUPS8)
        offset = SLOT * target + 8 * (place - GROUPS8 * target)
        state_s[pl.ds(pl.multiple_of(offset, 8), 8), :] = state[8 * part : 8 * part + 8]

    @pl.when(step_id == STEPS - 1)
    def _():
        parts_ref[...] = state_s[...].astype(BF16)


TOKEN_SCRATCH = [
    pltpu.VMEM((3, T, 128), BF16),
    pltpu.VMEM((2, T, 128), BF16),
    pltpu.VMEM((KERNEL - 1, T, BLK), F32),
    pltpu.VMEM((T, BLK), F32),
    pltpu.VMEM((T, BLK), F32),
    pltpu.VMEM((8, 128), F32),
]


def mixer_specs(heads):
    return [
        column_block(T), column_block(8), column_block(KERNEL), column_block(T),
        column_block(T), whole((heads, T)), whole((1, heads)), whole((1, heads)),
        whole((1, heads)), whole((SHARDS * T // 128, 128)), whole((T, 128)), whole((T, 128)),
    ]


def mixer_first(*arrays):
    heads = arrays[5].shape[0]
    return pl.pallas_call(
        mixer_first_kernel,
        grid=(STEPS,),
        in_specs=mixer_specs(heads),
        out_specs=whole((SHARDS * SLOT, 128)),
        out_shape=jax.ShapeDtypeStruct((SHARDS * SLOT, 128), BF16),
        scratch_shapes=TOKEN_SCRATCH + [
            pltpu.VMEM((SHARDS * SLOT, 128), F32),
            pltpu.VMEM((T, 128), BF16),
            pltpu.VMEM((T, 128), BF16),
        ],
        cost_estimate=pl.CostEstimate(flops=8 * 10**9, bytes_accessed=4 * 10**6, transcendentals=0),
        name="mixer_first",
    )(*arrays)


def chain_kernel(parts_ref, out_ref, forward_s):
    slot = seq_index()
    owner = (slot * ROWS + iota((ROWS, 128), 0)) // 64
    choose = jnp.where(owner == iota((ROWS, 128), 1), 1.0, 0.0)
    lane = iota((ROWS, 128), 1)
    through = []
    carry = jnp.zeros((ROWS, 128), F32)
    for shard in range(SHARDS):
        row = parts_ref[shard, ROWS : ROWS + 1].astype(F32)
        row = row + parts_ref[shard, ROWS + 1 : ROWS + 2].astype(F32)
        gain = jnp.sum(choose * row, axis=1, keepdims=True)
        through.append(gain)
        forward_s[shard] = carry
        carry = gain * carry + parts_ref[shard, 0:ROWS].astype(F32)
    carry = jnp.zeros((ROWS, 128), F32)
    for shard in reversed(range(SHARDS)):
        out_ref[shard] = jnp.where(lane < STATE, forward_s[shard], carry).astype(BF16)
        carry = through[shard] * carry + parts_ref[shard, 0:ROWS].astype(F32)


def chain(parts):
    return pl.pallas_call(
        chain_kernel,
        in_specs=[IN_VMEM],
        out_specs=IN_VMEM,
        out_shape=jax.ShapeDtypeStruct((SHARDS, ROWS, 128), BF16),
        scratch_shapes=[pltpu.VMEM((SHARDS, ROWS, 128), F32)],
        cost_estimate=pl.CostEstimate(flops=2 * 10**9, bytes_accessed=10**6, transcendentals=0),
        name="chain",
    )(parts)


BUNDLE = KERNEL * COLS // 128
LANES_BLK = BLK // 128


def mixer_second_kernel(
    x_ref, halo_ref, weight_ref, gate_ref, grad_ref, step_ref, bias_ref, rate_ref,
    skip_ref, docs_ref, in_ref, out_ref, state_ref,
    dx_ref, tail_ref, spill_ref, dgate_ref, dstep_ref, coeff_ref, bundle_ref,
    cum_s, step_s, mask_s, prev_s, end_s, params_s,
    cumt_s, pair_s, causal_s, dtop_s, dbottom_s, coeff_s, row_s, dt_s, ends_s, bundle_s,
    in_low_s, in_high_s, out_low_s, out_high_s,
):
    step_id = pl.program_id(0)
    lane = iota((T, 128), 1)

    @pl.when(step_id == 0)
    def _():
        params = padded_params(bias_ref, rate_ref, skip_ref, params_s)
        own, own_row, cum = token_setup(
            docs_ref, step_ref, params, cum_s, step_s, mask_s, prev_s, end_s
        )
        cumt_s[...] = jnp.transpose(cum)
        same = (own == own_row) & (iota((T, T), 0) >= iota((T, T), 1))
        causal_s[...] = jnp.where(same, 0.0, NEG)
        in_low_s[...], in_high_s[...] = group_halves(in_ref)
        out_low_s[...], out_high_s[...] = group_halves(out_ref)
        pair_s[...] = dot(out_low_s[...], in_low_s[...], NT)
        dtop_s[...] = jnp.zeros((HALF, HALF), F32)
        dbottom_s[...] = jnp.zeros((HALF, T), F32)
        coeff_s[...] = jnp.zeros((T, 128), F32)
        row_s[...] = jnp.zeros((T, 128), F32)
        dt_s[...] = jnp.zeros((T, 128), F32)
        ends_s[...] = jnp.zeros((8, 128), F32)

    out_low = out_low_s[...]
    in_high = in_high_s[...]
    spread, cum, step, enter, to_end = block_gains(step_id, cum_s, step_s, prev_s, end_s)
    skip = sum(dot(part, spread) for part in split(params_s[...], 3))[2:3]
    weight = weight_ref[...]
    pre, shifted = conv_pre(x_ref[...], halo_ref[...], weight, mask_s)
    sig = sigmoid(pre)
    act = pre * sig
    gate = gate_ref[...].astype(F32)
    gate_sig = sigmoid(gate)
    mix_grad = grad_ref[...].astype(F32)
    out_grad = mix_grad * gate * gate_sig
    scaled = act * step
    scaled_half = scaled.astype(BF16)
    grad_half = out_grad.astype(BF16)

    block_head = iota((T, BLK), 1) // 64
    tops, bottoms, scaled_parts, grad_parts = [], [], [], []
    dtop, dbottom = dtop_s[...], dbottom_s[...]
    for k in range(HEADS_BLK):
        mine = block_head == k
        cum_col = cum[:, 64 * k : 64 * k + 1]
        cum_row = cumt_s[pl.ds(step_id * HEADS_BLK + k, 1), :]
        top = jnp.exp2(
            jnp.broadcast_to(cum_col[:HALF], (HALF, HALF)) - cum_row[:, :HALF]
            + causal_s[:HALF, :HALF]
        )
        bottom = jnp.exp2(
            jnp.broadcast_to(cum_col[HALF:], (HALF, T)) - cum_row + causal_s[HALF:, :]
        )
        tops.append((pair_s[:HALF, :HALF] * top).astype(BF16))
        bottoms.append((pair_s[HALF:, :] * bottom).astype(BF16))
        scaled_k = jnp.where(mine, scaled_half, jnp.zeros_like(scaled_half))
        grad_k = jnp.where(mine, grad_half, jnp.zeros_like(grad_half))
        scaled_parts.append(scaled_k)
        grad_parts.append(grad_k)
        dtop = dtop + dot(grad_k[:HALF], scaled_half[:HALF], NT) * top
        dbottom = dbottom + dot(grad_k[HALF:], scaled_half, NT) * bottom
    dtop_s[...] = dtop
    dbottom_s[...] = dbottom
    join = jnp.concatenate
    inner = join(
        [
            dot(join(tops, axis=1), join([v[:HALF] for v in scaled_parts], axis=0)),
            dot(join(bottoms, axis=1), join(scaled_parts, axis=0)),
        ],
        axis=0,
    )
    upper_part = dot(join(tops, axis=0), join([v[:HALF] for v in grad_parts], axis=0), TN)
    dscaled = dot(join(bottoms, axis=0), join([v[HALF:] for v in grad_parts], axis=0), TN)
    dscaled = join([dscaled[:HALF] + upper_part, dscaled[HALF:]], axis=0)

    state = state_ref[...]
    carried = dot(out_low, state, NT) * enter
    from_end = dot(in_high, state, NT) * to_end
    ssm_out = inner + carried
    dscaled = dscaled + from_end
    mixed_out = ssm_out + skip * act
    dgate_ref[...] = (
        mix_grad * mixed_out * gate_sig * (1.0 + gate * (1.0 - gate_sig))
    ).astype(BF16)

    gave_out = dot((out_grad * enter).astype(BF16), state)
    gave_in = dot((scaled * to_end).astype(BF16), state)
    coeff_s[...] += jnp.where(lane < STATE, gave_out, gave_in)

    grad_round = grad_half.astype(F32)
    scaled_round = scaled_half.astype(F32)
    balance = grad_round * ssm_out - scaled_round * dscaled
    row_s[...] += sum(dot(part, spread, NT) for part in split(balance, 2))
    dt_s[...] += dot((dscaled * act).astype(BF16), spread, NT)

    state_wide = state.astype(F32)
    product = state_wide * pltpu.roll(state_wide, STATE, 1)
    through = jnp.sum(jnp.where(iota((BLK, 128), 1) < STATE, product, 0.0), axis=1, keepdims=True)
    through_row = jnp.transpose(jnp.broadcast_to(through, (BLK, BLK)))[0:1]
    end_row = jnp.sum(scaled_round * from_end, axis=0, keepdims=True)
    end_row = end_row + through_row * enter[T - 1 : T]
    skip_row = jnp.sum(out_grad * act, axis=0, keepdims=True)
    row8 = iota((8, BLK), 0)
    both = jnp.where(row8 == 0, end_row, jnp.where(row8 == 1, skip_row, 0.0))
    ends_s[...] += sum(dot(part, spread, NT) for part in split(both, 3))

    dact = step * dscaled + skip * out_grad
    dpre = dact * sig * (1.0 + pre * (1.0 - sig))
    zeros = jnp.zeros((8, BLK), F32)
    dx = weight[0:1] * dpre
    spill = zeros
    for lag in range(KERNEL):
        tap = jnp.sum(dpre * shifted[lag], axis=0, keepdims=True)
        for m in range(LANES_BLK):
            place = lag * (COLS // 128) + step_id * LANES_BLK + m
            bundle_s[pl.ds(place, 1), :] = tap[:, 128 * m : 128 * (m + 1)]
        if lag == 0:
            continue
        masked = dpre * mask_s[lag - 1]
        later = pltpu.roll(jnp.concatenate([masked, zeros], axis=0), T + 8 - lag, 0)[:T]
        dx = dx + weight[lag : lag + 1] * later
        edge = pltpu.roll(jnp.concatenate([zeros, masked[:8]], axis=0), 16 - lag, 0)[:8]
        spill = spill + weight[lag : lag + 1] * edge
    dx_ref[...] = dx.astype(BF16)
    tail_ref[...] = dx[T - 8 :]
    spill_ref[...] = spill

    @pl.when(step_id == STEPS - 1)
    def _():
        params = params_s[...]
        raw = raw_steps(step_ref) + params[0:1]
        rate = jnp.exp(params[1:2])
        decay = step_and_decay(raw, params)[1]
        upper = jnp.where(iota((T, T), 1) >= iota((T, T), 0), 1.0, 0.0)
        ends = ends_s[...]
        ddecay = exact(upper, row_s[...]) + ends[0:1]
        dstep = (dt_s[...] - ddecay * rate) * sigmoid(raw)
        dstep_ref[...] = jnp.transpose(dstep)[: dstep_ref.shape[0]]
        dbias = jnp.sum(dstep, axis=0, keepdims=True)
        drate = jnp.sum(ddecay * decay, axis=0, keepdims=True)
        row = iota((8, 128), 0)
        small = jnp.zeros((8, 128), F32)
        for n, vector in enumerate((dbias, drate, ends[1:2])):
            for m, part in enumerate(split(vector, 2)):
                small = jnp.where(row == 2 * n + m, part.astype(F32), small)
        bundle_s[BUNDLE : BUNDLE + 8] = small
        bundle = bundle_s[...].astype(BF16)
        for shard in range(SHARDS):
            bundle_ref[shard] = bundle
        top_half, bottom_half = dtop.astype(BF16), dbottom.astype(BF16)
        in_low, out_high = in_low_s[...], out_high_s[...]
        out_part = join([dot(top_half, in_low[:HALF]), dot(bottom_half, in_low)], axis=0)
        in_part = dot(bottom_half, out_high[HALF:], TN)
        in_part = join(
            [in_part[:HALF] + dot(top_half, out_high[:HALF], TN), in_part[HALF:]], axis=0
        )
        coeff_ref[...] = (coeff_s[...] + out_part + in_part).astype(BF16)


def mixer_second(*arrays):
    heads = arrays[5].shape[0]
    half = pltpu.VMEM((T, 128), BF16)
    return pl.pallas_call(
        mixer_second_kernel,
        grid=(STEPS,),
        in_specs=mixer_specs(heads) + [pl.BlockSpec((BLK, 128), lambda c: (c, 0))],
        out_specs=[
            column_block(T), column_block(8), column_block(8), column_block(T),
            whole((heads, T)), whole((T, 128)), whole((SHARDS, BUNDLE + 8, 128)),
        ],
        out_shape=[
            jax.ShapeDtypeStruct((T, COLS), BF16),
            jax.ShapeDtypeStruct((8, COLS), F32),
            jax.ShapeDtypeStruct((8, COLS), F32),
            jax.ShapeDtypeStruct((T, COLS), BF16),
            jax.ShapeDtypeStruct((heads, T), F32),
            jax.ShapeDtypeStruct((T, 128), BF16),
            jax.ShapeDtypeStruct((SHARDS, BUNDLE + 8, 128), BF16),
        ],
        scratch_shapes=TOKEN_SCRATCH + [
            pltpu.VMEM((128, T), F32),
            pltpu.VMEM((T, T), F32),
            pltpu.VMEM((T, T), F32),
            pltpu.VMEM((HALF, HALF), F32),
            pltpu.VMEM((HALF, T), F32),
            pltpu.VMEM((T, 128), F32),
            pltpu.VMEM((T, 128), F32),
            pltpu.VMEM((T, 128), F32),
            pltpu.VMEM((8, 128), F32),
            pltpu.VMEM((BUNDLE + 8, 128), F32),
            half, half, half, half,
        ],
        cost_estimate=pl.CostEstimate(flops=18 * 10**9, bytes_accessed=8 * 10**6, transcendentals=0),
        name="mixer_second",
    )(*arrays)


def finish_kernel(bundle_ref, *refs):
    coeff_refs = refs[:LOCAL_HEADS]
    weight_ref, bias_ref, rate_ref, skip_ref, in_ref, out_ref, coeff_s = refs[LOCAL_HEADS:]
    for turn, ref in enumerate(coeff_refs):
        coeff_s[lax.rem(lax.axis_index("head") - turn + LOCAL_HEADS, LOCAL_HEADS)] = ref[...].astype(F32)
    total = bundle_ref[0].astype(F32)
    for shard in range(1, SHARDS):
        total = total + bundle_ref[shard].astype(F32)
    tiles = COLS // 128
    for lag in range(KERNEL):
        for m in range(tiles):
            weight_ref[lag : lag + 1, 128 * m : 128 * (m + 1)] = total[
                lag * tiles + m : lag * tiles + m + 1
            ]
    for n, ref in enumerate((bias_ref, rate_ref, skip_ref)):
        row = BUNDLE + 2 * n
        ref[...] = (total[row : row + 1] + total[row + 1 : row + 2])[:, : ref.shape[1]]
    low, high = coeff_s[0] + coeff_s[1], coeff_s[2] + coeff_s[3]
    left = iota((T, 128), 1) < STATE
    out_ref[...] = jnp.where(left, low, pltpu.roll(high, STATE, 1))
    in_ref[...] = jnp.where(left, pltpu.roll(low, STATE, 1), high)


def finish(bundle, coeffs, heads):
    small = jax.ShapeDtypeStruct((1, heads), F32)
    wide = jax.ShapeDtypeStruct((T, 128), F32)
    return pl.pallas_call(
        finish_kernel,
        in_specs=[IN_VMEM] * (1 + LOCAL_HEADS),
        out_specs=[IN_VMEM] * 6,
        out_shape=[jax.ShapeDtypeStruct((KERNEL, COLS), F32), small, small, small, wide, wide],
        scratch_shapes=[pltpu.VMEM((LOCAL_HEADS, T, 128), F32)],
        name="finish",
    )(bundle, *coeffs)


ROW = 4
K_AT, V_AT, Q_AT, G_AT = (slice(n * HEAD_DIM, (n + 1) * HEAD_DIM) for n in range(4))
PAIR = (2 * HEAD_DIM, T)


def pack_kernel(k_ref, v_ref, q_ref, g_ref, *refs):
    out_refs, turned_s = refs[:ROW], refs[ROW]
    for ref, place in ((k_ref, K_AT), (v_ref, V_AT), (q_ref, Q_AT), (g_ref, G_AT)):
        turned_part = jnp.transpose(ref[...])
        for head in range(LOCAL_HEADS):
            turned_s[head, place] = turned_part[head * HEAD_DIM : (head + 1) * HEAD_DIM]
    for turn in range(ROW):
        out_refs[turn][...] = turned_s[lax.rem(row_place() + turn, ROW)]


def pack(keys, values, queries, grads):
    return pl.pallas_call(
        pack_kernel,
        in_specs=[IN_VMEM] * 4,
        out_specs=[IN_VMEM] * ROW,
        out_shape=[jax.ShapeDtypeStruct((4 * HEAD_DIM, T), BF16)] * ROW,
        scratch_shapes=[pltpu.VMEM((LOCAL_HEADS, 4 * HEAD_DIM, T), BF16)],
        name="pack",
    )(keys, values, queries, grads)


def lend_kernel(*refs):
    for turn, ref in enumerate(refs[:ROW]):
        refs[ROW][turn * PAIR[0] : (turn + 1) * PAIR[0]] = ref[: PAIR[0]]


def lend(own):
    return pl.pallas_call(
        lend_kernel,
        in_specs=[IN_VMEM] * ROW,
        out_specs=IN_VMEM,
        out_shape=jax.ShapeDtypeStruct((ROW * PAIR[0], T), BF16),
        name="lend",
    )(*own)


def attention_kernel(docs_ref, far_ref, *refs):
    arrived, (dq_ref, own_ref, back_ref, far_s, qg_s, kv_s) = refs[:ROW], refs[ROW:]
    for turn in range(ROW):
        block = lax.rem(row_place() - turn + ROW, ROW)
        kv_s[ROW + block] = arrived[turn][: PAIR[0]]
        qg_s[block] = arrived[turn][PAIR[0] :]
        kv_s[block] = far_ref[turn * PAIR[0] : (turn + 1) * PAIR[0]]
    first_block = lax.div(seq_index(), ROW) * ROW
    later = iota((T, T), 1) > iota((T, T), 0)
    scale = HEAD_DIM ** (-0.5)

    def doc_row(block):
        place = first_block + block
        row = doc_row_of(docs_ref, jnp.maximum(place, 0))
        return row if block >= 0 else jnp.where(place < 0, -1.0, row)

    rows = {block: doc_row(block) for block in range(-ROW, ROW)}
    for i in range(ROW):
        own_doc = columns_of(rows[i])
        qt, gt = qg_s[i, K_AT], qg_s[i, V_AT]
        q, g = jnp.transpose(qt), jnp.transpose(gt)

        def part(gap, place):
            return kv_s[ROW + i - gap, place]

        scores = []
        top = None
        for gap in range(ROW + 1):
            same = own_doc == rows[i - gap]
            if gap == 0:
                same = same & jnp.logical_not(later)
            if gap == ROW:
                same = same & later
            s = jnp.where(same, dot(q, part(gap, K_AT)) * (scale * LOG2E), NEG)
            scores.append(s)
            top = s if top is None else jnp.maximum(top, s)
        top = jnp.max(top, axis=1, keepdims=True)
        expos = [jnp.exp2(s - top) for s in scores]
        total = jnp.sum(sum(expos), axis=1, keepdims=True)
        inverse = 1.0 / jnp.maximum(total, 1.0)
        probs = [e * inverse for e in expos]
        halves = [p.astype(BF16) for p in probs]
        dprobs = [dot(g, part(gap, V_AT)) for gap in range(ROW + 1)]
        delta = sum(h.astype(F32) * d for h, d in zip(halves, dprobs))
        delta = jnp.sum(delta, axis=1, keepdims=True)
        dq = jnp.zeros((HEAD_DIM, T), F32)
        for gap in range(ROW + 1):
            dscore = (probs[gap] * (dprobs[gap] - delta)).astype(BF16)
            dq = dq + dot(part(gap, K_AT), dscore, NT)
            block = i - gap
            ref, index = (own_ref, block) if block >= 0 else (far_s, block + ROW)
            dk, dv = dot(qt, dscore), dot(gt, halves[gap])
            if gap == 0 or (block < 0 and i == 0):
                ref[index, K_AT] = dk
                ref[index, V_AT] = dv
            else:
                ref[index, K_AT] += dk
                ref[index, V_AT] += dv
            if gap == ROW:
                back_ref[index] = far_s[index].astype(BF16)
        dq_ref[i] = (dq * scale).astype(BF16)


def attention(docs, far, own):
    pairs = (ROW, *PAIR)
    return pl.pallas_call(
        attention_kernel,
        in_specs=[IN_VMEM] * (2 + ROW),
        out_specs=[IN_VMEM] * 3,
        out_shape=[
            jax.ShapeDtypeStruct((ROW, HEAD_DIM, T), BF16),
            jax.ShapeDtypeStruct(pairs, F32),
            jax.ShapeDtypeStruct(pairs, BF16),
        ],
        scratch_shapes=[
            pltpu.VMEM(pairs, F32),
            pltpu.VMEM(pairs, BF16),
            pltpu.VMEM((2 * ROW, *PAIR), BF16),
        ],
        cost_estimate=pl.CostEstimate(flops=12 * 10**9, bytes_accessed=8 * 10**6, transcendentals=0),
        name="attention",
    )(docs, far, *own)


def merge_kernel(dq_ref, dkv_ref, back_ref, *out_refs):
    scale = HEAD_DIM ** (-0.5)
    place = row_place()
    for turn, out_ref in enumerate(out_refs):
        block = lax.rem(place + turn, ROW)
        total = dkv_ref[block] + back_ref[block].astype(F32)
        out_ref[K_AT] = (total[K_AT] * scale).astype(BF16)
        out_ref[V_AT] = total[V_AT].astype(BF16)
        out_ref[Q_AT] = dq_ref[block]


def merge(dq, dkv, back):
    return pl.pallas_call(
        merge_kernel,
        in_specs=[IN_VMEM] * 3,
        out_specs=[IN_VMEM] * ROW,
        out_shape=[jax.ShapeDtypeStruct((3 * HEAD_DIM, T), BF16)] * ROW,
        cost_estimate=pl.CostEstimate(flops=3 * 10**9, bytes_accessed=4 * 10**6, transcendentals=0),
        name="merge",
    )(dq, dkv, back)


def unpack_kernel(*refs):
    parts, outs, stacked_s = refs[:ROW], refs[ROW : ROW + 3], refs[ROW + 3]
    place = row_place()
    for turn, part in enumerate(parts):
        source = lax.rem(place - turn + ROW, ROW)
        for n, at in enumerate((Q_AT, K_AT, V_AT)):
            stacked_s[n, source] = part[at]
    for n, ref in enumerate(outs):
        stacked = jnp.concatenate([stacked_s[n, h] for h in range(LOCAL_HEADS)], axis=0)
        ref[...] = jnp.transpose(stacked)


def unpack(parts):
    wide = jax.ShapeDtypeStruct((T, LOCAL_HEADS * HEAD_DIM), BF16)
    return pl.pallas_call(
        unpack_kernel,
        in_specs=[IN_VMEM] * ROW,
        out_specs=[IN_VMEM] * 3,
        out_shape=[wide] * 3,
        scratch_shapes=[pltpu.VMEM((3, LOCAL_HEADS, HEAD_DIM, T), BF16)],
        cost_estimate=pl.CostEstimate(flops=2 * 10**9, bytes_accessed=3 * 10**6, transcendentals=0),
        name="unpack",
    )(*parts)


def passed_along(value, axis, steps):
    count = lax.axis_size(axis)
    initial, last = (max(0, -steps), min(count, count - steps))
    return lax.ppermute(value, axis, [(source, source + steps) for source in range(initial, last)])


def turns(parts, axis):
    count = lax.axis_size(axis)
    return [parts[0]] + [
        lax.ppermute(part, axis, [(n, (n + turn) % count) for n in range(count)])
        for turn, part in enumerate(parts[1:], 1)
    ]


def near(array):
    return pltpu.with_memory_space_constraint(array, pltpu.VMEM)


def exchange(array, axis):
    return lax.all_to_all(array, axis, split_axis=0, concat_axis=0, tiled=True)


def local(
    queries, keys, values, attn_grad, doc_ids, conv_input, conv_weight, step_raw, step_bias,
    rate_log, skip_gain, input_coeff, output_coeff, gate_input, mix_grad,
):
    heads = step_raw.shape[1]
    docs = doc_ids.reshape(SHARDS * T // 128, 128)
    halo = passed_along(conv_input[T - 8 :], SEQ, 1)
    parts = pack(keys, values, queries, attn_grad)
    own = [near(v) for v in turns(parts, "seq_2")]
    lent = lend(own)
    far = passed_along(lent, SEQ, ROW)

    mixer_args = (
        conv_input, halo, conv_weight, gate_input, mix_grad, step_raw.T,
        step_bias.reshape(1, heads), rate_log.reshape(1, heads), skip_gain.reshape(1, heads),
        docs, input_coeff, output_coeff,
    )
    parts = mixer_first(*mixer_args).reshape(SHARDS, SLOT, 128)
    gathered = exchange(parts, SEQ)
    scanned = chain(near(gathered))
    entering = exchange(scanned, SEQ).reshape(COLS, 128)
    dq, dkv, back = attention(docs, near(far), own)
    returned = passed_along(back, SEQ, -ROW)
    dx, tail, spill, dgate, dstep, coeff, bundle = mixer_second(*mixer_args, entering)
    leaving = merge(dq, dkv, near(returned))
    swapped = turns(leaving, "seq_2")
    spilled = passed_along(spill, SEQ, -1)
    bundles = exchange(bundle, SEQ)
    coeffs = turns([coeff] * LOCAL_HEADS, "head")
    dq, dk, dv = unpack([near(v) for v in swapped])
    grad_weight, grad_bias, grad_rate, grad_skip, sum_in, sum_out = finish(
        near(bundles), [near(v) for v in coeffs], heads
    )
    tail = (tail + spilled).astype(BF16)
    grad_conv = lax.dynamic_update_slice_in_dim(dx, tail, T - 8, 0)
    return (
        dq, dk, dv, grad_conv, dgate, dstep.T, sum_in, sum_out, grad_weight,
        grad_bias.reshape(heads), grad_rate.reshape(heads), grad_skip.reshape(heads),
    )


def solution(mesh):
    finer = Mesh(
        mesh.devices.reshape(4, 2, 4, mesh.shape["head"]), ("seq_0", "seq_1", "seq_2", "head")
    )
    wide = P(SEQ, "head")
    return jax.shard_map(
        local,
        mesh=finer,
        in_specs=(
            wide, wide, wide, wide, P(), wide, P(None, "head"), wide, P("head"), P("head"),
            P("head"), P(SEQ, None), P(SEQ, None), wide, wide,
        ),
        out_specs=(
            wide, wide, wide, wide, wide, wide, P(SEQ, None), P(SEQ, None), P(None, "head"),
            P("head"), P("head"), P("head"),
        ),
        check_vma=False,
    )
```

```python
import jax
import jax.numpy as jnp
from jax import lax
from jax.experimental import pallas as pl
from jax.experimental.pallas import tpu as pltpu
from jax.sharding import Mesh
from jax.sharding import PartitionSpec as P


HEAD_DIM = 224
STATE = 64
KERNEL = 4
SEQ = ("seq_0", "seq_1", "seq_2")
SHARDS = 32
T = 256
LOCAL_HEADS = 4
BLK = 256
HALF = T // 2
HEADS_BLK = BLK // 64
COLS = 1792
STEPS = COLS // BLK
NEG = -1e30
LOG2E = 1.4426950408889634
F32 = jnp.float32
BF16 = jnp.bfloat16

NN = (((1,), (0,)), ((), ()))
NT = (((1,), (1,)), ((), ()))
TN = (((0,), (0,)), ((), ()))


def dot(a, b, dims=NN):
    return lax.dot_general(a, b, dims, preferred_element_type=F32)


def exact(a, b, dims=NN):
    return lax.dot_general(
        a, b, dims, preferred_element_type=F32, precision=lax.Precision.HIGHEST
    )


def split(a, pieces):
    parts = []
    for _ in range(pieces):
        part = a.astype(BF16)
        parts.append(part)
        a = a - part.astype(F32)
    return parts


def sigmoid(v):
    return 0.5 + 0.5 * jnp.tanh(0.5 * v)


def iota(shape, dim):
    return lax.broadcasted_iota(jnp.int32, shape, dim)


def columns_of(row):
    return jnp.transpose(jnp.broadcast_to(row, (T, T)))


def whole(shape):
    return pl.BlockSpec(shape, lambda c: (0,) * len(shape))


def column_block(rows):
    return pl.BlockSpec((rows, BLK), lambda c: (0, c))


IN_VMEM = pl.BlockSpec(memory_space=pltpu.VMEM)
GRANT = pltpu.CompilerParams(vmem_limit_bytes=32 * 2**20)


def seq_index():
    index = 0
    for axis in SEQ:
        index = index * lax.axis_size(axis) + lax.axis_index(axis)
    return index


def row_place():
    return lax.axis_index(SEQ[-1])


def doc_row_of(docs_ref, shard):
    return jnp.concatenate(
        [docs_ref[pl.ds(2 * shard + part, 1), :] for part in range(2)], axis=1
    ).astype(F32)


def doc_rows(docs_ref):
    shard = seq_index()
    own = doc_row_of(docs_ref, shard)
    before = doc_row_of(docs_ref, jnp.maximum(shard - 1, 0))
    return own, jnp.where(shard == 0, -1.0, before)


def group_halves(coeff_ref):
    coeff = coeff_ref[...].astype(F32)
    turned = pltpu.roll(coeff, STATE, 1)
    first = lax.axis_index("head") < 2
    low = iota((T, 128), 1) < STATE
    mine_low = jnp.where(low, jnp.where(first, coeff, turned), 0.0)
    mine_high = jnp.where(low, 0.0, jnp.where(first, turned, coeff))
    return mine_low.astype(BF16), mine_high.astype(BF16)


def padded_params(bias_ref, rate_ref, skip_ref, params_s):
    heads = bias_ref.shape[1]
    params_s[...] = jnp.zeros((8, 128), F32)
    for n, ref in enumerate((bias_ref, rate_ref, skip_ref)):
        params_s[n : n + 1, 0:heads] = ref[...]
    return params_s[...]


def raw_steps(step_ref):
    rows = step_ref.shape[0]
    filled = jnp.concatenate([step_ref[...], jnp.zeros((128 - rows, T), F32)], axis=0)
    return jnp.transpose(filled)


def step_and_decay(raw, params):
    step = jnp.maximum(raw, 0.0) + jnp.log1p(jnp.exp(-jnp.abs(raw)))
    return step, -step * jnp.exp(params[1:2])


def token_setup(docs_ref, step_ref, params, cum_s, step_s, mask_s, prev_s, end_s):
    own_row, before_row = doc_rows(docs_ref)
    own = columns_of(own_row)
    lane = iota((8, T), 1)
    own8 = jnp.broadcast_to(own_row, (8, T))
    before8 = jnp.broadcast_to(before_row, (8, T))
    for lag in range(1, KERNEL):
        lagged = jnp.where(lane < lag, pltpu.roll(before8, lag, 1), pltpu.roll(own8, lag, 1))
        mask_s[lag - 1] = jnp.where(own == columns_of(lagged[0:1]), 1.0, 0.0)
    prev_s[...] = jnp.where(own == before_row[:, T - 1 : T], 0.0, NEG)
    end_s[...] = jnp.where(own == own_row[:, T - 1 : T], 0.0, NEG)
    raw = raw_steps(step_ref) + params[0:1]
    step, decay = step_and_decay(raw, params)
    lower = jnp.where(iota((T, T), 0) >= iota((T, T), 1), 1.0, 0.0)
    cum = exact(lower, decay) * LOG2E
    for n, part in enumerate(split(cum, 3)):
        cum_s[n] = part
    for n, part in enumerate(split(step, 2)):
        step_s[n] = part
    return own, own_row, cum


def spread_of(step_id):
    head = iota((128, BLK), 0)
    owner = step_id * HEADS_BLK + iota((128, BLK), 1) // 64
    return jnp.where(head == owner, 1.0, 0.0).astype(BF16)


def block_gains(step_id, cum_s, step_s, prev_s, end_s):
    spread = spread_of(step_id)
    cum = dot(cum_s[0], spread) + dot(cum_s[1], spread) + dot(cum_s[2], spread)
    step = dot(step_s[0], spread) + dot(step_s[1], spread)
    enter = jnp.exp2(cum + prev_s[...])
    to_end = jnp.exp2(cum[T - 1 : T] - cum + end_s[...])
    return spread, cum, step, enter, to_end


def conv_pre(x, halo, weight, mask_s):
    extended = jnp.concatenate([halo.astype(F32), x.astype(F32)], axis=0)
    shifted = [extended[8:]]
    summed = weight[0:1] * shifted[0]
    for lag in range(1, KERNEL):
        moved = pltpu.roll(extended, lag, 0)[8:] * mask_s[lag - 1]
        shifted.append(moved)
        summed = summed + weight[lag : lag + 1] * moved
    return summed, shifted


ROWS = COLS // SHARDS
GROUPS8 = ROWS // 8
SLOT = ROWS + 8


def mixer_first_kernel(
    x_ref, halo_ref, weight_ref, gate_ref, grad_ref, step_ref, bias_ref, rate_ref,
    skip_ref, docs_ref, in_ref, out_ref,
    parts_ref,
    cum_s, step_s, mask_s, prev_s, end_s, params_s, state_s, in_s, out_s,
):
    step_id = pl.program_id(0)

    @pl.when(step_id == 0)
    def _():
        params = padded_params(bias_ref, rate_ref, skip_ref, params_s)
        cum = token_setup(
            docs_ref, step_ref, params, cum_s, step_s, mask_s, prev_s, end_s
        )[2]
        through = jnp.exp2(cum[T - 1 : T] + prev_s[T - 1 : T, 0:1])
        high, low = split(through, 2)
        row = iota((8, 128), 0)
        both = jnp.where(row == 0, high.astype(F32), jnp.where(row == 1, low.astype(F32), 0.0))
        for shard in range(SHARDS):
            state_s[SLOT * shard + ROWS : SLOT * (shard + 1)] = both
        in_s[...] = group_halves(in_ref)[0]
        out_s[...] = group_halves(out_ref)[1]

    _, _, step, enter, to_end = block_gains(step_id, cum_s, step_s, prev_s, end_s)
    pre, _ = conv_pre(x_ref[...], halo_ref[...], weight_ref[...], mask_s)
    act = pre * sigmoid(pre)
    gate = gate_ref[...].astype(F32)
    out_grad = grad_ref[...].astype(F32) * gate * sigmoid(gate)
    ended = (act * step * to_end).astype(BF16)
    entered = (out_grad * enter).astype(BF16)
    state = dot(ended, in_s[...], TN) + dot(entered, out_s[...], TN)
    for part in range(BLK // 8):
        place = step_id * (BLK // 8) + part
        target = lax.div(place, GROUPS8)
        offset = SLOT * target + 8 * (place - GROUPS8 * target)
        state_s[pl.ds(pl.multiple_of(offset, 8), 8), :] = state[8 * part : 8 * part + 8]

    @pl.when(step_id == STEPS - 1)
    def _():
        parts_ref[...] = state_s[...].astype(BF16)


TOKEN_SCRATCH = [
    pltpu.VMEM((3, T, 128), BF16),
    pltpu.VMEM((2, T, 128), BF16),
    pltpu.VMEM((KERNEL - 1, T, BLK), F32),
    pltpu.VMEM((T, BLK), F32),
    pltpu.VMEM((T, BLK), F32),
    pltpu.VMEM((8, 128), F32),
]


def mixer_specs(heads):
    return [
        column_block(T), column_block(8), column_block(KERNEL), column_block(T),
        column_block(T), whole((heads, T)), whole((1, heads)), whole((1, heads)),
        whole((1, heads)), whole((SHARDS * T // 128, 128)), whole((T, 128)), whole((T, 128)),
    ]


def mixer_first(*arrays):
    heads = arrays[5].shape[0]
    return pl.pallas_call(
        mixer_first_kernel,
        grid=(STEPS,),
        in_specs=mixer_specs(heads),
        out_specs=whole((SHARDS * SLOT, 128)),
        out_shape=jax.ShapeDtypeStruct((SHARDS * SLOT, 128), BF16),
        scratch_shapes=TOKEN_SCRATCH + [
            pltpu.VMEM((SHARDS * SLOT, 128), F32),
            pltpu.VMEM((T, 128), BF16),
            pltpu.VMEM((T, 128), BF16),
        ],
        cost_estimate=pl.CostEstimate(flops=8 * 10**9, bytes_accessed=4 * 10**6, transcendentals=0),
        compiler_params=GRANT,
        name="mixer_first",
    )(*arrays)


def chain_kernel(parts_ref, out_ref, forward_s):
    slot = seq_index()
    owner = (slot * ROWS + iota((ROWS, 128), 0)) // 64
    choose = jnp.where(owner == iota((ROWS, 128), 1), 1.0, 0.0)
    lane = iota((ROWS, 128), 1)
    through = []
    carry = jnp.zeros((ROWS, 128), F32)
    for shard in range(SHARDS):
        row = parts_ref[shard, ROWS : ROWS + 1].astype(F32)
        row = row + parts_ref[shard, ROWS + 1 : ROWS + 2].astype(F32)
        gain = jnp.sum(choose * row, axis=1, keepdims=True)
        through.append(gain)
        forward_s[shard] = carry
        carry = gain * carry + parts_ref[shard, 0:ROWS].astype(F32)
    carry = jnp.zeros((ROWS, 128), F32)
    for shard in reversed(range(SHARDS)):
        out_ref[shard] = jnp.where(lane < STATE, forward_s[shard], carry).astype(BF16)
        carry = through[shard] * carry + parts_ref[shard, 0:ROWS].astype(F32)


def chain(parts):
    return pl.pallas_call(
        chain_kernel,
        in_specs=[IN_VMEM],
        out_specs=IN_VMEM,
        out_shape=pltpu.VMEM((SHARDS, ROWS, 128), BF16),
        scratch_shapes=[pltpu.VMEM((SHARDS, ROWS, 128), F32)],
        cost_estimate=pl.CostEstimate(flops=2 * 10**9, bytes_accessed=10**6, transcendentals=0),
        compiler_params=GRANT,
        name="chain",
    )(parts)


BUNDLE = KERNEL * COLS // 128
LANES_BLK = BLK // 128


def mixer_second_kernel(
    x_ref, halo_ref, weight_ref, gate_ref, grad_ref, step_ref, bias_ref, rate_ref,
    skip_ref, docs_ref, in_ref, out_ref, state_ref,
    dx_ref, tail_ref, spill_ref, dgate_ref, dstep_ref, coeff_ref, bundle_ref,
    cum_s, step_s, mask_s, prev_s, end_s, params_s,
    cumt_s, pair_s, causal_s, dtop_s, dbottom_s, coeff_s, row_s, dt_s, ends_s, bundle_s,
    in_low_s, in_high_s, out_low_s, out_high_s,
):
    step_id = pl.program_id(0)
    lane = iota((T, 128), 1)

    @pl.when(step_id == 0)
    def _():
        params = padded_params(bias_ref, rate_ref, skip_ref, params_s)
        own, own_row, cum = token_setup(
            docs_ref, step_ref, params, cum_s, step_s, mask_s, prev_s, end_s
        )
        cumt_s[...] = jnp.transpose(cum)
        same = (own == own_row) & (iota((T, T), 0) >= iota((T, T), 1))
        causal_s[...] = jnp.where(same, 0.0, NEG)
        in_low_s[...], in_high_s[...] = group_halves(in_ref)
        out_low_s[...], out_high_s[...] = group_halves(out_ref)
        pair_s[...] = dot(out_low_s[...], in_low_s[...], NT)
        dtop_s[...] = jnp.zeros((HALF, HALF), F32)
        dbottom_s[...] = jnp.zeros((HALF, T), F32)
        coeff_s[...] = jnp.zeros((T, 128), F32)
        row_s[...] = jnp.zeros((T, 128), F32)
        dt_s[...] = jnp.zeros((T, 128), F32)
        ends_s[...] = jnp.zeros((8, 128), F32)

    out_low = out_low_s[...]
    in_high = in_high_s[...]
    spread, cum, step, enter, to_end = block_gains(step_id, cum_s, step_s, prev_s, end_s)
    skip = sum(dot(part, spread) for part in split(params_s[...], 3))[2:3]
    weight = weight_ref[...]
    pre, shifted = conv_pre(x_ref[...], halo_ref[...], weight, mask_s)
    sig = sigmoid(pre)
    act = pre * sig
    gate = gate_ref[...].astype(F32)
    gate_sig = sigmoid(gate)
    mix_grad = grad_ref[...].astype(F32)
    out_grad = mix_grad * gate * gate_sig
    scaled = act * step
    scaled_half = scaled.astype(BF16)
    grad_half = out_grad.astype(BF16)

    block_head = iota((T, BLK), 1) // 64
    tops, bottoms, scaled_parts, grad_parts = [], [], [], []
    dtop, dbottom = dtop_s[...], dbottom_s[...]
    for k in range(HEADS_BLK):
        mine = block_head == k
        cum_col = cum[:, 64 * k : 64 * k + 1]
        cum_row = cumt_s[pl.ds(step_id * HEADS_BLK + k, 1), :]
        top = jnp.exp2(
            jnp.broadcast_to(cum_col[:HALF], (HALF, HALF)) - cum_row[:, :HALF]
            + causal_s[:HALF, :HALF]
        )
        bottom = jnp.exp2(
            jnp.broadcast_to(cum_col[HALF:], (HALF, T)) - cum_row + causal_s[HALF:, :]
        )
        tops.append((pair_s[:HALF, :HALF] * top).astype(BF16))
        bottoms.append((pair_s[HALF:, :] * bottom).astype(BF16))
        scaled_k = jnp.where(mine, scaled_half, jnp.zeros_like(scaled_half))
        grad_k = jnp.where(mine, grad_half, jnp.zeros_like(grad_half))
        scaled_parts.append(scaled_k)
        grad_parts.append(grad_k)
        dtop = dtop + dot(grad_k[:HALF], scaled_half[:HALF], NT) * top
        dbottom = dbottom + dot(grad_k[HALF:], scaled_half, NT) * bottom
    dtop_s[...] = dtop
    dbottom_s[...] = dbottom
    join = jnp.concatenate
    inner = join(
        [
            dot(join(tops, axis=1), join([v[:HALF] for v in scaled_parts], axis=0)),
            dot(join(bottoms, axis=1), join(scaled_parts, axis=0)),
        ],
        axis=0,
    )
    upper_part = dot(join(tops, axis=0), join([v[:HALF] for v in grad_parts], axis=0), TN)
    dscaled = dot(join(bottoms, axis=0), join([v[HALF:] for v in grad_parts], axis=0), TN)
    dscaled = join([dscaled[:HALF] + upper_part, dscaled[HALF:]], axis=0)

    state = state_ref[...]
    carried = dot(out_low, state, NT) * enter
    from_end = dot(in_high, state, NT) * to_end
    ssm_out = inner + carried
    dscaled = dscaled + from_end
    mixed_out = ssm_out + skip * act
    dgate_ref[...] = (
        mix_grad * mixed_out * gate_sig * (1.0 + gate * (1.0 - gate_sig))
    ).astype(BF16)

    gave_out = dot((out_grad * enter).astype(BF16), state)
    gave_in = dot((scaled * to_end).astype(BF16), state)
    coeff_s[...] += jnp.where(lane < STATE, gave_out, gave_in)

    grad_round = grad_half.astype(F32)
    scaled_round = scaled_half.astype(F32)
    balance = grad_round * ssm_out - scaled_round * dscaled
    row_s[...] += sum(dot(part, spread, NT) for part in split(balance, 2))
    dt_s[...] += dot((dscaled * act).astype(BF16), spread, NT)

    state_wide = state.astype(F32)
    product = state_wide * pltpu.roll(state_wide, STATE, 1)
    through = jnp.sum(jnp.where(iota((BLK, 128), 1) < STATE, product, 0.0), axis=1, keepdims=True)
    through_row = jnp.transpose(jnp.broadcast_to(through, (BLK, BLK)))[0:1]
    end_row = jnp.sum(scaled_round * from_end, axis=0, keepdims=True)
    end_row = end_row + through_row * enter[T - 1 : T]
    skip_row = jnp.sum(out_grad * act, axis=0, keepdims=True)
    row8 = iota((8, BLK), 0)
    both = jnp.where(row8 == 0, end_row, jnp.where(row8 == 1, skip_row, 0.0))
    ends_s[...] += sum(dot(part, spread, NT) for part in split(both, 3))

    dact = step * dscaled + skip * out_grad
    dpre = dact * sig * (1.0 + pre * (1.0 - sig))
    zeros = jnp.zeros((8, BLK), F32)
    dx = weight[0:1] * dpre
    spill = zeros
    for lag in range(KERNEL):
        tap = jnp.sum(dpre * shifted[lag], axis=0, keepdims=True)
        for m in range(LANES_BLK):
            place = lag * (COLS // 128) + step_id * LANES_BLK + m
            bundle_s[pl.ds(place, 1), :] = tap[:, 128 * m : 128 * (m + 1)]
        if lag == 0:
            continue
        masked = dpre * mask_s[lag - 1]
        later = pltpu.roll(jnp.concatenate([masked, zeros], axis=0), T + 8 - lag, 0)[:T]
        dx = dx + weight[lag : lag + 1] * later
        edge = pltpu.roll(jnp.concatenate([zeros, masked[:8]], axis=0), 16 - lag, 0)[:8]
        spill = spill + weight[lag : lag + 1] * edge
    dx_ref[...] = dx.astype(BF16)
    tail_ref[...] = dx[T - 8 :]
    spill_ref[...] = spill

    @pl.when(step_id == STEPS - 1)
    def _():
        params = params_s[...]
        raw = raw_steps(step_ref) + params[0:1]
        rate = jnp.exp(params[1:2])
        decay = step_and_decay(raw, params)[1]
        upper = jnp.where(iota((T, T), 1) >= iota((T, T), 0), 1.0, 0.0)
        ends = ends_s[...]
        ddecay = exact(upper, row_s[...]) + ends[0:1]
        dstep = (dt_s[...] - ddecay * rate) * sigmoid(raw)
        dstep_ref[...] = jnp.transpose(dstep)[: dstep_ref.shape[0]]
        dbias = jnp.sum(dstep, axis=0, keepdims=True)
        drate = jnp.sum(ddecay * decay, axis=0, keepdims=True)
        row = iota((8, 128), 0)
        small = jnp.zeros((8, 128), F32)
        for n, vector in enumerate((dbias, drate, ends[1:2])):
            for m, part in enumerate(split(vector, 2)):
                small = jnp.where(row == 2 * n + m, part.astype(F32), small)
        bundle_s[BUNDLE : BUNDLE + 8] = small
        bundle = bundle_s[...].astype(BF16)
        for shard in range(SHARDS):
            bundle_ref[shard] = bundle
        top_half, bottom_half = dtop.astype(BF16), dbottom.astype(BF16)
        in_low, out_high = in_low_s[...], out_high_s[...]
        out_part = join([dot(top_half, in_low[:HALF]), dot(bottom_half, in_low)], axis=0)
        in_part = dot(bottom_half, out_high[HALF:], TN)
        in_part = join(
            [in_part[:HALF] + dot(top_half, out_high[:HALF], TN), in_part[HALF:]], axis=0
        )
        coeff_ref[...] = (coeff_s[...] + out_part + in_part).astype(BF16)


def mixer_second(*arrays):
    heads = arrays[5].shape[0]
    half = pltpu.VMEM((T, 128), BF16)
    return pl.pallas_call(
        mixer_second_kernel,
        grid=(STEPS,),
        in_specs=mixer_specs(heads) + [pl.BlockSpec((BLK, 128), lambda c: (c, 0))],
        out_specs=[
            column_block(T), column_block(8), column_block(8), column_block(T),
            whole((heads, T)), whole((T, 128)), whole((SHARDS, BUNDLE + 8, 128)),
        ],
        out_shape=[
            jax.ShapeDtypeStruct((T, COLS), BF16),
            jax.ShapeDtypeStruct((8, COLS), F32),
            jax.ShapeDtypeStruct((8, COLS), F32),
            jax.ShapeDtypeStruct((T, COLS), BF16),
            jax.ShapeDtypeStruct((heads, T), F32),
            jax.ShapeDtypeStruct((T, 128), BF16),
            jax.ShapeDtypeStruct((SHARDS, BUNDLE + 8, 128), BF16),
        ],
        scratch_shapes=TOKEN_SCRATCH + [
            pltpu.VMEM((128, T), F32),
            pltpu.VMEM((T, T), F32),
            pltpu.VMEM((T, T), F32),
            pltpu.VMEM((HALF, HALF), F32),
            pltpu.VMEM((HALF, T), F32),
            pltpu.VMEM((T, 128), F32),
            pltpu.VMEM((T, 128), F32),
            pltpu.VMEM((T, 128), F32),
            pltpu.VMEM((8, 128), F32),
            pltpu.VMEM((BUNDLE + 8, 128), F32),
            half, half, half, half,
        ],
        cost_estimate=pl.CostEstimate(flops=18 * 10**9, bytes_accessed=8 * 10**6, transcendentals=0),
        compiler_params=GRANT,
        name="mixer_second",
    )(*arrays)


def finish_kernel(bundle_ref, *refs):
    coeff_refs = refs[:LOCAL_HEADS]
    weight_ref, bias_ref, rate_ref, skip_ref, in_ref, out_ref, coeff_s = refs[LOCAL_HEADS:]
    for turn, ref in enumerate(coeff_refs):
        coeff_s[lax.rem(lax.axis_index("head") - turn + LOCAL_HEADS, LOCAL_HEADS)] = ref[...].astype(F32)
    total = bundle_ref[0].astype(F32)
    for shard in range(1, SHARDS):
        total = total + bundle_ref[shard].astype(F32)
    tiles = COLS // 128
    for lag in range(KERNEL):
        for m in range(tiles):
            weight_ref[lag : lag + 1, 128 * m : 128 * (m + 1)] = total[
                lag * tiles + m : lag * tiles + m + 1
            ]
    for n, ref in enumerate((bias_ref, rate_ref, skip_ref)):
        row = BUNDLE + 2 * n
        ref[...] = (total[row : row + 1] + total[row + 1 : row + 2])[:, : ref.shape[1]]
    low, high = coeff_s[0] + coeff_s[1], coeff_s[2] + coeff_s[3]
    left = iota((T, 128), 1) < STATE
    out_ref[...] = jnp.where(left, low, pltpu.roll(high, STATE, 1))
    in_ref[...] = jnp.where(left, pltpu.roll(low, STATE, 1), high)


def finish(bundle, coeffs, heads):
    small = jax.ShapeDtypeStruct((1, heads), F32)
    wide = jax.ShapeDtypeStruct((T, 128), F32)
    return pl.pallas_call(
        finish_kernel,
        in_specs=[IN_VMEM] * (1 + LOCAL_HEADS),
        out_specs=[IN_VMEM] * 6,
        out_shape=[jax.ShapeDtypeStruct((KERNEL, COLS), F32), small, small, small, wide, wide],
        scratch_shapes=[pltpu.VMEM((LOCAL_HEADS, T, 128), F32)],
        compiler_params=GRANT,
        name="finish",
    )(bundle, *coeffs)


ROW = 4
K_AT, V_AT, Q_AT, G_AT = (slice(n * HEAD_DIM, (n + 1) * HEAD_DIM) for n in range(4))
PAIR = (2 * HEAD_DIM, T)


def pack_kernel(k_ref, v_ref, q_ref, g_ref, *refs):
    out_refs, turned_s = refs[:ROW], refs[ROW]
    for ref, place in ((k_ref, K_AT), (v_ref, V_AT), (q_ref, Q_AT), (g_ref, G_AT)):
        turned_part = jnp.transpose(ref[...])
        for head in range(LOCAL_HEADS):
            turned_s[head, place] = turned_part[head * HEAD_DIM : (head + 1) * HEAD_DIM]
    for turn in range(ROW):
        out_refs[turn][...] = turned_s[lax.rem(row_place() + turn, ROW)]


def pack(keys, values, queries, grads):
    return pl.pallas_call(
        pack_kernel,
        in_specs=[IN_VMEM] * 4,
        out_specs=[IN_VMEM] * ROW,
        out_shape=[pltpu.VMEM((4 * HEAD_DIM, T), BF16)] * ROW,
        scratch_shapes=[pltpu.VMEM((LOCAL_HEADS, 4 * HEAD_DIM, T), BF16)],
        compiler_params=GRANT,
        name="pack",
    )(keys, values, queries, grads)


def lend_kernel(*refs):
    for turn, ref in enumerate(refs[:ROW]):
        refs[ROW][turn * PAIR[0] : (turn + 1) * PAIR[0]] = ref[: PAIR[0]]


def lend(own):
    return pl.pallas_call(
        lend_kernel,
        in_specs=[IN_VMEM] * ROW,
        out_specs=IN_VMEM,
        out_shape=pltpu.VMEM((ROW * PAIR[0], T), BF16),
        compiler_params=GRANT,
        name="lend",
    )(*own)


def attention_kernel(docs_ref, far_ref, *refs):
    arrived, (dq_ref, own_ref, back_ref, far_s, qg_s, kv_s) = refs[:ROW], refs[ROW:]
    for turn in range(ROW):
        block = lax.rem(row_place() - turn + ROW, ROW)
        kv_s[ROW + block] = arrived[turn][: PAIR[0]]
        qg_s[block] = arrived[turn][PAIR[0] :]
        kv_s[block] = far_ref[turn * PAIR[0] : (turn + 1) * PAIR[0]]
    first_block = lax.div(seq_index(), ROW) * ROW
    later = iota((T, T), 1) > iota((T, T), 0)
    scale = HEAD_DIM ** (-0.5)

    def doc_row(block):
        place = first_block + block
        row = doc_row_of(docs_ref, jnp.maximum(place, 0))
        return row if block >= 0 else jnp.where(place < 0, -1.0, row)

    rows = {block: doc_row(block) for block in range(-ROW, ROW)}
    for i in range(ROW):
        own_doc = columns_of(rows[i])
        qt, gt = qg_s[i, K_AT], qg_s[i, V_AT]
        q, g = jnp.transpose(qt), jnp.transpose(gt)

        def part(gap, place):
            return kv_s[ROW + i - gap, place]

        scores = []
        top = None
        for gap in range(ROW + 1):
            same = own_doc == rows[i - gap]
            if gap == 0:
                same = same & jnp.logical_not(later)
            if gap == ROW:
                same = same & later
            s = jnp.where(same, dot(q, part(gap, K_AT)) * (scale * LOG2E), NEG)
            scores.append(s)
            top = s if top is None else jnp.maximum(top, s)
        top = jnp.max(top, axis=1, keepdims=True)
        expos = [jnp.exp2(s - top) for s in scores]
        total = jnp.sum(sum(expos), axis=1, keepdims=True)
        inverse = 1.0 / jnp.maximum(total, 1.0)
        probs = [e * inverse for e in expos]
        halves = [p.astype(BF16) for p in probs]
        dprobs = [dot(g, part(gap, V_AT)) for gap in range(ROW + 1)]
        delta = sum(h.astype(F32) * d for h, d in zip(halves, dprobs))
        delta = jnp.sum(delta, axis=1, keepdims=True)
        dq = jnp.zeros((HEAD_DIM, T), F32)
        for gap in range(ROW + 1):
            dscore = (probs[gap] * (dprobs[gap] - delta)).astype(BF16)
            dq = dq + dot(part(gap, K_AT), dscore, NT)
            block = i - gap
            ref, index = (own_ref, block) if block >= 0 else (far_s, block + ROW)
            dk, dv = dot(qt, dscore), dot(gt, halves[gap])
            if gap == 0 or (block < 0 and i == 0):
                ref[index, K_AT] = dk
                ref[index, V_AT] = dv
            else:
                ref[index, K_AT] += dk
                ref[index, V_AT] += dv
            if gap == ROW:
                back_ref[index] = far_s[index].astype(BF16)
        dq_ref[i] = (dq * scale).astype(BF16)


def attention(docs, far, own):
    pairs = (ROW, *PAIR)
    return pl.pallas_call(
        attention_kernel,
        in_specs=[IN_VMEM] * (2 + ROW),
        out_specs=[IN_VMEM] * 3,
        out_shape=[
            pltpu.VMEM((ROW, HEAD_DIM, T), BF16),
            pltpu.VMEM(pairs, F32),
            pltpu.VMEM(pairs, BF16),
        ],
        scratch_shapes=[
            pltpu.VMEM(pairs, F32),
            pltpu.VMEM(pairs, BF16),
            pltpu.VMEM((2 * ROW, *PAIR), BF16),
        ],
        cost_estimate=pl.CostEstimate(flops=12 * 10**9, bytes_accessed=8 * 10**6, transcendentals=0),
        compiler_params=GRANT,
        name="attention",
    )(docs, far, *own)


def merge_kernel(dq_ref, dkv_ref, back_ref, *out_refs):
    scale = HEAD_DIM ** (-0.5)
    place = row_place()
    for turn, out_ref in enumerate(out_refs):
        block = lax.rem(place + turn, ROW)
        total = dkv_ref[block] + back_ref[block].astype(F32)
        out_ref[K_AT] = (total[K_AT] * scale).astype(BF16)
        out_ref[V_AT] = total[V_AT].astype(BF16)
        out_ref[Q_AT] = dq_ref[block]


def merge(dq, dkv, back):
    return pl.pallas_call(
        merge_kernel,
        in_specs=[IN_VMEM] * 3,
        out_specs=[IN_VMEM] * ROW,
        out_shape=[pltpu.VMEM((3 * HEAD_DIM, T), BF16)] * ROW,
        cost_estimate=pl.CostEstimate(flops=3 * 10**9, bytes_accessed=4 * 10**6, transcendentals=0),
        compiler_params=GRANT,
        name="merge",
    )(dq, dkv, back)


def unpack_kernel(*refs):
    parts, outs, stacked_s = refs[:ROW], refs[ROW : ROW + 3], refs[ROW + 3]
    place = row_place()
    for turn, part in enumerate(parts):
        source = lax.rem(place - turn + ROW, ROW)
        for n, at in enumerate((Q_AT, K_AT, V_AT)):
            stacked_s[n, source] = part[at]
    for n, ref in enumerate(outs):
        stacked = jnp.concatenate([stacked_s[n, h] for h in range(LOCAL_HEADS)], axis=0)
        ref[...] = jnp.transpose(stacked)


def unpack(parts):
    wide = jax.ShapeDtypeStruct((T, LOCAL_HEADS * HEAD_DIM), BF16)
    return pl.pallas_call(
        unpack_kernel,
        in_specs=[IN_VMEM] * ROW,
        out_specs=[IN_VMEM] * 3,
        out_shape=[wide] * 3,
        scratch_shapes=[pltpu.VMEM((3, LOCAL_HEADS, HEAD_DIM, T), BF16)],
        cost_estimate=pl.CostEstimate(flops=2 * 10**9, bytes_accessed=3 * 10**6, transcendentals=0),
        compiler_params=GRANT,
        name="unpack",
    )(*parts)


def passed_along(value, axis, steps):
    count = lax.axis_size(axis)
    initial, last = (max(0, -steps), min(count, count - steps))
    return lax.ppermute(value, axis, [(source, source + steps) for source in range(initial, last)])


def turns(parts, axis):
    count = lax.axis_size(axis)
    return [parts[0]] + [
        lax.ppermute(part, axis, [(n, (n + turn) % count) for n in range(count)])
        for turn, part in enumerate(parts[1:], 1)
    ]


def near(array):
    return pltpu.with_memory_space_constraint(array, pltpu.VMEM)


def exchange(array, axis):
    return lax.all_to_all(array, axis, split_axis=0, concat_axis=0, tiled=True)


def local(
    queries, keys, values, attn_grad, doc_ids, conv_input, conv_weight, step_raw, step_bias,
    rate_log, skip_gain, input_coeff, output_coeff, gate_input, mix_grad,
):
    heads = step_raw.shape[1]
    docs = doc_ids.reshape(SHARDS * T // 128, 128)
    halo = passed_along(conv_input[T - 8 :], SEQ, 1)
    parts = pack(keys, values, queries, attn_grad)
    own = [near(v) for v in turns(parts, "seq_2")]
    lent = lend(own)
    far = passed_along(lent, SEQ, ROW)

    mixer_args = (
        conv_input, halo, conv_weight, gate_input, mix_grad, step_raw.T,
        step_bias.reshape(1, heads), rate_log.reshape(1, heads), skip_gain.reshape(1, heads),
        docs, input_coeff, output_coeff,
    )
    parts = mixer_first(*mixer_args).reshape(SHARDS, SLOT, 128)
    gathered = exchange(parts, SEQ)
    scanned = chain(near(gathered))
    entering = exchange(scanned, SEQ).reshape(COLS, 128)
    dq, dkv, back = attention(docs, near(far), own)
    returned = passed_along(back, SEQ, -ROW)
    dx, tail, spill, dgate, dstep, coeff, bundle = mixer_second(*mixer_args, entering)
    leaving = merge(near(dq), near(dkv), near(returned))
    swapped = turns(leaving, "seq_2")
    spilled = passed_along(spill, SEQ, -1)
    bundles = exchange(bundle, SEQ)
    coeffs = turns([coeff] * LOCAL_HEADS, "head")
    dq, dk, dv = unpack([near(v) for v in swapped])
    grad_weight, grad_bias, grad_rate, grad_skip, sum_in, sum_out = finish(
        near(bundles), [near(v) for v in coeffs], heads
    )
    tail = (tail + spilled).astype(BF16)
    grad_conv = lax.dynamic_update_slice_in_dim(dx, tail, T - 8, 0)
    return (
        dq, dk, dv, grad_conv, dgate, dstep.T, sum_in, sum_out, grad_weight,
        grad_bias.reshape(heads), grad_rate.reshape(heads), grad_skip.reshape(heads),
    )


def solution(mesh):
    finer = Mesh(
        mesh.devices.reshape(4, 2, 4, mesh.shape["head"]), ("seq_0", "seq_1", "seq_2", "head")
    )
    wide = P(SEQ, "head")
    return jax.shard_map(
        local,
        mesh=finer,
        in_specs=(
            wide, wide, wide, wide, P(), wide, P(None, "head"), wide, P("head"), P("head"),
            P("head"), P(SEQ, None), P(SEQ, None), wide, wide,
        ),
        out_specs=(
            wide, wide, wide, wide, wide, wide, P(SEQ, None), P(SEQ, None), P(None, "head"),
            P("head"), P("head"), P("head"),
        ),
        check_vma=False,
    )
```

```python
import jax
import jax.numpy as jnp
from jax import lax
from jax.experimental import pallas as pl
from jax.experimental.pallas import tpu as pltpu
from jax.sharding import Mesh
from jax.sharding import PartitionSpec as P


HEAD_DIM = 224
STATE = 64
KERNEL = 4
SEQ = ("seq_0", "seq_1", "seq_2")
SHARDS = 32
T = 256
LOCAL_HEADS = 4
BLK = 256
HALF = T // 2
HEADS_BLK = BLK // 64
COLS = 1792
STEPS = COLS // BLK
NEG = -1e30
LOG2E = 1.4426950408889634
F32 = jnp.float32
BF16 = jnp.bfloat16

NN = (((1,), (0,)), ((), ()))
NT = (((1,), (1,)), ((), ()))
TN = (((0,), (0,)), ((), ()))


def dot(a, b, dims=NN):
    return lax.dot_general(a, b, dims, preferred_element_type=F32)


def exact(a, b, dims=NN):
    return lax.dot_general(
        a, b, dims, preferred_element_type=F32, precision=lax.Precision.HIGHEST
    )


def split(a, pieces):
    parts = []
    for _ in range(pieces):
        part = a.astype(BF16)
        parts.append(part)
        a = a - part.astype(F32)
    return parts


def sigmoid(v):
    return 0.5 + 0.5 * jnp.tanh(0.5 * v)


def iota(shape, dim):
    return lax.broadcasted_iota(jnp.int32, shape, dim)


def columns_of(row):
    return jnp.transpose(jnp.broadcast_to(row, (T, T)))


def whole(shape):
    return pl.BlockSpec(shape, lambda c: (0,) * len(shape))


def column_block(rows):
    return pl.BlockSpec((rows, BLK), lambda c: (0, c))


IN_VMEM = pl.BlockSpec(memory_space=pltpu.VMEM)
GRANT = pltpu.CompilerParams(vmem_limit_bytes=32 * 2**20)


def seq_index():
    index = 0
    for axis in SEQ:
        index = index * lax.axis_size(axis) + lax.axis_index(axis)
    return index


def row_place():
    return lax.axis_index(SEQ[-1])


def doc_row_of(docs_ref, shard):
    return jnp.concatenate(
        [docs_ref[pl.ds(2 * shard + part, 1), :] for part in range(2)], axis=1
    ).astype(F32)


def doc_rows(docs_ref):
    shard = seq_index()
    own = doc_row_of(docs_ref, shard)
    before = doc_row_of(docs_ref, jnp.maximum(shard - 1, 0))
    return own, jnp.where(shard == 0, -1.0, before)


def group_halves(coeff_ref):
    coeff = coeff_ref[...].astype(F32)
    turned = pltpu.roll(coeff, STATE, 1)
    first = lax.axis_index("head") < 2
    low = iota((T, 128), 1) < STATE
    mine_low = jnp.where(low, jnp.where(first, coeff, turned), 0.0)
    mine_high = jnp.where(low, 0.0, jnp.where(first, turned, coeff))
    return mine_low.astype(BF16), mine_high.astype(BF16)


def padded_params(bias_ref, rate_ref, skip_ref, params_s):
    heads = bias_ref.shape[1]
    params_s[...] = jnp.zeros((8, 128), F32)
    for n, ref in enumerate((bias_ref, rate_ref, skip_ref)):
        params_s[n : n + 1, 0:heads] = ref[...]
    return params_s[...]


def raw_steps(step_ref):
    rows = step_ref.shape[0]
    filled = jnp.concatenate([step_ref[...], jnp.zeros((128 - rows, T), F32)], axis=0)
    return jnp.transpose(filled)


def step_and_decay(raw, params):
    step = jnp.maximum(raw, 0.0) + jnp.log1p(jnp.exp(-jnp.abs(raw)))
    return step, -step * jnp.exp(params[1:2])


def token_setup(docs_ref, step_ref, params, cum_s, step_s, mask_s, prev_s, end_s):
    own_row, before_row = doc_rows(docs_ref)
    own = columns_of(own_row)
    lane = iota((8, T), 1)
    own8 = jnp.broadcast_to(own_row, (8, T))
    before8 = jnp.broadcast_to(before_row, (8, T))
    for lag in range(1, KERNEL):
        lagged = jnp.where(lane < lag, pltpu.roll(before8, lag, 1), pltpu.roll(own8, lag, 1))
        mask_s[lag - 1] = jnp.where(own == columns_of(lagged[0:1]), 1.0, 0.0)
    prev_s[...] = jnp.where(own == before_row[:, T - 1 : T], 0.0, NEG)
    end_s[...] = jnp.where(own == own_row[:, T - 1 : T], 0.0, NEG)
    raw = raw_steps(step_ref) + params[0:1]
    step, decay = step_and_decay(raw, params)
    lower = jnp.where(iota((T, T), 0) >= iota((T, T), 1), 1.0, 0.0)
    cum = exact(lower, decay) * LOG2E
    for n, part in enumerate(split(cum, 3)):
        cum_s[n] = part
    for n, part in enumerate(split(step, 2)):
        step_s[n] = part
    return own, own_row, cum


def spread_of(step_id):
    head = iota((128, BLK), 0)
    owner = step_id * HEADS_BLK + iota((128, BLK), 1) // 64
    return jnp.where(head == owner, 1.0, 0.0).astype(BF16)


def block_gains(step_id, cum_s, step_s, prev_s, end_s):
    spread = spread_of(step_id)
    cum = dot(cum_s[0], spread) + dot(cum_s[1], spread) + dot(cum_s[2], spread)
    step = dot(step_s[0], spread) + dot(step_s[1], spread)
    enter = jnp.exp2(cum + prev_s[...])
    to_end = jnp.exp2(cum[T - 1 : T] - cum + end_s[...])
    return spread, cum, step, enter, to_end


def conv_pre(x, halo, weight, mask_s):
    extended = jnp.concatenate([halo.astype(F32), x.astype(F32)], axis=0)
    shifted = [extended[8:]]
    summed = weight[0:1] * shifted[0]
    for lag in range(1, KERNEL):
        moved = pltpu.roll(extended, lag, 0)[8:] * mask_s[lag - 1]
        shifted.append(moved)
        summed = summed + weight[lag : lag + 1] * moved
    return summed, shifted


ROWS = COLS // SHARDS
GROUPS8 = ROWS // 8
SLOT = ROWS + 8


def mixer_first_kernel(
    x_ref, halo_ref, weight_ref, gate_ref, grad_ref, step_ref, bias_ref, rate_ref,
    skip_ref, docs_ref, in_ref, out_ref,
    parts_ref,
    cum_s, step_s, mask_s, prev_s, end_s, params_s, state_s, in_s, out_s,
):
    step_id = pl.program_id(0)

    @pl.when(step_id == 0)
    def _():
        params = padded_params(bias_ref, rate_ref, skip_ref, params_s)
        cum = token_setup(
            docs_ref, step_ref, params, cum_s, step_s, mask_s, prev_s, end_s
        )[2]
        through = jnp.exp2(cum[T - 1 : T] + prev_s[T - 1 : T, 0:1])
        high, low = split(through, 2)
        row = iota((8, 128), 0)
        both = jnp.where(row == 0, high.astype(F32), jnp.where(row == 1, low.astype(F32), 0.0))
        for shard in range(SHARDS):
            state_s[SLOT * shard + ROWS : SLOT * (shard + 1)] = both
        in_s[...] = group_halves(in_ref)[0]
        out_s[...] = group_halves(out_ref)[1]

    _, _, step, enter, to_end = block_gains(step_id, cum_s, step_s, prev_s, end_s)
    pre, _ = conv_pre(x_ref[...], halo_ref[...], weight_ref[...], mask_s)
    act = pre * sigmoid(pre)
    gate = gate_ref[...].astype(F32)
    out_grad = grad_ref[...].astype(F32) * gate * sigmoid(gate)
    ended = (act * step * to_end).astype(BF16)
    entered = (out_grad * enter).astype(BF16)
    state = dot(ended, in_s[...], TN) + dot(entered, out_s[...], TN)
    for part in range(BLK // 8):
        place = step_id * (BLK // 8) + part
        target = lax.div(place, GROUPS8)
        offset = SLOT * target + 8 * (place - GROUPS8 * target)
        state_s[pl.ds(pl.multiple_of(offset, 8), 8), :] = state[8 * part : 8 * part + 8]

    @pl.when(step_id == STEPS - 1)
    def _():
        parts_ref[...] = state_s[...].astype(BF16)


TOKEN_SCRATCH = [
    pltpu.VMEM((3, T, 128), BF16),
    pltpu.VMEM((2, T, 128), BF16),
    pltpu.VMEM((KERNEL - 1, T, BLK), F32),
    pltpu.VMEM((T, BLK), F32),
    pltpu.VMEM((T, BLK), F32),
    pltpu.VMEM((8, 128), F32),
]


def mixer_specs(heads):
    return [
        column_block(T), column_block(8), column_block(KERNEL), column_block(T),
        column_block(T), whole((heads, T)), whole((1, heads)), whole((1, heads)),
        whole((1, heads)), whole((SHARDS * T // 128, 128)), whole((T, 128)), whole((T, 128)),
    ]


def mixer_first(*arrays):
    heads = arrays[5].shape[0]
    return pl.pallas_call(
        mixer_first_kernel,
        grid=(STEPS,),
        in_specs=mixer_specs(heads),
        out_specs=whole((SHARDS * SLOT, 128)),
        out_shape=jax.ShapeDtypeStruct((SHARDS * SLOT, 128), BF16),
        scratch_shapes=TOKEN_SCRATCH + [
            pltpu.VMEM((SHARDS * SLOT, 128), F32),
            pltpu.VMEM((T, 128), BF16),
            pltpu.VMEM((T, 128), BF16),
        ],
        cost_estimate=pl.CostEstimate(flops=8 * 10**9, bytes_accessed=4 * 10**6, transcendentals=0),
        name="mixer_first",
    )(*arrays)


def chain_kernel(parts_ref, out_ref, forward_s):
    slot = seq_index()
    owner = (slot * ROWS + iota((ROWS, 128), 0)) // 64
    choose = jnp.where(owner == iota((ROWS, 128), 1), 1.0, 0.0)
    lane = iota((ROWS, 128), 1)
    through = []
    carry = jnp.zeros((ROWS, 128), F32)
    for shard in range(SHARDS):
        row = parts_ref[shard, ROWS : ROWS + 1].astype(F32)
        row = row + parts_ref[shard, ROWS + 1 : ROWS + 2].astype(F32)
        gain = jnp.sum(choose * row, axis=1, keepdims=True)
        through.append(gain)
        forward_s[shard] = carry
        carry = gain * carry + parts_ref[shard, 0:ROWS].astype(F32)
    carry = jnp.zeros((ROWS, 128), F32)
    for shard in reversed(range(SHARDS)):
        out_ref[shard] = jnp.where(lane < STATE, forward_s[shard], carry).astype(BF16)
        carry = through[shard] * carry + parts_ref[shard, 0:ROWS].astype(F32)


def chain(parts):
    return pl.pallas_call(
        chain_kernel,
        in_specs=[IN_VMEM],
        out_specs=IN_VMEM,
        out_shape=pltpu.VMEM((SHARDS, ROWS, 128), BF16),
        scratch_shapes=[pltpu.VMEM((SHARDS, ROWS, 128), F32)],
        cost_estimate=pl.CostEstimate(flops=2 * 10**9, bytes_accessed=10**6, transcendentals=0),
        compiler_params=GRANT,
        name="chain",
    )(parts)


BUNDLE = KERNEL * COLS // 128
LANES_BLK = BLK // 128


def mixer_second_kernel(
    x_ref, halo_ref, weight_ref, gate_ref, grad_ref, step_ref, bias_ref, rate_ref,
    skip_ref, docs_ref, in_ref, out_ref, state_ref,
    dx_ref, tail_ref, spill_ref, dgate_ref, dstep_ref, coeff_ref, bundle_ref,
    cum_s, step_s, mask_s, prev_s, end_s, params_s,
    cumt_s, pair_s, causal_s, dtop_s, dbottom_s, coeff_s, row_s, dt_s, ends_s, bundle_s,
    in_low_s, in_high_s, out_low_s, out_high_s,
):
    step_id = pl.program_id(0)
    lane = iota((T, 128), 1)

    @pl.when(step_id == 0)
    def _():
        params = padded_params(bias_ref, rate_ref, skip_ref, params_s)
        own, own_row, cum = token_setup(
            docs_ref, step_ref, params, cum_s, step_s, mask_s, prev_s, end_s
        )
        cumt_s[...] = jnp.transpose(cum)
        same = (own == own_row) & (iota((T, T), 0) >= iota((T, T), 1))
        causal_s[...] = jnp.where(same, 0.0, NEG)
        in_low_s[...], in_high_s[...] = group_halves(in_ref)
        out_low_s[...], out_high_s[...] = group_halves(out_ref)
        pair_s[...] = dot(out_low_s[...], in_low_s[...], NT)
        dtop_s[...] = jnp.zeros((HALF, HALF), F32)
        dbottom_s[...] = jnp.zeros((HALF, T), F32)
        coeff_s[...] = jnp.zeros((T, 128), F32)
        row_s[...] = jnp.zeros((T, 128), F32)
        dt_s[...] = jnp.zeros((T, 128), F32)
        ends_s[...] = jnp.zeros((8, 128), F32)

    out_low = out_low_s[...]
    in_high = in_high_s[...]
    spread, cum, step, enter, to_end = block_gains(step_id, cum_s, step_s, prev_s, end_s)
    skip = sum(dot(part, spread) for part in split(params_s[...], 3))[2:3]
    weight = weight_ref[...]
    pre, shifted = conv_pre(x_ref[...], halo_ref[...], weight, mask_s)
    sig = sigmoid(pre)
    act = pre * sig
    gate = gate_ref[...].astype(F32)
    gate_sig = sigmoid(gate)
    mix_grad = grad_ref[...].astype(F32)
    out_grad = mix_grad * gate * gate_sig
    scaled = act * step
    scaled_half = scaled.astype(BF16)
    grad_half = out_grad.astype(BF16)

    block_head = iota((T, BLK), 1) // 64
    tops, bottoms, scaled_parts, grad_parts = [], [], [], []
    dtop, dbottom = dtop_s[...], dbottom_s[...]
    for k in range(HEADS_BLK):
        mine = block_head == k
        cum_col = cum[:, 64 * k : 64 * k + 1]
        cum_row = cumt_s[pl.ds(step_id * HEADS_BLK + k, 1), :]
        top = jnp.exp2(
            jnp.broadcast_to(cum_col[:HALF], (HALF, HALF)) - cum_row[:, :HALF]
            + causal_s[:HALF, :HALF]
        )
        bottom = jnp.exp2(
            jnp.broadcast_to(cum_col[HALF:], (HALF, T)) - cum_row + causal_s[HALF:, :]
        )
        tops.append((pair_s[:HALF, :HALF] * top).astype(BF16))
        bottoms.append((pair_s[HALF:, :] * bottom).astype(BF16))
        scaled_k = jnp.where(mine, scaled_half, jnp.zeros_like(scaled_half))
        grad_k = jnp.where(mine, grad_half, jnp.zeros_like(grad_half))
        scaled_parts.append(scaled_k)
        grad_parts.append(grad_k)
        dtop = dtop + dot(grad_k[:HALF], scaled_half[:HALF], NT) * top
        dbottom = dbottom + dot(grad_k[HALF:], scaled_half, NT) * bottom
    dtop_s[...] = dtop
    dbottom_s[...] = dbottom
    join = jnp.concatenate
    inner = join(
        [
            dot(join(tops, axis=1), join([v[:HALF] for v in scaled_parts], axis=0)),
            dot(join(bottoms, axis=1), join(scaled_parts, axis=0)),
        ],
        axis=0,
    )
    upper_part = dot(join(tops, axis=0), join([v[:HALF] for v in grad_parts], axis=0), TN)
    dscaled = dot(join(bottoms, axis=0), join([v[HALF:] for v in grad_parts], axis=0), TN)
    dscaled = join([dscaled[:HALF] + upper_part, dscaled[HALF:]], axis=0)

    state = state_ref[...]
    carried = dot(out_low, state, NT) * enter
    from_end = dot(in_high, state, NT) * to_end
    ssm_out = inner + carried
    dscaled = dscaled + from_end
    mixed_out = ssm_out + skip * act
    dgate_ref[...] = (
        mix_grad * mixed_out * gate_sig * (1.0 + gate * (1.0 - gate_sig))
    ).astype(BF16)

    gave_out = dot((out_grad * enter).astype(BF16), state)
    gave_in = dot((scaled * to_end).astype(BF16), state)
    coeff_s[...] += jnp.where(lane < STATE, gave_out, gave_in)

    grad_round = grad_half.astype(F32)
    scaled_round = scaled_half.astype(F32)
    balance = grad_round * ssm_out - scaled_round * dscaled
    row_s[...] += sum(dot(part, spread, NT) for part in split(balance, 2))
    dt_s[...] += dot((dscaled * act).astype(BF16), spread, NT)

    state_wide = state.astype(F32)
    product = state_wide * pltpu.roll(state_wide, STATE, 1)
    through = jnp.sum(jnp.where(iota((BLK, 128), 1) < STATE, product, 0.0), axis=1, keepdims=True)
    through_row = jnp.transpose(jnp.broadcast_to(through, (BLK, BLK)))[0:1]
    end_row = jnp.sum(scaled_round * from_end, axis=0, keepdims=True)
    end_row = end_row + through_row * enter[T - 1 : T]
    skip_row = jnp.sum(out_grad * act, axis=0, keepdims=True)
    row8 = iota((8, BLK), 0)
    both = jnp.where(row8 == 0, end_row, jnp.where(row8 == 1, skip_row, 0.0))
    ends_s[...] += sum(dot(part, spread, NT) for part in split(both, 3))

    dact = step * dscaled + skip * out_grad
    dpre = dact * sig * (1.0 + pre * (1.0 - sig))
    zeros = jnp.zeros((8, BLK), F32)
    dx = weight[0:1] * dpre
    spill = zeros
    for lag in range(KERNEL):
        tap = jnp.sum(dpre * shifted[lag], axis=0, keepdims=True)
        for m in range(LANES_BLK):
            place = lag * (COLS // 128) + step_id * LANES_BLK + m
            bundle_s[pl.ds(place, 1), :] = tap[:, 128 * m : 128 * (m + 1)]
        if lag == 0:
            continue
        masked = dpre * mask_s[lag - 1]
        later = pltpu.roll(jnp.concatenate([masked, zeros], axis=0), T + 8 - lag, 0)[:T]
        dx = dx + weight[lag : lag + 1] * later
        edge = pltpu.roll(jnp.concatenate([zeros, masked[:8]], axis=0), 16 - lag, 0)[:8]
        spill = spill + weight[lag : lag + 1] * edge
    dx_ref[...] = dx.astype(BF16)
    tail_ref[...] = dx[T - 8 :]
    spill_ref[...] = spill

    @pl.when(step_id == STEPS - 1)
    def _():
        params = params_s[...]
        raw = raw_steps(step_ref) + params[0:1]
        rate = jnp.exp(params[1:2])
        decay = step_and_decay(raw, params)[1]
        upper = jnp.where(iota((T, T), 1) >= iota((T, T), 0), 1.0, 0.0)
        ends = ends_s[...]
        ddecay = exact(upper, row_s[...]) + ends[0:1]
        dstep = (dt_s[...] - ddecay * rate) * sigmoid(raw)
        dstep_ref[...] = jnp.transpose(dstep)[: dstep_ref.shape[0]]
        dbias = jnp.sum(dstep, axis=0, keepdims=True)
        drate = jnp.sum(ddecay * decay, axis=0, keepdims=True)
        row = iota((8, 128), 0)
        small = jnp.zeros((8, 128), F32)
        for n, vector in enumerate((dbias, drate, ends[1:2])):
            for m, part in enumerate(split(vector, 2)):
                small = jnp.where(row == 2 * n + m, part.astype(F32), small)
        bundle_s[BUNDLE : BUNDLE + 8] = small
        bundle = bundle_s[...].astype(BF16)
        for shard in range(SHARDS):
            bundle_ref[shard] = bundle
        top_half, bottom_half = dtop.astype(BF16), dbottom.astype(BF16)
        in_low, out_high = in_low_s[...], out_high_s[...]
        out_part = join([dot(top_half, in_low[:HALF]), dot(bottom_half, in_low)], axis=0)
        in_part = dot(bottom_half, out_high[HALF:], TN)
        in_part = join(
            [in_part[:HALF] + dot(top_half, out_high[:HALF], TN), in_part[HALF:]], axis=0
        )
        coeff_ref[...] = (coeff_s[...] + out_part + in_part).astype(BF16)


def mixer_second(*arrays):
    heads = arrays[5].shape[0]
    half = pltpu.VMEM((T, 128), BF16)
    return pl.pallas_call(
        mixer_second_kernel,
        grid=(STEPS,),
        in_specs=mixer_specs(heads) + [pl.BlockSpec((BLK, 128), lambda c: (c, 0))],
        out_specs=[
            column_block(T), column_block(8), column_block(8), column_block(T),
            whole((heads, T)), whole((T, 128)), whole((SHARDS, BUNDLE + 8, 128)),
        ],
        out_shape=[
            jax.ShapeDtypeStruct((T, COLS), BF16),
            jax.ShapeDtypeStruct((8, COLS), F32),
            jax.ShapeDtypeStruct((8, COLS), F32),
            jax.ShapeDtypeStruct((T, COLS), BF16),
            jax.ShapeDtypeStruct((heads, T), F32),
            jax.ShapeDtypeStruct((T, 128), BF16),
            jax.ShapeDtypeStruct((SHARDS, BUNDLE + 8, 128), BF16),
        ],
        scratch_shapes=TOKEN_SCRATCH + [
            pltpu.VMEM((128, T), F32),
            pltpu.VMEM((T, T), F32),
            pltpu.VMEM((T, T), F32),
            pltpu.VMEM((HALF, HALF), F32),
            pltpu.VMEM((HALF, T), F32),
            pltpu.VMEM((T, 128), F32),
            pltpu.VMEM((T, 128), F32),
            pltpu.VMEM((T, 128), F32),
            pltpu.VMEM((8, 128), F32),
            pltpu.VMEM((BUNDLE + 8, 128), F32),
            half, half, half, half,
        ],
        cost_estimate=pl.CostEstimate(flops=18 * 10**9, bytes_accessed=8 * 10**6, transcendentals=0),
        name="mixer_second",
    )(*arrays)


def finish_kernel(bundle_ref, *refs):
    coeff_refs = refs[:LOCAL_HEADS]
    weight_ref, bias_ref, rate_ref, skip_ref, in_ref, out_ref, coeff_s = refs[LOCAL_HEADS:]
    for turn, ref in enumerate(coeff_refs):
        coeff_s[lax.rem(lax.axis_index("head") - turn + LOCAL_HEADS, LOCAL_HEADS)] = ref[...].astype(F32)
    total = bundle_ref[0].astype(F32)
    for shard in range(1, SHARDS):
        total = total + bundle_ref[shard].astype(F32)
    tiles = COLS // 128
    for lag in range(KERNEL):
        for m in range(tiles):
            weight_ref[lag : lag + 1, 128 * m : 128 * (m + 1)] = total[
                lag * tiles + m : lag * tiles + m + 1
            ]
    for n, ref in enumerate((bias_ref, rate_ref, skip_ref)):
        row = BUNDLE + 2 * n
        ref[...] = (total[row : row + 1] + total[row + 1 : row + 2])[:, : ref.shape[1]]
    low, high = coeff_s[0] + coeff_s[1], coeff_s[2] + coeff_s[3]
    left = iota((T, 128), 1) < STATE
    out_ref[...] = jnp.where(left, low, pltpu.roll(high, STATE, 1))
    in_ref[...] = jnp.where(left, pltpu.roll(low, STATE, 1), high)


def finish(bundle, coeffs, heads):
    small = jax.ShapeDtypeStruct((1, heads), F32)
    wide = jax.ShapeDtypeStruct((T, 128), F32)
    return pl.pallas_call(
        finish_kernel,
        in_specs=[IN_VMEM] * (1 + LOCAL_HEADS),
        out_specs=[IN_VMEM] * 6,
        out_shape=[jax.ShapeDtypeStruct((KERNEL, COLS), F32), small, small, small, wide, wide],
        scratch_shapes=[pltpu.VMEM((LOCAL_HEADS, T, 128), F32)],
        compiler_params=GRANT,
        name="finish",
    )(bundle, *coeffs)


ROW = 4
K_AT, V_AT, Q_AT, G_AT = (slice(n * HEAD_DIM, (n + 1) * HEAD_DIM) for n in range(4))
PAIR = (2 * HEAD_DIM, T)


def pack_kernel(k_ref, v_ref, q_ref, g_ref, *refs):
    out_refs, turned_s = refs[:ROW], refs[ROW]
    for ref, place in ((k_ref, K_AT), (v_ref, V_AT), (q_ref, Q_AT), (g_ref, G_AT)):
        turned_part = jnp.transpose(ref[...])
        for head in range(LOCAL_HEADS):
            turned_s[head, place] = turned_part[head * HEAD_DIM : (head + 1) * HEAD_DIM]
    for turn in range(ROW):
        out_refs[turn][...] = turned_s[lax.rem(row_place() + turn, ROW)]


def pack(keys, values, queries, grads):
    return pl.pallas_call(
        pack_kernel,
        in_specs=[IN_VMEM] * 4,
        out_specs=[IN_VMEM] * ROW,
        out_shape=[pltpu.VMEM((4 * HEAD_DIM, T), BF16)] * ROW,
        scratch_shapes=[pltpu.VMEM((LOCAL_HEADS, 4 * HEAD_DIM, T), BF16)],
        name="pack",
    )(keys, values, queries, grads)


def lend_kernel(*refs):
    for turn, ref in enumerate(refs[:ROW]):
        refs[ROW][turn * PAIR[0] : (turn + 1) * PAIR[0]] = ref[: PAIR[0]]


def lend(own):
    return pl.pallas_call(
        lend_kernel,
        in_specs=[IN_VMEM] * ROW,
        out_specs=IN_VMEM,
        out_shape=pltpu.VMEM((ROW * PAIR[0], T), BF16),
        compiler_params=GRANT,
        name="lend",
    )(*own)


def attention_kernel(docs_ref, far_ref, *refs):
    arrived, (dq_ref, own_ref, back_ref, far_s, qg_s, kv_s) = refs[:ROW], refs[ROW:]
    for turn in range(ROW):
        block = lax.rem(row_place() - turn + ROW, ROW)
        kv_s[ROW + block] = arrived[turn][: PAIR[0]]
        qg_s[block] = arrived[turn][PAIR[0] :]
        kv_s[block] = far_ref[turn * PAIR[0] : (turn + 1) * PAIR[0]]
    first_block = lax.div(seq_index(), ROW) * ROW
    later = iota((T, T), 1) > iota((T, T), 0)
    scale = HEAD_DIM ** (-0.5)

    def doc_row(block):
        place = first_block + block
        row = doc_row_of(docs_ref, jnp.maximum(place, 0))
        return row if block >= 0 else jnp.where(place < 0, -1.0, row)

    rows = {block: doc_row(block) for block in range(-ROW, ROW)}
    for i in range(ROW):
        own_doc = columns_of(rows[i])
        qt, gt = qg_s[i, K_AT], qg_s[i, V_AT]
        q, g = jnp.transpose(qt), jnp.transpose(gt)

        def part(gap, place):
            return kv_s[ROW + i - gap, place]

        scores = []
        top = None
        for gap in range(ROW + 1):
            same = own_doc == rows[i - gap]
            if gap == 0:
                same = same & jnp.logical_not(later)
            if gap == ROW:
                same = same & later
            s = jnp.where(same, dot(q, part(gap, K_AT)) * (scale * LOG2E), NEG)
            scores.append(s)
            top = s if top is None else jnp.maximum(top, s)
        top = jnp.max(top, axis=1, keepdims=True)
        expos = [jnp.exp2(s - top) for s in scores]
        total = jnp.sum(sum(expos), axis=1, keepdims=True)
        inverse = 1.0 / jnp.maximum(total, 1.0)
        probs = [e * inverse for e in expos]
        halves = [p.astype(BF16) for p in probs]
        dprobs = [dot(g, part(gap, V_AT)) for gap in range(ROW + 1)]
        delta = sum(h.astype(F32) * d for h, d in zip(halves, dprobs))
        delta = jnp.sum(delta, axis=1, keepdims=True)
        dq = jnp.zeros((HEAD_DIM, T), F32)
        for gap in range(ROW + 1):
            dscore = (probs[gap] * (dprobs[gap] - delta)).astype(BF16)
            dq = dq + dot(part(gap, K_AT), dscore, NT)
            block = i - gap
            ref, index = (own_ref, block) if block >= 0 else (far_s, block + ROW)
            dk, dv = dot(qt, dscore), dot(gt, halves[gap])
            if gap == 0 or (block < 0 and i == 0):
                ref[index, K_AT] = dk
                ref[index, V_AT] = dv
            else:
                ref[index, K_AT] += dk
                ref[index, V_AT] += dv
            if gap == ROW:
                back_ref[index] = far_s[index].astype(BF16)
        dq_ref[i] = (dq * scale).astype(BF16)


def attention(docs, far, own):
    pairs = (ROW, *PAIR)
    return pl.pallas_call(
        attention_kernel,
        in_specs=[IN_VMEM] * (2 + ROW),
        out_specs=[IN_VMEM] * 3,
        out_shape=[
            jax.ShapeDtypeStruct((ROW, HEAD_DIM, T), BF16),
            jax.ShapeDtypeStruct(pairs, F32),
            jax.ShapeDtypeStruct(pairs, BF16),
        ],
        scratch_shapes=[
            pltpu.VMEM(pairs, F32),
            pltpu.VMEM(pairs, BF16),
            pltpu.VMEM((2 * ROW, *PAIR), BF16),
        ],
        cost_estimate=pl.CostEstimate(flops=12 * 10**9, bytes_accessed=8 * 10**6, transcendentals=0),
        name="attention",
    )(docs, far, *own)


def merge_kernel(dq_ref, dkv_ref, back_ref, *out_refs):
    scale = HEAD_DIM ** (-0.5)
    place = row_place()
    for turn, out_ref in enumerate(out_refs):
        block = lax.rem(place + turn, ROW)
        total = dkv_ref[block] + back_ref[block].astype(F32)
        out_ref[K_AT] = (total[K_AT] * scale).astype(BF16)
        out_ref[V_AT] = total[V_AT].astype(BF16)
        out_ref[Q_AT] = dq_ref[block]


def merge(dq, dkv, back):
    return pl.pallas_call(
        merge_kernel,
        in_specs=[IN_VMEM] * 3,
        out_specs=[IN_VMEM] * ROW,
        out_shape=[pltpu.VMEM((3 * HEAD_DIM, T), BF16)] * ROW,
        cost_estimate=pl.CostEstimate(flops=3 * 10**9, bytes_accessed=4 * 10**6, transcendentals=0),
        compiler_params=GRANT,
        name="merge",
    )(dq, dkv, back)


def unpack_kernel(*refs):
    parts, outs, stacked_s = refs[:ROW], refs[ROW : ROW + 3], refs[ROW + 3]
    place = row_place()
    for turn, part in enumerate(parts):
        source = lax.rem(place - turn + ROW, ROW)
        for n, at in enumerate((Q_AT, K_AT, V_AT)):
            stacked_s[n, source] = part[at]
    for n, ref in enumerate(outs):
        stacked = jnp.concatenate([stacked_s[n, h] for h in range(LOCAL_HEADS)], axis=0)
        ref[...] = jnp.transpose(stacked)


def unpack(parts):
    wide = jax.ShapeDtypeStruct((T, LOCAL_HEADS * HEAD_DIM), BF16)
    return pl.pallas_call(
        unpack_kernel,
        in_specs=[IN_VMEM] * ROW,
        out_specs=[IN_VMEM] * 3,
        out_shape=[wide] * 3,
        scratch_shapes=[pltpu.VMEM((3, LOCAL_HEADS, HEAD_DIM, T), BF16)],
        cost_estimate=pl.CostEstimate(flops=2 * 10**9, bytes_accessed=3 * 10**6, transcendentals=0),
        compiler_params=GRANT,
        name="unpack",
    )(*parts)


def passed_along(value, axis, steps):
    count = lax.axis_size(axis)
    initial, last = (max(0, -steps), min(count, count - steps))
    return lax.ppermute(value, axis, [(source, source + steps) for source in range(initial, last)])


def turns(parts, axis):
    count = lax.axis_size(axis)
    return [parts[0]] + [
        lax.ppermute(part, axis, [(n, (n + turn) % count) for n in range(count)])
        for turn, part in enumerate(parts[1:], 1)
    ]


def near(array):
    return pltpu.with_memory_space_constraint(array, pltpu.VMEM)


def exchange(array, axis):
    return lax.all_to_all(array, axis, split_axis=0, concat_axis=0, tiled=True)


def local(
    queries, keys, values, attn_grad, doc_ids, conv_input, conv_weight, step_raw, step_bias,
    rate_log, skip_gain, input_coeff, output_coeff, gate_input, mix_grad,
):
    heads = step_raw.shape[1]
    docs = doc_ids.reshape(SHARDS * T // 128, 128)
    halo = passed_along(conv_input[T - 8 :], SEQ, 1)
    parts = pack(keys, values, queries, attn_grad)
    own = [near(v) for v in turns(parts, "seq_2")]
    lent = lend(own)
    far = passed_along(lent, SEQ, ROW)

    mixer_args = (
        conv_input, halo, conv_weight, gate_input, mix_grad, step_raw.T,
        step_bias.reshape(1, heads), rate_log.reshape(1, heads), skip_gain.reshape(1, heads),
        docs, input_coeff, output_coeff,
    )
    parts = mixer_first(*mixer_args).reshape(SHARDS, SLOT, 128)
    gathered = exchange(parts, SEQ)
    scanned = chain(near(gathered))
    entering = exchange(scanned, SEQ).reshape(COLS, 128)
    dq, dkv, back = attention(docs, near(far), own)
    returned = passed_along(back, SEQ, -ROW)
    dx, tail, spill, dgate, dstep, coeff, bundle = mixer_second(*mixer_args, entering)
    leaving = merge(near(dq), near(dkv), near(returned))
    swapped = turns(leaving, "seq_2")
    spilled = passed_along(spill, SEQ, -1)
    bundles = exchange(bundle, SEQ)
    coeffs = turns([coeff] * LOCAL_HEADS, "head")
    dq, dk, dv = unpack([near(v) for v in swapped])
    grad_weight, grad_bias, grad_rate, grad_skip, sum_in, sum_out = finish(
        near(bundles), [near(v) for v in coeffs], heads
    )
    tail = (tail + spilled).astype(BF16)
    grad_conv = lax.dynamic_update_slice_in_dim(dx, tail, T - 8, 0)
    return (
        dq, dk, dv, grad_conv, dgate, dstep.T, sum_in, sum_out, grad_weight,
        grad_bias.reshape(heads), grad_rate.reshape(heads), grad_skip.reshape(heads),
    )


def solution(mesh):
    finer = Mesh(
        mesh.devices.reshape(4, 2, 4, mesh.shape["head"]), ("seq_0", "seq_1", "seq_2", "head")
    )
    wide = P(SEQ, "head")
    return jax.shard_map(
        local,
        mesh=finer,
        in_specs=(
            wide, wide, wide, wide, P(), wide, P(None, "head"), wide, P("head"), P("head"),
            P("head"), P(SEQ, None), P(SEQ, None), wide, wide,
        ),
        out_specs=(
            wide, wide, wide, wide, wide, wide, P(SEQ, None), P(SEQ, None), P(None, "head"),
            P("head"), P("head"), P("head"),
        ),
        check_vma=False,
    )
```

```python
import jax
import jax.numpy as jnp
from jax import lax
from jax.experimental import pallas as pl
from jax.experimental.pallas import tpu as pltpu
from jax.sharding import Mesh
from jax.sharding import PartitionSpec as P


HEAD_DIM = 224
STATE = 64
KERNEL = 4
SEQ = ("seq_0", "seq_1", "seq_2")
SHARDS = 32
T = 256
LOCAL_HEADS = 4
BLK = 256
HALF = T // 2
HEADS_BLK = BLK // 64
COLS = 1792
STEPS = COLS // BLK
NEG = -1e30
LOG2E = 1.4426950408889634
F32 = jnp.float32
BF16 = jnp.bfloat16

NN = (((1,), (0,)), ((), ()))
NT = (((1,), (1,)), ((), ()))
TN = (((0,), (0,)), ((), ()))


def dot(a, b, dims=NN):
    return lax.dot_general(a, b, dims, preferred_element_type=F32)


def exact(a, b, dims=NN):
    return lax.dot_general(
        a, b, dims, preferred_element_type=F32, precision=lax.Precision.HIGHEST
    )


def split(a, pieces):
    parts = []
    for _ in range(pieces):
        part = a.astype(BF16)
        parts.append(part)
        a = a - part.astype(F32)
    return parts


def sigmoid(v):
    return 0.5 + 0.5 * jnp.tanh(0.5 * v)


def iota(shape, dim):
    return lax.broadcasted_iota(jnp.int32, shape, dim)


def columns_of(row):
    return jnp.transpose(jnp.broadcast_to(row, (T, T)))


def whole(shape):
    return pl.BlockSpec(shape, lambda c: (0,) * len(shape))


def column_block(rows):
    return pl.BlockSpec((rows, BLK), lambda c: (0, c))


IN_VMEM = pl.BlockSpec(memory_space=pltpu.VMEM)
GRANT = pltpu.CompilerParams(vmem_limit_bytes=32 * 2**20)


def seq_index():
    index = 0
    for axis in SEQ:
        index = index * lax.axis_size(axis) + lax.axis_index(axis)
    return index


def row_place():
    return lax.axis_index(SEQ[-1])


def doc_row_of(docs_ref, shard):
    return jnp.concatenate(
        [docs_ref[pl.ds(2 * shard + part, 1), :] for part in range(2)], axis=1
    ).astype(F32)


def doc_rows(docs_ref):
    shard = seq_index()
    own = doc_row_of(docs_ref, shard)
    before = doc_row_of(docs_ref, jnp.maximum(shard - 1, 0))
    return own, jnp.where(shard == 0, -1.0, before)


def group_halves(coeff_ref):
    coeff = coeff_ref[...].astype(F32)
    turned = pltpu.roll(coeff, STATE, 1)
    first = lax.axis_index("head") < 2
    low = iota((T, 128), 1) < STATE
    mine_low = jnp.where(low, jnp.where(first, coeff, turned), 0.0)
    mine_high = jnp.where(low, 0.0, jnp.where(first, turned, coeff))
    return mine_low.astype(BF16), mine_high.astype(BF16)


def padded_params(bias_ref, rate_ref, skip_ref, params_s):
    heads = bias_ref.shape[1]
    params_s[...] = jnp.zeros((8, 128), F32)
    for n, ref in enumerate((bias_ref, rate_ref, skip_ref)):
        params_s[n : n + 1, 0:heads] = ref[...]
    return params_s[...]


def raw_steps(step_ref):
    rows = step_ref.shape[0]
    filled = jnp.concatenate([step_ref[...], jnp.zeros((128 - rows, T), F32)], axis=0)
    return jnp.transpose(filled)


def step_and_decay(raw, params):
    step = jnp.maximum(raw, 0.0) + jnp.log1p(jnp.exp(-jnp.abs(raw)))
    return step, -step * jnp.exp(params[1:2])


def token_setup(docs_ref, step_ref, params, cum_s, step_s, mask_s, prev_s, end_s):
    own_row, before_row = doc_rows(docs_ref)
    own = columns_of(own_row)
    lane = iota((8, T), 1)
    own8 = jnp.broadcast_to(own_row, (8, T))
    before8 = jnp.broadcast_to(before_row, (8, T))
    for lag in range(1, KERNEL):
        lagged = jnp.where(lane < lag, pltpu.roll(before8, lag, 1), pltpu.roll(own8, lag, 1))
        mask_s[lag - 1] = jnp.where(own == columns_of(lagged[0:1]), 1.0, 0.0)
    prev_s[...] = jnp.where(own == before_row[:, T - 1 : T], 0.0, NEG)
    end_s[...] = jnp.where(own == own_row[:, T - 1 : T], 0.0, NEG)
    raw = raw_steps(step_ref) + params[0:1]
    step, decay = step_and_decay(raw, params)
    lower = jnp.where(iota((T, T), 0) >= iota((T, T), 1), 1.0, 0.0)
    cum = exact(lower, decay) * LOG2E
    for n, part in enumerate(split(cum, 3)):
        cum_s[n] = part
    for n, part in enumerate(split(step, 2)):
        step_s[n] = part
    return own, own_row, cum


def spread_of(step_id):
    head = iota((128, BLK), 0)
    owner = step_id * HEADS_BLK + iota((128, BLK), 1) // 64
    return jnp.where(head == owner, 1.0, 0.0).astype(BF16)


def block_gains(step_id, cum_s, step_s, prev_s, end_s):
    spread = spread_of(step_id)
    cum = dot(cum_s[0], spread) + dot(cum_s[1], spread) + dot(cum_s[2], spread)
    step = dot(step_s[0], spread) + dot(step_s[1], spread)
    enter = jnp.exp2(cum + prev_s[...])
    to_end = jnp.exp2(cum[T - 1 : T] - cum + end_s[...])
    return spread, cum, step, enter, to_end


def conv_pre(x, halo, weight, mask_s):
    extended = jnp.concatenate([halo.astype(F32), x.astype(F32)], axis=0)
    shifted = [extended[8:]]
    summed = weight[0:1] * shifted[0]
    for lag in range(1, KERNEL):
        moved = pltpu.roll(extended, lag, 0)[8:] * mask_s[lag - 1]
        shifted.append(moved)
        summed = summed + weight[lag : lag + 1] * moved
    return summed, shifted


ROWS = COLS // SHARDS
GROUPS8 = ROWS // 8
SLOT = ROWS + 8


def mixer_first_kernel(
    x_ref, halo_ref, weight_ref, gate_ref, grad_ref, step_ref, bias_ref, rate_ref,
    skip_ref, docs_ref, in_ref, out_ref,
    parts_ref,
    cum_s, step_s, mask_s, prev_s, end_s, params_s, state_s, in_s, out_s,
):
    step_id = pl.program_id(0)

    @pl.when(step_id == 0)
    def _():
        params = padded_params(bias_ref, rate_ref, skip_ref, params_s)
        cum = token_setup(
            docs_ref, step_ref, params, cum_s, step_s, mask_s, prev_s, end_s
        )[2]
        through = jnp.exp2(cum[T - 1 : T] + prev_s[T - 1 : T, 0:1])
        high, low = split(through, 2)
        row = iota((8, 128), 0)
        both = jnp.where(row == 0, high.astype(F32), jnp.where(row == 1, low.astype(F32), 0.0))
        for shard in range(SHARDS):
            state_s[SLOT * shard + ROWS : SLOT * (shard + 1)] = both
        in_s[...] = group_halves(in_ref)[0]
        out_s[...] = group_halves(out_ref)[1]

    _, _, step, enter, to_end = block_gains(step_id, cum_s, step_s, prev_s, end_s)
    pre, _ = conv_pre(x_ref[...], halo_ref[...], weight_ref[...], mask_s)
    act = pre * sigmoid(pre)
    gate = gate_ref[...].astype(F32)
    out_grad = grad_ref[...].astype(F32) * gate * sigmoid(gate)
    ended = (act * step * to_end).astype(BF16)
    entered = (out_grad * enter).astype(BF16)
    state = dot(ended, in_s[...], TN) + dot(entered, out_s[...], TN)
    for part in range(BLK // 8):
        place = step_id * (BLK // 8) + part
        target = lax.div(place, GROUPS8)
        offset = SLOT * target + 8 * (place - GROUPS8 * target)
        state_s[pl.ds(pl.multiple_of(offset, 8), 8), :] = state[8 * part : 8 * part + 8]

    @pl.when(step_id == STEPS - 1)
    def _():
        parts_ref[...] = state_s[...].astype(BF16)


TOKEN_SCRATCH = [
    pltpu.VMEM((3, T, 128), BF16),
    pltpu.VMEM((2, T, 128), BF16),
    pltpu.VMEM((KERNEL - 1, T, BLK), F32),
    pltpu.VMEM((T, BLK), F32),
    pltpu.VMEM((T, BLK), F32),
    pltpu.VMEM((8, 128), F32),
]


def mixer_specs(heads):
    return [
        column_block(T), column_block(8), column_block(KERNEL), column_block(T),
        column_block(T), whole((heads, T)), whole((1, heads)), whole((1, heads)),
        whole((1, heads)), whole((SHARDS * T // 128, 128)), whole((T, 128)), whole((T, 128)),
    ]


def mixer_first(*arrays):
    heads = arrays[5].shape[0]
    return pl.pallas_call(
        mixer_first_kernel,
        grid=(STEPS,),
        in_specs=mixer_specs(heads),
        out_specs=whole((SHARDS * SLOT, 128)),
        out_shape=jax.ShapeDtypeStruct((SHARDS * SLOT, 128), BF16),
        scratch_shapes=TOKEN_SCRATCH + [
            pltpu.VMEM((SHARDS * SLOT, 128), F32),
            pltpu.VMEM((T, 128), BF16),
            pltpu.VMEM((T, 128), BF16),
        ],
        cost_estimate=pl.CostEstimate(flops=8 * 10**9, bytes_accessed=4 * 10**6, transcendentals=0),
        name="mixer_first",
    )(*arrays)


def chain_kernel(parts_ref, out_ref, forward_s):
    slot = seq_index()
    owner = (slot * ROWS + iota((ROWS, 128), 0)) // 64
    choose = jnp.where(owner == iota((ROWS, 128), 1), 1.0, 0.0)
    lane = iota((ROWS, 128), 1)
    through = []
    carry = jnp.zeros((ROWS, 128), F32)
    for shard in range(SHARDS):
        row = parts_ref[shard, ROWS : ROWS + 1].astype(F32)
        row = row + parts_ref[shard, ROWS + 1 : ROWS + 2].astype(F32)
        gain = jnp.sum(choose * row, axis=1, keepdims=True)
        through.append(gain)
        forward_s[shard] = carry
        carry = gain * carry + parts_ref[shard, 0:ROWS].astype(F32)
    carry = jnp.zeros((ROWS, 128), F32)
    for shard in reversed(range(SHARDS)):
        out_ref[shard] = jnp.where(lane < STATE, forward_s[shard], carry).astype(BF16)
        carry = through[shard] * carry + parts_ref[shard, 0:ROWS].astype(F32)


def chain(parts):
    return pl.pallas_call(
        chain_kernel,
        in_specs=[IN_VMEM],
        out_specs=IN_VMEM,
        out_shape=jax.ShapeDtypeStruct((SHARDS, ROWS, 128), BF16),
        scratch_shapes=[pltpu.VMEM((SHARDS, ROWS, 128), F32)],
        cost_estimate=pl.CostEstimate(flops=2 * 10**9, bytes_accessed=10**6, transcendentals=0),
        name="chain",
    )(parts)


BUNDLE = KERNEL * COLS // 128
LANES_BLK = BLK // 128


def mixer_inner_kernel(
    x_ref, halo_ref, weight_ref, gate_ref, grad_ref, step_ref, bias_ref, rate_ref,
    skip_ref, docs_ref, in_ref, out_ref,
    inner_ref, dscaled_ref, dtop_ref, dbottom_ref,
    cum_s, step_s, mask_s, prev_s, end_s, params_s,
    cumt_s, pair_s, causal_s, dtop_s, dbottom_s,
):
    step_id = pl.program_id(0)

    @pl.when(step_id == 0)
    def _():
        params = padded_params(bias_ref, rate_ref, skip_ref, params_s)
        own, own_row, cum = token_setup(
            docs_ref, step_ref, params, cum_s, step_s, mask_s, prev_s, end_s
        )
        cumt_s[...] = jnp.transpose(cum)
        same = (own == own_row) & (iota((T, T), 0) >= iota((T, T), 1))
        causal_s[...] = jnp.where(same, 0.0, NEG)
        pair_s[...] = dot(group_halves(out_ref)[0], group_halves(in_ref)[0], NT)
        dtop_s[...] = jnp.zeros((HALF, HALF), F32)
        dbottom_s[...] = jnp.zeros((HALF, T), F32)

    spread = spread_of(step_id)
    cum = dot(cum_s[0], spread) + dot(cum_s[1], spread) + dot(cum_s[2], spread)
    step = dot(step_s[0], spread) + dot(step_s[1], spread)
    pre, _ = conv_pre(x_ref[...], halo_ref[...], weight_ref[...], mask_s)
    gate = gate_ref[...].astype(F32)
    scaled_half = (pre * sigmoid(pre) * step).astype(BF16)
    grad_half = (grad_ref[...].astype(F32) * gate * sigmoid(gate)).astype(BF16)

    block_head = iota((T, BLK), 1) // 64
    tops, bottoms, scaled_parts, grad_parts = [], [], [], []
    dtop, dbottom = dtop_s[...], dbottom_s[...]
    for k in range(HEADS_BLK):
        mine = block_head == k
        cum_col = cum[:, 64 * k : 64 * k + 1]
        cum_row = cumt_s[pl.ds(step_id * HEADS_BLK + k, 1), :]
        top = jnp.exp2(
            jnp.broadcast_to(cum_col[:HALF], (HALF, HALF)) - cum_row[:, :HALF]
            + causal_s[:HALF, :HALF]
        )
        bottom = jnp.exp2(
            jnp.broadcast_to(cum_col[HALF:], (HALF, T)) - cum_row + causal_s[HALF:, :]
        )
        tops.append((pair_s[:HALF, :HALF] * top).astype(BF16))
        bottoms.append((pair_s[HALF:, :] * bottom).astype(BF16))
        scaled_k = jnp.where(mine, scaled_half, jnp.zeros_like(scaled_half))
        grad_k = jnp.where(mine, grad_half, jnp.zeros_like(grad_half))
        scaled_parts.append(scaled_k)
        grad_parts.append(grad_k)
        dtop = dtop + dot(grad_k[:HALF], scaled_half[:HALF], NT) * top
        dbottom = dbottom + dot(grad_k[HALF:], scaled_half, NT) * bottom
    dtop_s[...] = dtop
    dbottom_s[...] = dbottom
    join = jnp.concatenate
    inner_ref[...] = join(
        [
            dot(join(tops, axis=1), join([v[:HALF] for v in scaled_parts], axis=0)),
            dot(join(bottoms, axis=1), join(scaled_parts, axis=0)),
        ],
        axis=0,
    )
    upper_part = dot(join(tops, axis=0), join([v[:HALF] for v in grad_parts], axis=0), TN)
    dscaled = dot(join(bottoms, axis=0), join([v[HALF:] for v in grad_parts], axis=0), TN)
    dscaled_ref[...] = join([dscaled[:HALF] + upper_part, dscaled[HALF:]], axis=0)
    dtop_ref[...] = dtop
    dbottom_ref[...] = dbottom


def mixer_inner(*arrays):
    heads = arrays[5].shape[0]
    return pl.pallas_call(
        mixer_inner_kernel,
        grid=(STEPS,),
        in_specs=mixer_specs(heads),
        out_specs=[column_block(T), column_block(T), whole((HALF, HALF)), whole((HALF, T))],
        out_shape=[
            jax.ShapeDtypeStruct((T, COLS), F32),
            jax.ShapeDtypeStruct((T, COLS), F32),
            jax.ShapeDtypeStruct((HALF, HALF), F32),
            jax.ShapeDtypeStruct((HALF, T), F32),
        ],
        scratch_shapes=TOKEN_SCRATCH + [
            pltpu.VMEM((128, T), F32),
            pltpu.VMEM((T, T), F32),
            pltpu.VMEM((T, T), F32),
            pltpu.VMEM((HALF, HALF), F32),
            pltpu.VMEM((HALF, T), F32),
        ],
        cost_estimate=pl.CostEstimate(flops=10**10, bytes_accessed=6 * 10**6, transcendentals=0),
        name="mixer_inner",
    )(*arrays)


def mixer_second_kernel(
    x_ref, halo_ref, weight_ref, gate_ref, grad_ref, step_ref, bias_ref, rate_ref,
    skip_ref, docs_ref, in_ref, out_ref, inner_ref, dscaled_ref, dtop_ref, dbottom_ref,
    state_ref,
    dx_ref, tail_ref, spill_ref, dgate_ref, dstep_ref, coeff_ref, bundle_ref,
    cum_s, step_s, mask_s, prev_s, end_s, params_s,
    coeff_s, row_s, dt_s, ends_s, bundle_s,
    in_low_s, in_high_s, out_low_s, out_high_s,
):
    step_id = pl.program_id(0)
    lane = iota((T, 128), 1)

    @pl.when(step_id == 0)
    def _():
        params = padded_params(bias_ref, rate_ref, skip_ref, params_s)
        token_setup(docs_ref, step_ref, params, cum_s, step_s, mask_s, prev_s, end_s)
        in_low_s[...], in_high_s[...] = group_halves(in_ref)
        out_low_s[...], out_high_s[...] = group_halves(out_ref)
        coeff_s[...] = jnp.zeros((T, 128), F32)
        row_s[...] = jnp.zeros((T, 128), F32)
        dt_s[...] = jnp.zeros((T, 128), F32)
        ends_s[...] = jnp.zeros((8, 128), F32)

    out_low = out_low_s[...]
    in_high = in_high_s[...]
    spread, _, step, enter, to_end = block_gains(step_id, cum_s, step_s, prev_s, end_s)
    skip = sum(dot(part, spread) for part in split(params_s[...], 3))[2:3]
    weight = weight_ref[...]
    pre, shifted = conv_pre(x_ref[...], halo_ref[...], weight, mask_s)
    sig = sigmoid(pre)
    act = pre * sig
    gate = gate_ref[...].astype(F32)
    gate_sig = sigmoid(gate)
    mix_grad = grad_ref[...].astype(F32)
    out_grad = mix_grad * gate * gate_sig
    scaled = act * step
    scaled_half = scaled.astype(BF16)
    grad_half = out_grad.astype(BF16)

    join = jnp.concatenate
    inner, dscaled = inner_ref[...], dscaled_ref[...]
    state = state_ref[...]
    carried = dot(out_low, state, NT) * enter
    from_end = dot(in_high, state, NT) * to_end
    ssm_out = inner + carried
    dscaled = dscaled + from_end
    mixed_out = ssm_out + skip * act
    dgate_ref[...] = (
        mix_grad * mixed_out * gate_sig * (1.0 + gate * (1.0 - gate_sig))
    ).astype(BF16)

    gave_out = dot((out_grad * enter).astype(BF16), state)
    gave_in = dot((scaled * to_end).astype(BF16), state)
    coeff_s[...] += jnp.where(lane < STATE, gave_out, gave_in)

    grad_round = grad_half.astype(F32)
    scaled_round = scaled_half.astype(F32)
    balance = grad_round * ssm_out - scaled_round * dscaled
    row_s[...] += sum(dot(part, spread, NT) for part in split(balance, 2))
    dt_s[...] += dot((dscaled * act).astype(BF16), spread, NT)

    state_wide = state.astype(F32)
    product = state_wide * pltpu.roll(state_wide, STATE, 1)
    through = jnp.sum(jnp.where(iota((BLK, 128), 1) < STATE, product, 0.0), axis=1, keepdims=True)
    through_row = jnp.transpose(jnp.broadcast_to(through, (BLK, BLK)))[0:1]
    end_row = jnp.sum(scaled_round * from_end, axis=0, keepdims=True)
    end_row = end_row + through_row * enter[T - 1 : T]
    skip_row = jnp.sum(out_grad * act, axis=0, keepdims=True)
    row8 = iota((8, BLK), 0)
    both = jnp.where(row8 == 0, end_row, jnp.where(row8 == 1, skip_row, 0.0))
    ends_s[...] += sum(dot(part, spread, NT) for part in split(both, 3))

    dact = step * dscaled + skip * out_grad
    dpre = dact * sig * (1.0 + pre * (1.0 - sig))
    zeros = jnp.zeros((8, BLK), F32)
    dx = weight[0:1] * dpre
    spill = zeros
    for lag in range(KERNEL):
        tap = jnp.sum(dpre * shifted[lag], axis=0, keepdims=True)
        for m in range(LANES_BLK):
            place = lag * (COLS // 128) + step_id * LANES_BLK + m
            bundle_s[pl.ds(place, 1), :] = tap[:, 128 * m : 128 * (m + 1)]
        if lag == 0:
            continue
        masked = dpre * mask_s[lag - 1]
        later = pltpu.roll(jnp.concatenate([masked, zeros], axis=0), T + 8 - lag, 0)[:T]
        dx = dx + weight[lag : lag + 1] * later
        edge = pltpu.roll(jnp.concatenate([zeros, masked[:8]], axis=0), 16 - lag, 0)[:8]
        spill = spill + weight[lag : lag + 1] * edge
    dx_ref[...] = dx.astype(BF16)
    tail_ref[...] = dx[T - 8 :]
    spill_ref[...] = spill

    @pl.when(step_id == STEPS - 1)
    def _():
        params = params_s[...]
        raw = raw_steps(step_ref) + params[0:1]
        rate = jnp.exp(params[1:2])
        decay = step_and_decay(raw, params)[1]
        upper = jnp.where(iota((T, T), 1) >= iota((T, T), 0), 1.0, 0.0)
        ends = ends_s[...]
        ddecay = exact(upper, row_s[...]) + ends[0:1]
        dstep = (dt_s[...] - ddecay * rate) * sigmoid(raw)
        dstep_ref[...] = jnp.transpose(dstep)[: dstep_ref.shape[0]]
        dbias = jnp.sum(dstep, axis=0, keepdims=True)
        drate = jnp.sum(ddecay * decay, axis=0, keepdims=True)
        row = iota((8, 128), 0)
        small = jnp.zeros((8, 128), F32)
        for n, vector in enumerate((dbias, drate, ends[1:2])):
            for m, part in enumerate(split(vector, 2)):
                small = jnp.where(row == 2 * n + m, part.astype(F32), small)
        bundle_s[BUNDLE : BUNDLE + 8] = small
        bundle = bundle_s[...].astype(BF16)
        for shard in range(SHARDS):
            bundle_ref[shard] = bundle
        top_half, bottom_half = dtop_ref[...].astype(BF16), dbottom_ref[...].astype(BF16)
        in_low, out_high = in_low_s[...], out_high_s[...]
        out_part = join([dot(top_half, in_low[:HALF]), dot(bottom_half, in_low)], axis=0)
        in_part = dot(bottom_half, out_high[HALF:], TN)
        in_part = join(
            [in_part[:HALF] + dot(top_half, out_high[:HALF], TN), in_part[HALF:]], axis=0
        )
        coeff_ref[...] = (coeff_s[...] + out_part + in_part).astype(BF16)


def mixer_second(*arrays):
    heads = arrays[5].shape[0]
    half = pltpu.VMEM((T, 128), BF16)
    return pl.pallas_call(
        mixer_second_kernel,
        grid=(STEPS,),
        in_specs=mixer_specs(heads) + [
            column_block(T), column_block(T), whole((HALF, HALF)), whole((HALF, T)),
            pl.BlockSpec((BLK, 128), lambda c: (c, 0)),
        ],
        out_specs=[
            column_block(T), column_block(8), column_block(8), column_block(T),
            whole((heads, T)), whole((T, 128)), whole((SHARDS, BUNDLE + 8, 128)),
        ],
        out_shape=[
            jax.ShapeDtypeStruct((T, COLS), BF16),
            jax.ShapeDtypeStruct((8, COLS), F32),
            jax.ShapeDtypeStruct((8, COLS), F32),
            jax.ShapeDtypeStruct((T, COLS), BF16),
            jax.ShapeDtypeStruct((heads, T), F32),
            jax.ShapeDtypeStruct((T, 128), BF16),
            jax.ShapeDtypeStruct((SHARDS, BUNDLE + 8, 128), BF16),
        ],
        scratch_shapes=TOKEN_SCRATCH + [
            pltpu.VMEM((T, 128), F32),
            pltpu.VMEM((T, 128), F32),
            pltpu.VMEM((T, 128), F32),
            pltpu.VMEM((8, 128), F32),
            pltpu.VMEM((BUNDLE + 8, 128), F32),
            half, half, half, half,
        ],
        cost_estimate=pl.CostEstimate(flops=18 * 10**9, bytes_accessed=8 * 10**6, transcendentals=0),
        name="mixer_second",
    )(*arrays)


def finish_kernel(bundle_ref, *refs):
    coeff_refs = refs[:LOCAL_HEADS]
    weight_ref, bias_ref, rate_ref, skip_ref, in_ref, out_ref, coeff_s = refs[LOCAL_HEADS:]
    for turn, ref in enumerate(coeff_refs):
        coeff_s[lax.rem(lax.axis_index("head") - turn + LOCAL_HEADS, LOCAL_HEADS)] = ref[...].astype(F32)
    total = bundle_ref[0].astype(F32)
    for shard in range(1, SHARDS):
        total = total + bundle_ref[shard].astype(F32)
    tiles = COLS // 128
    for lag in range(KERNEL):
        for m in range(tiles):
            weight_ref[lag : lag + 1, 128 * m : 128 * (m + 1)] = total[
                lag * tiles + m : lag * tiles + m + 1
            ]
    for n, ref in enumerate((bias_ref, rate_ref, skip_ref)):
        row = BUNDLE + 2 * n
        ref[...] = (total[row : row + 1] + total[row + 1 : row + 2])[:, : ref.shape[1]]
    low, high = coeff_s[0] + coeff_s[1], coeff_s[2] + coeff_s[3]
    left = iota((T, 128), 1) < STATE
    out_ref[...] = jnp.where(left, low, pltpu.roll(high, STATE, 1))
    in_ref[...] = jnp.where(left, pltpu.roll(low, STATE, 1), high)


def finish(bundle, coeffs, heads):
    small = jax.ShapeDtypeStruct((1, heads), F32)
    wide = jax.ShapeDtypeStruct((T, 128), F32)
    return pl.pallas_call(
        finish_kernel,
        in_specs=[IN_VMEM] * (1 + LOCAL_HEADS),
        out_specs=[IN_VMEM] * 6,
        out_shape=[jax.ShapeDtypeStruct((KERNEL, COLS), F32), small, small, small, wide, wide],
        scratch_shapes=[pltpu.VMEM((LOCAL_HEADS, T, 128), F32)],
        name="finish",
    )(bundle, *coeffs)


ROW = 4
K_AT, V_AT, Q_AT, G_AT = (slice(n * HEAD_DIM, (n + 1) * HEAD_DIM) for n in range(4))
PAIR = (2 * HEAD_DIM, T)


def pack_kernel(k_ref, v_ref, q_ref, g_ref, *refs):
    out_refs, turned_s = refs[:ROW], refs[ROW]
    for ref, place in ((k_ref, K_AT), (v_ref, V_AT), (q_ref, Q_AT), (g_ref, G_AT)):
        turned_part = jnp.transpose(ref[...])
        for head in range(LOCAL_HEADS):
            turned_s[head, place] = turned_part[head * HEAD_DIM : (head + 1) * HEAD_DIM]
    for turn in range(ROW):
        out_refs[turn][...] = turned_s[lax.rem(row_place() + turn, ROW)]


def pack(keys, values, queries, grads):
    return pl.pallas_call(
        pack_kernel,
        in_specs=[IN_VMEM] * 4,
        out_specs=[IN_VMEM] * ROW,
        out_shape=[jax.ShapeDtypeStruct((4 * HEAD_DIM, T), BF16)] * ROW,
        scratch_shapes=[pltpu.VMEM((LOCAL_HEADS, 4 * HEAD_DIM, T), BF16)],
        name="pack",
    )(keys, values, queries, grads)


def lend_kernel(*refs):
    for turn, ref in enumerate(refs[:ROW]):
        refs[ROW][turn * PAIR[0] : (turn + 1) * PAIR[0]] = ref[: PAIR[0]]


def lend(own):
    return pl.pallas_call(
        lend_kernel,
        in_specs=[IN_VMEM] * ROW,
        out_specs=IN_VMEM,
        out_shape=jax.ShapeDtypeStruct((ROW * PAIR[0], T), BF16),
        name="lend",
    )(*own)


def attention_kernel(docs_ref, far_ref, *refs):
    arrived, (dq_ref, own_ref, back_ref, far_s, qg_s, kv_s) = refs[:ROW], refs[ROW:]
    for turn in range(ROW):
        block = lax.rem(row_place() - turn + ROW, ROW)
        kv_s[ROW + block] = arrived[turn][: PAIR[0]]
        qg_s[block] = arrived[turn][PAIR[0] :]
        kv_s[block] = far_ref[turn * PAIR[0] : (turn + 1) * PAIR[0]]
    first_block = lax.div(seq_index(), ROW) * ROW
    later = iota((T, T), 1) > iota((T, T), 0)
    scale = HEAD_DIM ** (-0.5)

    def doc_row(block):
        place = first_block + block
        row = doc_row_of(docs_ref, jnp.maximum(place, 0))
        return row if block >= 0 else jnp.where(place < 0, -1.0, row)

    rows = {block: doc_row(block) for block in range(-ROW, ROW)}
    for i in range(ROW):
        own_doc = columns_of(rows[i])
        qt, gt = qg_s[i, K_AT], qg_s[i, V_AT]
        q, g = jnp.transpose(qt), jnp.transpose(gt)

        def part(gap, place):
            return kv_s[ROW + i - gap, place]

        scores = []
        top = None
        for gap in range(ROW + 1):
            same = own_doc == rows[i - gap]
            if gap == 0:
                same = same & jnp.logical_not(later)
            if gap == ROW:
                same = same & later
            s = jnp.where(same, dot(q, part(gap, K_AT)) * (scale * LOG2E), NEG)
            scores.append(s)
            top = s if top is None else jnp.maximum(top, s)
        top = jnp.max(top, axis=1, keepdims=True)
        expos = [jnp.exp2(s - top) for s in scores]
        total = jnp.sum(sum(expos), axis=1, keepdims=True)
        inverse = 1.0 / jnp.maximum(total, 1.0)
        probs = [e * inverse for e in expos]
        halves = [p.astype(BF16) for p in probs]
        dprobs = [dot(g, part(gap, V_AT)) for gap in range(ROW + 1)]
        delta = sum(h.astype(F32) * d for h, d in zip(halves, dprobs))
        delta = jnp.sum(delta, axis=1, keepdims=True)
        dq = jnp.zeros((HEAD_DIM, T), F32)
        for gap in range(ROW + 1):
            dscore = (probs[gap] * (dprobs[gap] - delta)).astype(BF16)
            dq = dq + dot(part(gap, K_AT), dscore, NT)
            block = i - gap
            ref, index = (own_ref, block) if block >= 0 else (far_s, block + ROW)
            dk, dv = dot(qt, dscore), dot(gt, halves[gap])
            if gap == 0 or (block < 0 and i == 0):
                ref[index, K_AT] = dk
                ref[index, V_AT] = dv
            else:
                ref[index, K_AT] += dk
                ref[index, V_AT] += dv
            if gap == ROW:
                back_ref[index] = far_s[index].astype(BF16)
        dq_ref[i] = (dq * scale).astype(BF16)


def attention(docs, far, own):
    pairs = (ROW, *PAIR)
    return pl.pallas_call(
        attention_kernel,
        in_specs=[IN_VMEM] * (2 + ROW),
        out_specs=[IN_VMEM] * 3,
        out_shape=[
            jax.ShapeDtypeStruct((ROW, HEAD_DIM, T), BF16),
            jax.ShapeDtypeStruct(pairs, F32),
            jax.ShapeDtypeStruct(pairs, BF16),
        ],
        scratch_shapes=[
            pltpu.VMEM(pairs, F32),
            pltpu.VMEM(pairs, BF16),
            pltpu.VMEM((2 * ROW, *PAIR), BF16),
        ],
        cost_estimate=pl.CostEstimate(flops=12 * 10**9, bytes_accessed=8 * 10**6, transcendentals=0),
        name="attention",
    )(docs, far, *own)


def merge_kernel(dq_ref, dkv_ref, back_ref, *out_refs):
    scale = HEAD_DIM ** (-0.5)
    place = row_place()
    for turn, out_ref in enumerate(out_refs):
        block = lax.rem(place + turn, ROW)
        total = dkv_ref[block] + back_ref[block].astype(F32)
        out_ref[K_AT] = (total[K_AT] * scale).astype(BF16)
        out_ref[V_AT] = total[V_AT].astype(BF16)
        out_ref[Q_AT] = dq_ref[block]


def merge(dq, dkv, back):
    return pl.pallas_call(
        merge_kernel,
        in_specs=[IN_VMEM] * 3,
        out_specs=[IN_VMEM] * ROW,
        out_shape=[pltpu.VMEM((3 * HEAD_DIM, T), BF16)] * ROW,
        cost_estimate=pl.CostEstimate(flops=3 * 10**9, bytes_accessed=4 * 10**6, transcendentals=0),
        compiler_params=GRANT,
        name="merge",
    )(dq, dkv, back)


def unpack_kernel(*refs):
    parts, outs, stacked_s = refs[:ROW], refs[ROW : ROW + 3], refs[ROW + 3]
    place = row_place()
    for turn, part in enumerate(parts):
        source = lax.rem(place - turn + ROW, ROW)
        for n, at in enumerate((Q_AT, K_AT, V_AT)):
            stacked_s[n, source] = part[at]
    for n, ref in enumerate(outs):
        stacked = jnp.concatenate([stacked_s[n, h] for h in range(LOCAL_HEADS)], axis=0)
        ref[...] = jnp.transpose(stacked)


def unpack(parts):
    wide = jax.ShapeDtypeStruct((T, LOCAL_HEADS * HEAD_DIM), BF16)
    return pl.pallas_call(
        unpack_kernel,
        in_specs=[IN_VMEM] * ROW,
        out_specs=[IN_VMEM] * 3,
        out_shape=[wide] * 3,
        scratch_shapes=[pltpu.VMEM((3, LOCAL_HEADS, HEAD_DIM, T), BF16)],
        cost_estimate=pl.CostEstimate(flops=2 * 10**9, bytes_accessed=3 * 10**6, transcendentals=0),
        name="unpack",
    )(*parts)


def passed_along(value, axis, steps):
    count = lax.axis_size(axis)
    initial, last = (max(0, -steps), min(count, count - steps))
    return lax.ppermute(value, axis, [(source, source + steps) for source in range(initial, last)])


def turns(parts, axis):
    count = lax.axis_size(axis)
    return [parts[0]] + [
        lax.ppermute(part, axis, [(n, (n + turn) % count) for n in range(count)])
        for turn, part in enumerate(parts[1:], 1)
    ]


def near(array):
    return pltpu.with_memory_space_constraint(array, pltpu.VMEM)


def exchange(array, axis):
    return lax.all_to_all(array, axis, split_axis=0, concat_axis=0, tiled=True)


def local(
    queries, keys, values, attn_grad, doc_ids, conv_input, conv_weight, step_raw, step_bias,
    rate_log, skip_gain, input_coeff, output_coeff, gate_input, mix_grad,
):
    heads = step_raw.shape[1]
    docs = doc_ids.reshape(SHARDS * T // 128, 128)
    halo = passed_along(conv_input[T - 8 :], SEQ, 1)
    parts = pack(keys, values, queries, attn_grad)
    own = [near(v) for v in turns(parts, "seq_2")]
    lent = lend(own)
    far = passed_along(lent, SEQ, ROW)

    mixer_args = (
        conv_input, halo, conv_weight, gate_input, mix_grad, step_raw.T,
        step_bias.reshape(1, heads), rate_log.reshape(1, heads), skip_gain.reshape(1, heads),
        docs, input_coeff, output_coeff,
    )
    parts = mixer_first(*mixer_args).reshape(SHARDS, SLOT, 128)
    gathered = exchange(parts, SEQ)
    scanned = chain(near(gathered))
    entering = exchange(scanned, SEQ).reshape(COLS, 128)
    inside = mixer_inner(*mixer_args)
    dq, dkv, back = attention(docs, near(far), own)
    returned = passed_along(back, SEQ, -ROW)
    dx, tail, spill, dgate, dstep, coeff, bundle = mixer_second(
        *mixer_args, *inside, entering
    )
    leaving = merge(near(dq), near(dkv), near(returned))
    swapped = turns(leaving, "seq_2")
    spilled = passed_along(spill, SEQ, -1)
    bundles = exchange(bundle, SEQ)
    coeffs = turns([coeff] * LOCAL_HEADS, "head")
    dq, dk, dv = unpack([near(v) for v in swapped])
    grad_weight, grad_bias, grad_rate, grad_skip, sum_in, sum_out = finish(
        near(bundles), [near(v) for v in coeffs], heads
    )
    tail = (tail + spilled).astype(BF16)
    grad_conv = lax.dynamic_update_slice_in_dim(dx, tail, T - 8, 0)
    return (
        dq, dk, dv, grad_conv, dgate, dstep.T, sum_in, sum_out, grad_weight,
        grad_bias.reshape(heads), grad_rate.reshape(heads), grad_skip.reshape(heads),
    )


def solution(mesh):
    finer = Mesh(
        mesh.devices.reshape(4, 2, 4, mesh.shape["head"]), ("seq_0", "seq_1", "seq_2", "head")
    )
    wide = P(SEQ, "head")
    return jax.shard_map(
        local,
        mesh=finer,
        in_specs=(
            wide, wide, wide, wide, P(), wide, P(None, "head"), wide, P("head"), P("head"),
            P("head"), P(SEQ, None), P(SEQ, None), wide, wide,
        ),
        out_specs=(
            wide, wide, wide, wide, wide, wide, P(SEQ, None), P(SEQ, None), P(None, "head"),
            P("head"), P("head"), P("head"),
        ),
        check_vma=False,
    )
```

```python
import jax
import jax.numpy as jnp
from jax import lax
from jax.experimental import pallas as pl
from jax.experimental.pallas import tpu as pltpu
from jax.sharding import Mesh
from jax.sharding import PartitionSpec as P


HEAD_DIM = 224
STATE = 64
KERNEL = 4
SEQ = ("seq_0", "seq_1", "seq_2")
SHARDS = 32
T = 256
LOCAL_HEADS = 4
BLK = 256
HALF = T // 2
HEADS_BLK = BLK // 64
COLS = 1792
STEPS = COLS // BLK
NEG = -1e30
LOG2E = 1.4426950408889634
F32 = jnp.float32
BF16 = jnp.bfloat16

NN = (((1,), (0,)), ((), ()))
NT = (((1,), (1,)), ((), ()))
TN = (((0,), (0,)), ((), ()))


def dot(a, b, dims=NN):
    return lax.dot_general(a, b, dims, preferred_element_type=F32)


def exact(a, b, dims=NN):
    return lax.dot_general(
        a, b, dims, preferred_element_type=F32, precision=lax.Precision.HIGHEST
    )


def split(a, pieces):
    parts = []
    for _ in range(pieces):
        part = a.astype(BF16)
        parts.append(part)
        a = a - part.astype(F32)
    return parts


def sigmoid(v):
    return 0.5 + 0.5 * jnp.tanh(0.5 * v)


def iota(shape, dim):
    return lax.broadcasted_iota(jnp.int32, shape, dim)


def columns_of(row):
    return jnp.transpose(jnp.broadcast_to(row, (T, T)))


def whole(shape):
    return pl.BlockSpec(shape, lambda c: (0,) * len(shape))


def column_block(rows):
    return pl.BlockSpec((rows, BLK), lambda c: (0, c))


IN_VMEM = pl.BlockSpec(memory_space=pltpu.VMEM)


def seq_index():
    index = 0
    for axis in SEQ:
        index = index * lax.axis_size(axis) + lax.axis_index(axis)
    return index


def row_place():
    return lax.axis_index(SEQ[-1])


def doc_row_of(docs_ref, shard):
    return jnp.concatenate(
        [docs_ref[pl.ds(2 * shard + part, 1), :] for part in range(2)], axis=1
    ).astype(F32)


def doc_rows(docs_ref):
    shard = seq_index()
    own = doc_row_of(docs_ref, shard)
    before = doc_row_of(docs_ref, jnp.maximum(shard - 1, 0))
    return own, jnp.where(shard == 0, -1.0, before)


def group_halves(coeff_ref):
    coeff = coeff_ref[...].astype(F32)
    turned = pltpu.roll(coeff, STATE, 1)
    first = lax.axis_index("head") < 2
    low = iota((T, 128), 1) < STATE
    mine_low = jnp.where(low, jnp.where(first, coeff, turned), 0.0)
    mine_high = jnp.where(low, 0.0, jnp.where(first, turned, coeff))
    return mine_low.astype(BF16), mine_high.astype(BF16)


def padded_params(bias_ref, rate_ref, skip_ref, params_s):
    heads = bias_ref.shape[1]
    params_s[...] = jnp.zeros((8, 128), F32)
    for n, ref in enumerate((bias_ref, rate_ref, skip_ref)):
        params_s[n : n + 1, 0:heads] = ref[...]
    return params_s[...]


def raw_steps(step_ref):
    rows = step_ref.shape[0]
    filled = jnp.concatenate([step_ref[...], jnp.zeros((128 - rows, T), F32)], axis=0)
    return jnp.transpose(filled)


def step_and_decay(raw, params):
    step = jnp.maximum(raw, 0.0) + jnp.log1p(jnp.exp(-jnp.abs(raw)))
    return step, -step * jnp.exp(params[1:2])


def token_setup(docs_ref, step_ref, params, cum_s, step_s, mask_s, prev_s, end_s):
    own_row, before_row = doc_rows(docs_ref)
    own = columns_of(own_row)
    lane = iota((8, T), 1)
    own8 = jnp.broadcast_to(own_row, (8, T))
    before8 = jnp.broadcast_to(before_row, (8, T))
    for lag in range(1, KERNEL):
        lagged = jnp.where(lane < lag, pltpu.roll(before8, lag, 1), pltpu.roll(own8, lag, 1))
        mask_s[lag - 1] = jnp.where(own == columns_of(lagged[0:1]), 1.0, 0.0)
    prev_s[...] = jnp.where(own == before_row[:, T - 1 : T], 0.0, NEG)
    end_s[...] = jnp.where(own == own_row[:, T - 1 : T], 0.0, NEG)
    raw = raw_steps(step_ref) + params[0:1]
    step, decay = step_and_decay(raw, params)
    lower = jnp.where(iota((T, T), 0) >= iota((T, T), 1), 1.0, 0.0)
    cum = exact(lower, decay) * LOG2E
    for n, part in enumerate(split(cum, 3)):
        cum_s[n] = part
    for n, part in enumerate(split(step, 2)):
        step_s[n] = part
    return own, own_row, cum


def spread_of(step_id):
    head = iota((128, BLK), 0)
    owner = step_id * HEADS_BLK + iota((128, BLK), 1) // 64
    return jnp.where(head == owner, 1.0, 0.0).astype(BF16)


def block_gains(step_id, cum_s, step_s, prev_s, end_s):
    spread = spread_of(step_id)
    cum = dot(cum_s[0], spread) + dot(cum_s[1], spread) + dot(cum_s[2], spread)
    step = dot(step_s[0], spread) + dot(step_s[1], spread)
    enter = jnp.exp2(cum + prev_s[...])
    to_end = jnp.exp2(cum[T - 1 : T] - cum + end_s[...])
    return spread, cum, step, enter, to_end


def conv_pre(x, halo, weight, mask_s):
    extended = jnp.concatenate([halo.astype(F32), x.astype(F32)], axis=0)
    shifted = [extended[8:]]
    summed = weight[0:1] * shifted[0]
    for lag in range(1, KERNEL):
        moved = pltpu.roll(extended, lag, 0)[8:] * mask_s[lag - 1]
        shifted.append(moved)
        summed = summed + weight[lag : lag + 1] * moved
    return summed, shifted


ROWS = COLS // SHARDS
GROUPS8 = ROWS // 8
SLOT = ROWS + 8


def mixer_first_kernel(
    x_ref, halo_ref, weight_ref, gate_ref, grad_ref, step_ref, bias_ref, rate_ref,
    skip_ref, docs_ref, in_ref, out_ref,
    parts_ref,
    cum_s, step_s, mask_s, prev_s, end_s, params_s, state_s, in_s, out_s,
):
    step_id = pl.program_id(0)

    @pl.when(step_id == 0)
    def _():
        params = padded_params(bias_ref, rate_ref, skip_ref, params_s)
        cum = token_setup(
            docs_ref, step_ref, params, cum_s, step_s, mask_s, prev_s, end_s
        )[2]
        through = jnp.exp2(cum[T - 1 : T] + prev_s[T - 1 : T, 0:1])
        high, low = split(through, 2)
        row = iota((8, 128), 0)
        both = jnp.where(row == 0, high.astype(F32), jnp.where(row == 1, low.astype(F32), 0.0))
        for shard in range(SHARDS):
            state_s[SLOT * shard + ROWS : SLOT * (shard + 1)] = both
        in_s[...] = group_halves(in_ref)[0]
        out_s[...] = group_halves(out_ref)[1]

    _, _, step, enter, to_end = block_gains(step_id, cum_s, step_s, prev_s, end_s)
    pre, _ = conv_pre(x_ref[...], halo_ref[...], weight_ref[...], mask_s)
    act = pre * sigmoid(pre)
    gate = gate_ref[...].astype(F32)
    out_grad = grad_ref[...].astype(F32) * gate * sigmoid(gate)
    ended = (act * step * to_end).astype(BF16)
    entered = (out_grad * enter).astype(BF16)
    state = dot(ended, in_s[...], TN) + dot(entered, out_s[...], TN)
    for part in range(BLK // 8):
        place = step_id * (BLK // 8) + part
        target = lax.div(place, GROUPS8)
        offset = SLOT * target + 8 * (place - GROUPS8 * target)
        state_s[pl.ds(pl.multiple_of(offset, 8), 8), :] = state[8 * part : 8 * part + 8]

    @pl.when(step_id == STEPS - 1)
    def _():
        parts_ref[...] = state_s[...].astype(BF16)


TOKEN_SCRATCH = [
    pltpu.VMEM((3, T, 128), BF16),
    pltpu.VMEM((2, T, 128), BF16),
    pltpu.VMEM((KERNEL - 1, T, BLK), F32),
    pltpu.VMEM((T, BLK), F32),
    pltpu.VMEM((T, BLK), F32),
    pltpu.VMEM((8, 128), F32),
]


def mixer_specs(heads):
    return [
        column_block(T), column_block(8), column_block(KERNEL), column_block(T),
        column_block(T), whole((heads, T)), whole((1, heads)), whole((1, heads)),
        whole((1, heads)), whole((SHARDS * T // 128, 128)), whole((T, 128)), whole((T, 128)),
    ]


def mixer_first(*arrays):
    heads = arrays[5].shape[0]
    return pl.pallas_call(
        mixer_first_kernel,
        grid=(STEPS,),
        in_specs=mixer_specs(heads),
        out_specs=whole((SHARDS * SLOT, 128)),
        out_shape=jax.ShapeDtypeStruct((SHARDS * SLOT, 128), BF16),
        scratch_shapes=TOKEN_SCRATCH + [
            pltpu.VMEM((SHARDS * SLOT, 128), F32),
            pltpu.VMEM((T, 128), BF16),
            pltpu.VMEM((T, 128), BF16),
        ],
        cost_estimate=pl.CostEstimate(flops=8 * 10**9, bytes_accessed=4 * 10**6, transcendentals=0),
        name="mixer_first",
    )(*arrays)


def chain_kernel(parts_ref, out_ref, forward_s):
    slot = seq_index()
    owner = (slot * ROWS + iota((ROWS, 128), 0)) // 64
    choose = jnp.where(owner == iota((ROWS, 128), 1), 1.0, 0.0)
    lane = iota((ROWS, 128), 1)
    through = []
    carry = jnp.zeros((ROWS, 128), F32)
    for shard in range(SHARDS):
        row = parts_ref[shard, ROWS : ROWS + 1].astype(F32)
        row = row + parts_ref[shard, ROWS + 1 : ROWS + 2].astype(F32)
        gain = jnp.sum(choose * row, axis=1, keepdims=True)
        through.append(gain)
        forward_s[shard] = carry
        carry = gain * carry + parts_ref[shard, 0:ROWS].astype(F32)
    carry = jnp.zeros((ROWS, 128), F32)
    for shard in reversed(range(SHARDS)):
        out_ref[shard] = jnp.where(lane < STATE, forward_s[shard], carry).astype(BF16)
        carry = through[shard] * carry + parts_ref[shard, 0:ROWS].astype(F32)


def chain(parts):
    return pl.pallas_call(
        chain_kernel,
        in_specs=[IN_VMEM],
        out_specs=IN_VMEM,
        out_shape=jax.ShapeDtypeStruct((SHARDS, ROWS, 128), BF16),
        scratch_shapes=[pltpu.VMEM((SHARDS, ROWS, 128), F32)],
        cost_estimate=pl.CostEstimate(flops=2 * 10**9, bytes_accessed=10**6, transcendentals=0),
        name="chain",
    )(parts)


BUNDLE = KERNEL * COLS // 128
LANES_BLK = BLK // 128


def mixer_inner_kernel(
    x_ref, halo_ref, weight_ref, gate_ref, grad_ref, step_ref, bias_ref, rate_ref,
    skip_ref, docs_ref, in_ref, out_ref,
    inner_ref, dscaled_ref, dtop_ref, dbottom_ref,
    cum_s, step_s, mask_s, prev_s, end_s, params_s,
    cumt_s, pair_s, causal_s, dtop_s, dbottom_s,
):
    step_id = pl.program_id(0)

    @pl.when(step_id == 0)
    def _():
        params = padded_params(bias_ref, rate_ref, skip_ref, params_s)
        own, own_row, cum = token_setup(
            docs_ref, step_ref, params, cum_s, step_s, mask_s, prev_s, end_s
        )
        cumt_s[...] = jnp.transpose(cum)
        same = (own == own_row) & (iota((T, T), 0) >= iota((T, T), 1))
        causal_s[...] = jnp.where(same, 0.0, NEG)
        pair_s[...] = dot(group_halves(out_ref)[0], group_halves(in_ref)[0], NT)
        dtop_s[...] = jnp.zeros((HALF, HALF), F32)
        dbottom_s[...] = jnp.zeros((HALF, T), F32)

    spread = spread_of(step_id)
    cum = dot(cum_s[0], spread) + dot(cum_s[1], spread) + dot(cum_s[2], spread)
    step = dot(step_s[0], spread) + dot(step_s[1], spread)
    pre, _ = conv_pre(x_ref[...], halo_ref[...], weight_ref[...], mask_s)
    gate = gate_ref[...].astype(F32)
    scaled_half = (pre * sigmoid(pre) * step).astype(BF16)
    grad_half = (grad_ref[...].astype(F32) * gate * sigmoid(gate)).astype(BF16)

    block_head = iota((T, BLK), 1) // 64
    tops, bottoms, scaled_parts, grad_parts = [], [], [], []
    dtop, dbottom = dtop_s[...], dbottom_s[...]
    for k in range(HEADS_BLK):
        mine = block_head == k
        cum_col = cum[:, 64 * k : 64 * k + 1]
        cum_row = cumt_s[pl.ds(step_id * HEADS_BLK + k, 1), :]
        top = jnp.exp2(
            jnp.broadcast_to(cum_col[:HALF], (HALF, HALF)) - cum_row[:, :HALF]
            + causal_s[:HALF, :HALF]
        )
        bottom = jnp.exp2(
            jnp.broadcast_to(cum_col[HALF:], (HALF, T)) - cum_row + causal_s[HALF:, :]
        )
        tops.append((pair_s[:HALF, :HALF] * top).astype(BF16))
        bottoms.append((pair_s[HALF:, :] * bottom).astype(BF16))
        scaled_k = jnp.where(mine, scaled_half, jnp.zeros_like(scaled_half))
        grad_k = jnp.where(mine, grad_half, jnp.zeros_like(grad_half))
        scaled_parts.append(scaled_k)
        grad_parts.append(grad_k)
        dtop = dtop + dot(grad_k[:HALF], scaled_half[:HALF], NT) * top
        dbottom = dbottom + dot(grad_k[HALF:], scaled_half, NT) * bottom
    dtop_s[...] = dtop
    dbottom_s[...] = dbottom
    join = jnp.concatenate
    inner_ref[...] = join(
        [
            dot(join(tops, axis=1), join([v[:HALF] for v in scaled_parts], axis=0)),
            dot(join(bottoms, axis=1), join(scaled_parts, axis=0)),
        ],
        axis=0,
    )
    upper_part = dot(join(tops, axis=0), join([v[:HALF] for v in grad_parts], axis=0), TN)
    dscaled = dot(join(bottoms, axis=0), join([v[HALF:] for v in grad_parts], axis=0), TN)
    dscaled_ref[...] = join([dscaled[:HALF] + upper_part, dscaled[HALF:]], axis=0)
    dtop_ref[...] = dtop
    dbottom_ref[...] = dbottom


def mixer_inner(*arrays):
    heads = arrays[5].shape[0]
    return pl.pallas_call(
        mixer_inner_kernel,
        grid=(STEPS,),
        in_specs=mixer_specs(heads),
        out_specs=[column_block(T), column_block(T), whole((HALF, HALF)), whole((HALF, T))],
        out_shape=[
            jax.ShapeDtypeStruct((T, COLS), F32),
            jax.ShapeDtypeStruct((T, COLS), F32),
            jax.ShapeDtypeStruct((HALF, HALF), F32),
            jax.ShapeDtypeStruct((HALF, T), F32),
        ],
        scratch_shapes=TOKEN_SCRATCH + [
            pltpu.VMEM((128, T), F32),
            pltpu.VMEM((T, T), F32),
            pltpu.VMEM((T, T), F32),
            pltpu.VMEM((HALF, HALF), F32),
            pltpu.VMEM((HALF, T), F32),
        ],
        cost_estimate=pl.CostEstimate(flops=10**10, bytes_accessed=6 * 10**6, transcendentals=0),
        name="mixer_inner",
    )(*arrays)


def mixer_second_kernel(
    x_ref, halo_ref, weight_ref, gate_ref, grad_ref, step_ref, bias_ref, rate_ref,
    skip_ref, docs_ref, in_ref, out_ref, inner_ref, dscaled_ref, dtop_ref, dbottom_ref,
    state_ref,
    dx_ref, tail_ref, spill_ref, dgate_ref, dstep_ref, coeff_ref, bundle_ref,
    cum_s, step_s, mask_s, prev_s, end_s, params_s,
    coeff_s, row_s, dt_s, ends_s, bundle_s,
    in_low_s, in_high_s, out_low_s, out_high_s,
):
    step_id = pl.program_id(0)
    lane = iota((T, 128), 1)

    @pl.when(step_id == 0)
    def _():
        params = padded_params(bias_ref, rate_ref, skip_ref, params_s)
        token_setup(docs_ref, step_ref, params, cum_s, step_s, mask_s, prev_s, end_s)
        in_low_s[...], in_high_s[...] = group_halves(in_ref)
        out_low_s[...], out_high_s[...] = group_halves(out_ref)
        coeff_s[...] = jnp.zeros((T, 128), F32)
        row_s[...] = jnp.zeros((T, 128), F32)
        dt_s[...] = jnp.zeros((T, 128), F32)
        ends_s[...] = jnp.zeros((8, 128), F32)

    out_low = out_low_s[...]
    in_high = in_high_s[...]
    spread, _, step, enter, to_end = block_gains(step_id, cum_s, step_s, prev_s, end_s)
    skip = sum(dot(part, spread) for part in split(params_s[...], 3))[2:3]
    weight = weight_ref[...]
    pre, shifted = conv_pre(x_ref[...], halo_ref[...], weight, mask_s)
    sig = sigmoid(pre)
    act = pre * sig
    gate = gate_ref[...].astype(F32)
    gate_sig = sigmoid(gate)
    mix_grad = grad_ref[...].astype(F32)
    out_grad = mix_grad * gate * gate_sig
    scaled = act * step
    scaled_half = scaled.astype(BF16)
    grad_half = out_grad.astype(BF16)

    join = jnp.concatenate
    inner, dscaled = inner_ref[...], dscaled_ref[...]
    state = state_ref[...]
    carried = dot(out_low, state, NT) * enter
    from_end = dot(in_high, state, NT) * to_end
    ssm_out = inner + carried
    dscaled = dscaled + from_end
    mixed_out = ssm_out + skip * act
    dgate_ref[...] = (
        mix_grad * mixed_out * gate_sig * (1.0 + gate * (1.0 - gate_sig))
    ).astype(BF16)

    gave_out = dot((out_grad * enter).astype(BF16), state)
    gave_in = dot((scaled * to_end).astype(BF16), state)
    coeff_s[...] += jnp.where(lane < STATE, gave_out, gave_in)

    grad_round = grad_half.astype(F32)
    scaled_round = scaled_half.astype(F32)
    balance = grad_round * ssm_out - scaled_round * dscaled
    row_s[...] += sum(dot(part, spread, NT) for part in split(balance, 2))
    dt_s[...] += dot((dscaled * act).astype(BF16), spread, NT)

    state_wide = state.astype(F32)
    product = state_wide * pltpu.roll(state_wide, STATE, 1)
    through = jnp.sum(jnp.where(iota((BLK, 128), 1) < STATE, product, 0.0), axis=1, keepdims=True)
    through_row = jnp.transpose(jnp.broadcast_to(through, (BLK, BLK)))[0:1]
    end_row = jnp.sum(scaled_round * from_end, axis=0, keepdims=True)
    end_row = end_row + through_row * enter[T - 1 : T]
    skip_row = jnp.sum(out_grad * act, axis=0, keepdims=True)
    row8 = iota((8, BLK), 0)
    both = jnp.where(row8 == 0, end_row, jnp.where(row8 == 1, skip_row, 0.0))
    ends_s[...] += sum(dot(part, spread, NT) for part in split(both, 3))

    dact = step * dscaled + skip * out_grad
    dpre = dact * sig * (1.0 + pre * (1.0 - sig))
    zeros = jnp.zeros((8, BLK), F32)
    dx = weight[0:1] * dpre
    spill = zeros
    for lag in range(KERNEL):
        tap = jnp.sum(dpre * shifted[lag], axis=0, keepdims=True)
        for m in range(LANES_BLK):
            place = lag * (COLS // 128) + step_id * LANES_BLK + m
            bundle_s[pl.ds(place, 1), :] = tap[:, 128 * m : 128 * (m + 1)]
        if lag == 0:
            continue
        masked = dpre * mask_s[lag - 1]
        later = pltpu.roll(jnp.concatenate([masked, zeros], axis=0), T + 8 - lag, 0)[:T]
        dx = dx + weight[lag : lag + 1] * later
        edge = pltpu.roll(jnp.concatenate([zeros, masked[:8]], axis=0), 16 - lag, 0)[:8]
        spill = spill + weight[lag : lag + 1] * edge
    dx_ref[...] = dx.astype(BF16)
    tail_ref[...] = dx[T - 8 :]
    spill_ref[...] = spill

    @pl.when(step_id == STEPS - 1)
    def _():
        params = params_s[...]
        raw = raw_steps(step_ref) + params[0:1]
        rate = jnp.exp(params[1:2])
        decay = step_and_decay(raw, params)[1]
        upper = jnp.where(iota((T, T), 1) >= iota((T, T), 0), 1.0, 0.0)
        ends = ends_s[...]
        ddecay = exact(upper, row_s[...]) + ends[0:1]
        dstep = (dt_s[...] - ddecay * rate) * sigmoid(raw)
        dstep_ref[...] = jnp.transpose(dstep)[: dstep_ref.shape[0]]
        dbias = jnp.sum(dstep, axis=0, keepdims=True)
        drate = jnp.sum(ddecay * decay, axis=0, keepdims=True)
        row = iota((8, 128), 0)
        small = jnp.zeros((8, 128), F32)
        for n, vector in enumerate((dbias, drate, ends[1:2])):
            for m, part in enumerate(split(vector, 2)):
                small = jnp.where(row == 2 * n + m, part.astype(F32), small)
        bundle_s[BUNDLE : BUNDLE + 8] = small
        bundle = bundle_s[...].astype(BF16)
        for shard in range(SHARDS):
            bundle_ref[shard] = bundle
        top_half, bottom_half = dtop_ref[...].astype(BF16), dbottom_ref[...].astype(BF16)
        in_low, out_high = in_low_s[...], out_high_s[...]
        out_part = join([dot(top_half, in_low[:HALF]), dot(bottom_half, in_low)], axis=0)
        in_part = dot(bottom_half, out_high[HALF:], TN)
        in_part = join(
            [in_part[:HALF] + dot(top_half, out_high[:HALF], TN), in_part[HALF:]], axis=0
        )
        coeff_ref[...] = (coeff_s[...] + out_part + in_part).astype(BF16)


def mixer_second(*arrays):
    heads = arrays[5].shape[0]
    half = pltpu.VMEM((T, 128), BF16)
    return pl.pallas_call(
        mixer_second_kernel,
        grid=(STEPS,),
        in_specs=mixer_specs(heads) + [
            column_block(T), column_block(T), whole((HALF, HALF)), whole((HALF, T)),
            pl.BlockSpec((BLK, 128), lambda c: (c, 0)),
        ],
        out_specs=[
            column_block(T), column_block(8), column_block(8), column_block(T),
            whole((heads, T)), whole((T, 128)), whole((SHARDS, BUNDLE + 8, 128)),
        ],
        out_shape=[
            jax.ShapeDtypeStruct((T, COLS), BF16),
            jax.ShapeDtypeStruct((8, COLS), F32),
            jax.ShapeDtypeStruct((8, COLS), F32),
            jax.ShapeDtypeStruct((T, COLS), BF16),
            jax.ShapeDtypeStruct((heads, T), F32),
            jax.ShapeDtypeStruct((T, 128), BF16),
            jax.ShapeDtypeStruct((SHARDS, BUNDLE + 8, 128), BF16),
        ],
        scratch_shapes=TOKEN_SCRATCH + [
            pltpu.VMEM((T, 128), F32),
            pltpu.VMEM((T, 128), F32),
            pltpu.VMEM((T, 128), F32),
            pltpu.VMEM((8, 128), F32),
            pltpu.VMEM((BUNDLE + 8, 128), F32),
            half, half, half, half,
        ],
        cost_estimate=pl.CostEstimate(flops=18 * 10**9, bytes_accessed=8 * 10**6, transcendentals=0),
        name="mixer_second",
    )(*arrays)


def finish_kernel(bundle_ref, *refs):
    coeff_refs = refs[:LOCAL_HEADS]
    weight_ref, bias_ref, rate_ref, skip_ref, in_ref, out_ref, coeff_s = refs[LOCAL_HEADS:]
    for turn, ref in enumerate(coeff_refs):
        coeff_s[lax.rem(lax.axis_index("head") - turn + LOCAL_HEADS, LOCAL_HEADS)] = ref[...].astype(F32)
    total = bundle_ref[0].astype(F32)
    for shard in range(1, SHARDS):
        total = total + bundle_ref[shard].astype(F32)
    tiles = COLS // 128
    for lag in range(KERNEL):
        for m in range(tiles):
            weight_ref[lag : lag + 1, 128 * m : 128 * (m + 1)] = total[
                lag * tiles + m : lag * tiles + m + 1
            ]
    for n, ref in enumerate((bias_ref, rate_ref, skip_ref)):
        row = BUNDLE + 2 * n
        ref[...] = (total[row : row + 1] + total[row + 1 : row + 2])[:, : ref.shape[1]]
    low, high = coeff_s[0] + coeff_s[1], coeff_s[2] + coeff_s[3]
    left = iota((T, 128), 1) < STATE
    out_ref[...] = jnp.where(left, low, pltpu.roll(high, STATE, 1))
    in_ref[...] = jnp.where(left, pltpu.roll(low, STATE, 1), high)


def finish(bundle, coeffs, heads):
    small = jax.ShapeDtypeStruct((1, heads), F32)
    wide = jax.ShapeDtypeStruct((T, 128), F32)
    return pl.pallas_call(
        finish_kernel,
        in_specs=[IN_VMEM] * (1 + LOCAL_HEADS),
        out_specs=[IN_VMEM] * 6,
        out_shape=[jax.ShapeDtypeStruct((KERNEL, COLS), F32), small, small, small, wide, wide],
        scratch_shapes=[pltpu.VMEM((LOCAL_HEADS, T, 128), F32)],
        name="finish",
    )(bundle, *coeffs)


ROW = 4
K_AT, V_AT, Q_AT, G_AT = (slice(n * HEAD_DIM, (n + 1) * HEAD_DIM) for n in range(4))
PAIR = (2 * HEAD_DIM, T)


def pack_kernel(k_ref, v_ref, q_ref, g_ref, *refs):
    out_refs, turned_s = refs[:ROW], refs[ROW]
    for ref, place in ((k_ref, K_AT), (v_ref, V_AT), (q_ref, Q_AT), (g_ref, G_AT)):
        turned_part = jnp.transpose(ref[...])
        for head in range(LOCAL_HEADS):
            turned_s[head, place] = turned_part[head * HEAD_DIM : (head + 1) * HEAD_DIM]
    for turn in range(ROW):
        out_refs[turn][...] = turned_s[lax.rem(row_place() + turn, ROW)]


def pack(keys, values, queries, grads):
    return pl.pallas_call(
        pack_kernel,
        in_specs=[IN_VMEM] * 4,
        out_specs=[IN_VMEM] * ROW,
        out_shape=[jax.ShapeDtypeStruct((4 * HEAD_DIM, T), BF16)] * ROW,
        scratch_shapes=[pltpu.VMEM((LOCAL_HEADS, 4 * HEAD_DIM, T), BF16)],
        name="pack",
    )(keys, values, queries, grads)


def lend_kernel(*refs):
    for turn, ref in enumerate(refs[:ROW]):
        refs[ROW][turn * PAIR[0] : (turn + 1) * PAIR[0]] = ref[: PAIR[0]]


def lend(own):
    return pl.pallas_call(
        lend_kernel,
        in_specs=[IN_VMEM] * ROW,
        out_specs=IN_VMEM,
        out_shape=jax.ShapeDtypeStruct((ROW * PAIR[0], T), BF16),
        name="lend",
    )(*own)


def attention_kernel(docs_ref, far_ref, *refs):
    arrived, (dq_ref, own_ref, back_ref, far_s, qg_s, kv_s) = refs[:ROW], refs[ROW:]
    for turn in range(ROW):
        block = lax.rem(row_place() - turn + ROW, ROW)
        kv_s[ROW + block] = arrived[turn][: PAIR[0]]
        qg_s[block] = arrived[turn][PAIR[0] :]
        kv_s[block] = far_ref[turn * PAIR[0] : (turn + 1) * PAIR[0]]
    first_block = lax.div(seq_index(), ROW) * ROW
    later = iota((T, T), 1) > iota((T, T), 0)
    scale = HEAD_DIM ** (-0.5)

    def doc_row(block):
        place = first_block + block
        row = doc_row_of(docs_ref, jnp.maximum(place, 0))
        return row if block >= 0 else jnp.where(place < 0, -1.0, row)

    rows = {block: doc_row(block) for block in range(-ROW, ROW)}
    for i in range(ROW):
        own_doc = columns_of(rows[i])
        qt, gt = qg_s[i, K_AT], qg_s[i, V_AT]
        q, g = jnp.transpose(qt), jnp.transpose(gt)

        def part(gap, place):
            return kv_s[ROW + i - gap, place]

        scores = []
        top = None
        for gap in range(ROW + 1):
            same = own_doc == rows[i - gap]
            if gap == 0:
                same = same & jnp.logical_not(later)
            if gap == ROW:
                same = same & later
            s = jnp.where(same, dot(q, part(gap, K_AT)) * (scale * LOG2E), NEG)
            scores.append(s)
            top = s if top is None else jnp.maximum(top, s)
        top = jnp.max(top, axis=1, keepdims=True)
        expos = [jnp.exp2(s - top) for s in scores]
        total = jnp.sum(sum(expos), axis=1, keepdims=True)
        inverse = 1.0 / jnp.maximum(total, 1.0)
        probs = [e * inverse for e in expos]
        halves = [p.astype(BF16) for p in probs]
        dprobs = [dot(g, part(gap, V_AT)) for gap in range(ROW + 1)]
        delta = sum(h.astype(F32) * d for h, d in zip(halves, dprobs))
        delta = jnp.sum(delta, axis=1, keepdims=True)
        dq = jnp.zeros((HEAD_DIM, T), F32)
        for gap in range(ROW + 1):
            dscore = (probs[gap] * (dprobs[gap] - delta)).astype(BF16)
            dq = dq + dot(part(gap, K_AT), dscore, NT)
            block = i - gap
            ref, index = (own_ref, block) if block >= 0 else (far_s, block + ROW)
            dk, dv = dot(qt, dscore), dot(gt, halves[gap])
            if gap == 0 or (block < 0 and i == 0):
                ref[index, K_AT] = dk
                ref[index, V_AT] = dv
            else:
                ref[index, K_AT] += dk
                ref[index, V_AT] += dv
            if gap == ROW:
                back_ref[index] = far_s[index].astype(BF16)
        dq_ref[i] = (dq * scale).astype(BF16)


def attention(docs, far, own):
    pairs = (ROW, *PAIR)
    return pl.pallas_call(
        attention_kernel,
        in_specs=[IN_VMEM] * (2 + ROW),
        out_specs=[IN_VMEM] * 3,
        out_shape=[
            jax.ShapeDtypeStruct((ROW, HEAD_DIM, T), BF16),
            jax.ShapeDtypeStruct(pairs, F32),
            jax.ShapeDtypeStruct(pairs, BF16),
        ],
        scratch_shapes=[
            pltpu.VMEM(pairs, F32),
            pltpu.VMEM(pairs, BF16),
            pltpu.VMEM((2 * ROW, *PAIR), BF16),
        ],
        cost_estimate=pl.CostEstimate(flops=12 * 10**9, bytes_accessed=8 * 10**6, transcendentals=0),
        name="attention",
    )(docs, far, *own)


def merge_kernel(dq_ref, dkv_ref, back_ref, *out_refs):
    scale = HEAD_DIM ** (-0.5)
    place = row_place()
    for turn, out_ref in enumerate(out_refs):
        block = lax.rem(place + turn, ROW)
        total = dkv_ref[block] + back_ref[block].astype(F32)
        out_ref[K_AT] = (total[K_AT] * scale).astype(BF16)
        out_ref[V_AT] = total[V_AT].astype(BF16)
        out_ref[Q_AT] = dq_ref[block]


def merge(dq, dkv, back):
    return pl.pallas_call(
        merge_kernel,
        in_specs=[IN_VMEM] * 3,
        out_specs=[IN_VMEM] * ROW,
        out_shape=[jax.ShapeDtypeStruct((3 * HEAD_DIM, T), BF16)] * ROW,
        cost_estimate=pl.CostEstimate(flops=3 * 10**9, bytes_accessed=4 * 10**6, transcendentals=0),
        name="merge",
    )(dq, dkv, back)


def unpack_kernel(*refs):
    parts, outs, stacked_s = refs[:ROW], refs[ROW : ROW + 3], refs[ROW + 3]
    place = row_place()
    for turn, part in enumerate(parts):
        source = lax.rem(place - turn + ROW, ROW)
        for n, at in enumerate((Q_AT, K_AT, V_AT)):
            stacked_s[n, source] = part[at]
    for n, ref in enumerate(outs):
        stacked = jnp.concatenate([stacked_s[n, h] for h in range(LOCAL_HEADS)], axis=0)
        ref[...] = jnp.transpose(stacked)


def unpack(parts):
    wide = jax.ShapeDtypeStruct((T, LOCAL_HEADS * HEAD_DIM), BF16)
    return pl.pallas_call(
        unpack_kernel,
        in_specs=[IN_VMEM] * ROW,
        out_specs=[IN_VMEM] * 3,
        out_shape=[wide] * 3,
        scratch_shapes=[pltpu.VMEM((3, LOCAL_HEADS, HEAD_DIM, T), BF16)],
        cost_estimate=pl.CostEstimate(flops=2 * 10**9, bytes_accessed=3 * 10**6, transcendentals=0),
        name="unpack",
    )(*parts)


def passed_along(value, axis, steps):
    count = lax.axis_size(axis)
    initial, last = (max(0, -steps), min(count, count - steps))
    return lax.ppermute(value, axis, [(source, source + steps) for source in range(initial, last)])


def turns(parts, axis):
    count = lax.axis_size(axis)
    return [parts[0]] + [
        lax.ppermute(part, axis, [(n, (n + turn) % count) for n in range(count)])
        for turn, part in enumerate(parts[1:], 1)
    ]


def near(array):
    return pltpu.with_memory_space_constraint(array, pltpu.VMEM)


def exchange(array, axis):
    return lax.all_to_all(array, axis, split_axis=0, concat_axis=0, tiled=True)


def local(
    queries, keys, values, attn_grad, doc_ids, conv_input, conv_weight, step_raw, step_bias,
    rate_log, skip_gain, input_coeff, output_coeff, gate_input, mix_grad,
):
    heads = step_raw.shape[1]
    docs = doc_ids.reshape(SHARDS * T // 128, 128)
    halo = passed_along(conv_input[T - 8 :], SEQ, 1)
    parts = pack(keys, values, queries, attn_grad)
    own = [near(v) for v in turns(parts, "seq_2")]
    lent = lend(own)
    far = passed_along(lent, SEQ, ROW)

    mixer_args = (
        conv_input, halo, conv_weight, gate_input, mix_grad, step_raw.T,
        step_bias.reshape(1, heads), rate_log.reshape(1, heads), skip_gain.reshape(1, heads),
        docs, input_coeff, output_coeff,
    )
    parts = mixer_first(*mixer_args).reshape(SHARDS, SLOT, 128)
    gathered = exchange(parts, SEQ)
    scanned = chain(near(gathered))
    entering = exchange(scanned, SEQ).reshape(COLS, 128)
    inside = mixer_inner(*mixer_args)
    dq, dkv, back = attention(docs, near(far), own)
    returned = passed_along(back, SEQ, -ROW)
    dx, tail, spill, dgate, dstep, coeff, bundle = mixer_second(
        *mixer_args, *inside, entering
    )
    leaving = merge(dq, dkv, near(returned))
    swapped = turns(leaving, "seq_2")
    spilled = passed_along(spill, SEQ, -1)
    bundles = exchange(bundle, SEQ)
    coeffs = turns([coeff] * LOCAL_HEADS, "head")
    dq, dk, dv = unpack(swapped[:1] + [near(v) for v in swapped[1:]])
    grad_weight, grad_bias, grad_rate, grad_skip, sum_in, sum_out = finish(
        near(bundles), coeffs[:1] + [near(v) for v in coeffs[1:]], heads
    )
    tail = (tail + spilled).astype(BF16)
    grad_conv = lax.dynamic_update_slice_in_dim(dx, tail, T - 8, 0)
    return (
        dq, dk, dv, grad_conv, dgate, dstep.T, sum_in, sum_out, grad_weight,
        grad_bias.reshape(heads), grad_rate.reshape(heads), grad_skip.reshape(heads),
    )


def solution(mesh):
    finer = Mesh(
        mesh.devices.reshape(4, 2, 4, mesh.shape["head"]), ("seq_0", "seq_1", "seq_2", "head")
    )
    wide = P(SEQ, "head")
    return jax.shard_map(
        local,
        mesh=finer,
        in_specs=(
            wide, wide, wide, wide, P(), wide, P(None, "head"), wide, P("head"), P("head"),
            P("head"), P(SEQ, None), P(SEQ, None), wide, wide,
        ),
        out_specs=(
            wide, wide, wide, wide, wide, wide, P(SEQ, None), P(SEQ, None), P(None, "head"),
            P("head"), P("head"), P("head"),
        ),
        check_vma=False,
    )
```
